32 devices in a mesh: lat: 8 (over y, x, core), lon: 4 (over z).
Axes of the slice: x: 2, y: 2, z: 4, core: 2. Of those that a mesh axis runs over, the one named last changes fastest.
Arguments:
- tokens: bfloat16 [2, 48, 48, 1024], P(None, 'lat', 'lon'), may hold values from -6 to 6
- layer_norm_gain: float32 [1024], replicated, may hold values from 0.5 to 1.5
- layer_norm_bias: float32 [1024], replicated, may hold values from -3 to 3
- w_qkv: bfloat16 [1024, 1536], replicated, may hold values from -2 to 2
- w_out: bfloat16 [512, 1024], replicated, may hold values from -0.25 to 0.25
- output_cotangent: bfloat16 [2, 48, 48, 1024], P(None, 'lat', 'lon'), may hold values from -6 to 6
Outputs:
- output: bfloat16 [2, 48, 48, 1024], P(None, 'lat', 'lon')
- token_gradient: bfloat16 [2, 48, 48, 1024], P(None, 'lat', 'lon')
- d_qkv: float32 [1024, 1536], P(('lat', 'lon'))
- d_out: float32 [512, 1024], P(None, ('lat', 'lon'))
- gain_gradient_scaled: float32 [1024], P(('lat', 'lon'))
- d_bias: float32 [1024], P(('lat', 'lon'))
The draws below stay inside these ranges and needn't reach their ends.
All inputs are finite; a program needn't handle non-finite values.
Results may differ from the reference program's by a relative error of at most 0.0093.
Values may be sent and summed in bfloat16 or wider, within the bound.
No kernel may reach another device: no remote copies, remote signals or barrier semaphores. Data moves between devices by JAX's collectives and lax.ppermute only.
A program may use at most 64 MiB of HBM per device.

```python
import math
import jax
import jax.numpy as jnp
from jax import lax

D = 1024
HEADS = 8
HDIM = 64
WLAT = 6
WLON = 12
LEV = 2
HD = 512
NLAT = 48
NLON = 48
TOKENS = 4608


def draw_w_qkv(key, part):
    inner_width = HEADS * HDIM
    first_key = jax.random.fold_in(jax.random.fold_in(key, 11), 0)
    base = jax.random.normal(first_key, (D, 3 * inner_width), jnp.float32) / math.sqrt(D)
    result = base
    return jnp.clip(result, -2.0, 2.0).astype(jnp.bfloat16)


def with_spikes(entries, rng, source, target, blocks, factor):
    owner, partner = [(jnp.arange(entries.shape[position]) // (entries.shape[position] // blocks)).reshape([-1 if axis == position else 1 for axis in range(entries.ndim)]) for position in (source, target)]
    chosen = jax.random.permutation(rng, blocks)[partner]
    strong = (owner == chosen) | (owner == (partner + blocks // 2) % blocks)
    return jnp.where(strong, factor * entries, entries)


def block_levels(rng, dims, cuts, least, largest):
    def one(axis_at, blocks):
        draws = jax.random.uniform(jax.random.fold_in(jax.random.fold_in(rng, 6), axis_at), (blocks,), jnp.float32, least / len(cuts), largest / len(cuts))
        return jnp.repeat(jnp.exp(draws), dims[axis_at] // blocks).reshape((-1,) + (1,) * (len(dims) - axis_at - 1))

    loudness = one(*cuts[0])
    for cut in cuts[1:]:
        loudness = loudness * one(*cut)
    return loudness


def centred(own_key, shape, width, bound, cuts=(), held_as=jnp.bfloat16):
    values = jax.random.normal(own_key, shape, jnp.float32) * width
    if len(cuts) > 0:
        values = block_levels(own_key, shape, cuts, -0.22, 0.18) * values
    return jnp.clip(values, min=-bound, max=bound).astype(held_as)


def bell_draw_with(rng, extent, spread, limit, shards, heavy, dtype=jnp.bfloat16):
    drawn = spread * jax.random.normal(rng, extent, jnp.float32)
    if shards:
        drawn = drawn * block_levels(rng, extent, shards, -0.22, 0.18)
    return jnp.clip(with_spikes(drawn, jax.random.fold_in(rng, 3), *heavy), -limit, limit).astype(dtype)


def setup_inputs(seed: int = 0) -> dict:
    key_list = jax.random.split(jax.random.key(seed), 7)
    return {
        "tokens": centred(key_list[0], (LEV, NLAT, NLON, D), 1.0, 6.0, ((1, 8), (2, 4))),
        "layer_norm_gain": jnp.clip(1.0 + 0.1 * jax.random.normal(key_list[1], (D,), jnp.float32), 0.5, 1.5),
        "layer_norm_bias": centred(key_list[2], (D,), 0.5, 3.0, (), jnp.float32),
        "w_qkv": draw_w_qkv(jax.random.fold_in(key_list[6], 71), 0),
        "w_out": centred(key_list[4], (HD, D), HD ** -0.5, 0.25),
        "output_cotangent": bell_draw_with(key_list[5], (LEV, NLAT, NLON, D), 1.0, 6.0, ((1, 8), (2, 4)), (2, 3, 4, 2.0)),
    }


def windows(grid_data, win_rows):
    levels, row_total, col_total, channels = grid_data.shape
    grid_data = grid_data.reshape(levels, row_total // win_rows, win_rows, col_total // WLON, WLON, channels)
    grid_data = grid_data.transpose(1, 3, 0, 2, 4, 5)
    return grid_data.reshape(-1, levels * win_rows * WLON, channels)

def from_windows(win_data, levels, row_total, col_total, win_rows):
    channels = win_data.shape[-1]
    grid_data = win_data.reshape(row_total // win_rows, col_total // WLON, levels, win_rows, WLON, channels)
    grid_data = grid_data.transpose(2, 0, 3, 1, 4, 5)
    return grid_data.reshape(levels, row_total, col_total, channels)

def attend(queries, key_part, value_part, grad_att, key_valid):
    score_scale = queries.shape[-1] ** (-0.5)
    query_wide = queries.astype(jnp.float32)
    key_wide = key_part.astype(jnp.float32)
    value_wide = value_part.astype(jnp.float32)
    grad_wide = grad_att.astype(jnp.float32)
    scores = jnp.einsum('nqhd,nkhd->nhqk', query_wide, key_wide) * score_scale
    scores = jnp.where(key_valid[:, None, None, :], scores, -1e+30)
    row_max = lax.optimization_barrier(jnp.max(scores, axis=-1, keepdims=True))
    exp_scores = jnp.exp(scores - row_max)
    probabilities = exp_scores / lax.optimization_barrier(jnp.sum(exp_scores, axis=-1, keepdims=True))
    probs_low = lax.optimization_barrier(probabilities.astype(jnp.bfloat16)).astype(jnp.float32)
    attended = jnp.einsum('nhqk,nkhd->nqhd', probs_low, value_wide).astype(jnp.bfloat16)
    grad_prob = jnp.einsum('nqhd,nkhd->nhqk', grad_wide, value_wide)
    row_inner = lax.optimization_barrier(jnp.sum(probabilities * grad_prob, axis=-1, keepdims=True))
    grad_score = lax.optimization_barrier((probabilities * (grad_prob - row_inner)).astype(jnp.bfloat16)).astype(jnp.float32)
    grad_query = (jnp.einsum('nhqk,nkhd->nqhd', grad_score, key_wide) * score_scale).astype(jnp.bfloat16)
    grad_key = jnp.einsum('nhqk,nqhd->nkhd', grad_score, query_wide) * score_scale
    grad_value = jnp.einsum('nhqk,nqhd->nkhd', probs_low, grad_wide)
    return (attended, grad_query, grad_key, grad_value)

def reference(tokens, layer_norm_gain, layer_norm_bias, w_qkv, w_out, output_cotangent):
    half_lat = WLAT // 2
    half_lon = WLON // 2
    norm_factor = 1.0 / math.sqrt(TOKENS)
    tokens_wide = tokens.astype(jnp.float32)
    average = lax.optimization_barrier(jnp.mean(tokens_wide, axis=-1, keepdims=True))
    centered_input = tokens_wide - average
    inverse_deviation = lax.rsqrt(lax.optimization_barrier(jnp.mean(centered_input * centered_input, axis=-1, keepdims=True)) + 1e-05)
    standardized_input = centered_input * inverse_deviation
    normalized_tokens = (standardized_input * layer_norm_gain + layer_norm_bias).astype(jnp.bfloat16)
    flat_normed = normalized_tokens.reshape(-1, D)
    projected = jnp.dot(flat_normed, w_qkv, preferred_element_type=jnp.float32).astype(jnp.bfloat16)
    grad_flat = output_cotangent.reshape(-1, D)
    grad_att = jnp.dot(grad_flat, w_out.T, preferred_element_type=jnp.float32).astype(jnp.bfloat16)
    stacked = jnp.concatenate([projected, grad_att], axis=-1).reshape(LEV, NLAT, NLON, 4 * HD)
    stacked = jnp.pad(stacked, ((0, 0), (half_lat, half_lat), (half_lon, half_lon), (0, 0)))
    row_index = jnp.arange(NLAT + WLAT)
    row_ok = jnp.logical_and(row_index >= half_lat, row_index < NLAT + half_lat).astype(jnp.float32)
    col_index = jnp.arange(NLON + WLON)
    col_ok = jnp.logical_and(col_index >= half_lon, col_index < NLON + half_lon).astype(jnp.float32)
    valid_grid = row_ok.reshape(1, NLAT + WLAT, 1, 1) * col_ok.reshape(1, 1, NLON + WLON, 1)
    valid_grid = jnp.broadcast_to(valid_grid, (LEV, NLAT + WLAT, NLON + WLON, 1))
    lat_groups = (NLAT + WLAT) // WLAT
    lon_groups = (NLON + WLON) // WLON
    win_data = windows(stacked, WLAT)
    win_len = win_data.shape[1]
    win_data = win_data.reshape(lat_groups, lon_groups, win_len, 4 * HD)
    win_valid = (windows(valid_grid, WLAT)[..., 0] > 0.5).reshape(lat_groups, lon_groups, win_len)

    def one_band(operands):
        block, block_valid = operands
        parts = block.reshape(lon_groups, win_len, 4, HEADS, HDIM)
        attended, grad_query, grad_key, grad_value = attend(parts[:, :, 0], parts[:, :, 1], parts[:, :, 2], parts[:, :, 3], block_valid)
        pieces = [attended, grad_query, grad_key.astype(jnp.bfloat16), grad_value.astype(jnp.bfloat16)]
        return jnp.concatenate([piece.reshape(lon_groups, win_len, HD) for piece in pieces], axis=-1)
    results = lax.map(one_band, (win_data, win_valid))
    results = from_windows(results.reshape(lat_groups * lon_groups, win_len, 4 * HD), LEV, NLAT + WLAT, NLON + WLON, WLAT)
    results = results[:, half_lat:half_lat + NLAT, half_lon:half_lon + NLON]
    attended = results[..., :HD].reshape(-1, HD)
    grad_proj = results[..., HD:].reshape(-1, 3 * HD)
    mixed = jnp.dot(attended, w_out, preferred_element_type=jnp.float32).reshape(tokens_wide.shape)
    y_out = (tokens_wide + mixed).astype(jnp.bfloat16)
    d_out = jnp.dot(attended.T, grad_flat, preferred_element_type=jnp.float32) * norm_factor
    d_qkv = jnp.dot(flat_normed.T, grad_proj, preferred_element_type=jnp.float32) * norm_factor
    gradient_of_normalized = jnp.dot(grad_proj, w_qkv.T, preferred_element_type=jnp.float32).reshape(tokens_wide.shape)
    gain_gradient_scaled = lax.optimization_barrier(jnp.sum(gradient_of_normalized * standardized_input, axis=(0, 1, 2))) * norm_factor
    d_bias = lax.optimization_barrier(jnp.sum(gradient_of_normalized, axis=(0, 1, 2))) * norm_factor
    gradient_of_standardized = gradient_of_normalized * layer_norm_gain
    first_moment_term = lax.optimization_barrier(jnp.mean(gradient_of_standardized, axis=-1, keepdims=True))
    second_moment_term = lax.optimization_barrier(jnp.mean(gradient_of_standardized * standardized_input, axis=-1, keepdims=True))
    token_gradient = (output_cotangent.astype(jnp.float32) + (gradient_of_standardized - first_moment_term - standardized_input * second_moment_term) * inverse_deviation).astype(jnp.bfloat16)
    return (y_out, token_gradient, d_qkv, d_out, gain_gradient_scaled, d_bias)
```

```python
import functools
import math

import jax
import jax.numpy as jnp
from jax import lax
from jax.experimental import pallas as pl
from jax.experimental.pallas import tpu as pltpu
from jax.sharding import PartitionSpec as P

HDIM = 64
WLAT = 6
WLON = 12
F32 = jnp.float32
BF16 = jnp.bfloat16
LANES = 128

VMEM_SPEC = pl.BlockSpec(memory_space=pltpu.VMEM)
SMEM_SPEC = pl.BlockSpec(memory_space=pltpu.SMEM)


def dot(a, b, contract):
    return lax.dot_general(a, b, ((contract[0], contract[1]), ((), ())), preferred_element_type=F32)


def call(body, name, outs, args, scratch=(), smem=0, cost=None):
    specs = [SMEM_SPEC] * smem + [VMEM_SPEC] * (len(args) - smem)
    return pl.pallas_call(
        body,
        name=name,
        out_shape=[jax.ShapeDtypeStruct(s, d) for s, d in outs],
        in_specs=specs,
        out_specs=[VMEM_SPEC] * len(outs),
        scratch_shapes=list(scratch),
        cost_estimate=cost,
    )(*args)


def corners(rows, cols):
    return ((rows // 2, cols // 2), (rows // 2, 0), (0, cols // 2), (0, 0))


def pack_body(tok_ref, cot_ref, *refs):
    outs, wide = refs[:4], refs[4]
    levels, rows, cols, width = tok_ref.shape
    half_rows, half_cols = rows // 2, cols // 2
    for out_ref, (row0, col0) in zip(outs, corners(rows, cols)):
        for part, ref in enumerate((tok_ref, cot_ref)):
            for level in range(levels):
                for row in range(half_rows):
                    at = (level * half_rows + row) * half_cols
                    line = ref[level, row0 + row].astype(F32)
                    wide[at : at + half_cols, :] = line[col0 : col0 + half_cols]
            out_ref[:, part * width : (part + 1) * width] = wide[...].astype(BF16)


def gather_tokens(quads, part, wide):
    count, width = quads[0].shape[0], wide.shape[1]
    for place, quad in enumerate(quads):
        wide[place * count : (place + 1) * count, :] = quad[
            :, part * width : (part + 1) * width
        ].astype(F32)
    return wide[...]


def normalize(tokens_wide):
    average = jnp.mean(tokens_wide, axis=-1, keepdims=True)
    centered = tokens_wide - average
    inverse = lax.rsqrt(jnp.mean(centered * centered, axis=-1, keepdims=True) + 1e-05)
    return centered * inverse, inverse


def reorder(order_ref, source, target, group):
    for place in range(source.shape[0] // group):
        start = pl.multiple_of(order_ref[place] * group, group)
        target[place * group : (place + 1) * group, :] = source[pl.ds(start, group), :]


def attention_body(
    group, order_ref, edge_ref, q0, q1, q2, q3, gain_ref, bias_ref, w_qkv_ref, w_out_ref,
    keep_ref, send_ref, y_ref, gproj_ref, normed_t_ref,
    wide, att, side, turned,
):
    quads = (q0, q1, q2, q3)
    count = q0.shape[0]
    inner = w_out_ref.shape[0]
    heads = inner // HDIM
    scale = HDIM ** (-0.5)
    grad = gather_tokens(quads, 1, wide).astype(BF16)
    side[...] = wide[...].T.astype(BF16)
    reorder(order_ref, side, turned, group)
    tokens_wide = gather_tokens(quads, 0, wide)
    standard, _ = normalize(tokens_wide)
    normed = standard * gain_ref[...] + bias_ref[...]
    side[...] = normed.T.astype(BF16)
    reorder(order_ref, side, normed_t_ref, group)
    projected = dot(normed.astype(BF16), w_qkv_ref[...], ((1,), (0,))).astype(BF16)
    grad_att = dot(grad, w_out_ref[...], ((1,), (1,))).astype(BF16)
    total = 4 * count
    row_id = lax.broadcasted_iota(jnp.int32, (total, total), 0) // count
    col_id = lax.broadcasted_iota(jnp.int32, (total, total), 1) // count
    apart = jnp.where((row_id >= 2) != (col_id >= 2), edge_ref[0], 0) + jnp.where(
        (row_id % 2) != (col_id % 2), edge_ref[1], 0
    )
    blocked = apart > 0
    for head in range(heads):
        at = slice(head * HDIM, (head + 1) * HDIM)
        query = projected[:, at]
        key = projected[:, inner + head * HDIM : inner + (head + 1) * HDIM]
        value = projected[:, 2 * inner + head * HDIM : 2 * inner + (head + 1) * HDIM]
        grad_head = grad_att[:, at]
        scores = dot(query, key, ((1,), (1,))) * scale
        scores = jnp.where(blocked, -1e30, scores)
        exps = jnp.exp(scores - jnp.max(scores, axis=-1, keepdims=True))
        probs = exps / jnp.sum(exps, axis=-1, keepdims=True)
        low = probs.astype(BF16)
        att[:, at] = dot(low, value, ((1,), (0,))).astype(BF16)
        grad_prob = dot(grad_head, value, ((1,), (1,)))
        inner_sum = jnp.sum(probs * grad_prob, axis=-1, keepdims=True)
        grad_score = probs * (grad_prob - inner_sum)
        score_low = grad_score.astype(BF16)
        gproj_ref[:, at] = (dot(score_low, key, ((1,), (0,))) * scale).astype(BF16)
        gproj_ref[:, inner + head * HDIM : inner + (head + 1) * HDIM] = (
            dot(score_low, query, ((0,), (0,))) * scale
        ).astype(BF16)
        gproj_ref[:, 2 * inner + head * HDIM : 2 * inner + (head + 1) * HDIM] = dot(
            low, grad_head, ((0,), (0,))
        ).astype(BF16)
    half = keep_ref.shape[0]
    for ref, rows in ((keep_ref, slice(0, half)), (send_ref, slice(half, 2 * half))):
        ref[:, :inner] = dot(turned[rows, :], att[...], ((1,), (0,))).astype(BF16)
        ref[:, inner:] = dot(
            normed_t_ref[rows, :], gproj_ref[:, 2 * inner :], ((1,), (0,))
        ).astype(BF16)
    wide[...] = wide[...] + dot(att[...], w_out_ref[...], ((1,), (0,)))
    for place in range(4):
        y_ref[place] = wide[place * count : (place + 1) * count, :].astype(BF16)


def gradient_body(
    group, order_ref, q0, q1, q2, q3, y_ref, gproj_ref, normed_t_ref, gain_ref, w_qkv_ref,
    keep_ref, send_ref, o0, o1, o2, o3,
    wide, flat, turned,
):
    quads = (q0, q1, q2, q3)
    count = q0.shape[0]
    width = wide.shape[1]
    standard, inverse = normalize(gather_tokens(quads, 0, wide))
    grad_normed = dot(gproj_ref[...], w_qkv_ref[...], ((1,), (1,)))
    sums = [
        jnp.sum(grad_normed * standard, axis=0, keepdims=True),
        jnp.sum(grad_normed, axis=0, keepdims=True),
    ]
    line = lax.broadcasted_iota(jnp.int32, (LANES, width), 0)
    block = jnp.where(line == 0, sums[0], jnp.where(line == 1, sums[1], 0.0))
    flat[...] = block.T
    reorder(order_ref, flat, turned, group)
    grad_hat = grad_normed * gain_ref[...]
    first = jnp.mean(grad_hat, axis=-1, keepdims=True)
    second = jnp.mean(grad_hat * standard, axis=-1, keepdims=True)
    change = (grad_hat - first - standard * second) * inverse
    wide[...] = gather_tokens(quads, 1, wide) + change
    for place, out in enumerate((o0, o1, o2, o3)):
        out[:, :width] = y_ref[place]
        out[:, width:] = wide[place * count : (place + 1) * count, :].astype(BF16)
    half, cols = keep_ref.shape
    cols = cols - LANES
    for ref, rows in ((keep_ref, slice(0, half)), (send_ref, slice(half, 2 * half))):
        ref[:, :cols] = dot(normed_t_ref[rows, :], gproj_ref[:, :cols], ((1,), (0,))).astype(BF16)
        ref[:, cols:] = turned[rows, :].astype(BF16)


def unpack_body(q0, q1, q2, q3, y_ref, grad_ref, wide, lines):
    levels, rows, cols, width = y_ref.shape
    half_rows, half_cols = rows // 2, cols // 2
    for part, out in enumerate((y_ref, grad_ref)):
        for quad, (row0, col0) in zip((q0, q1, q2, q3), corners(rows, cols)):
            wide[...] = quad[:, part * width : (part + 1) * width].astype(F32)
            for level in range(levels):
                for row in range(half_rows):
                    at = (level * half_rows + row) * half_cols
                    lines[level, row0 + row, col0 : col0 + half_cols, :] = wide[
                        at : at + half_cols, :
                    ]
        out[...] = lines[...].astype(BF16)


def first_body(keep, got, both, send_a, send_b):
    quarter = send_a.shape[0]
    for out, to, start in (
        (both, 0, 0), (send_a, 0, quarter), (both, quarter, 2 * quarter), (send_b, 0, 3 * quarter),
    ):
        out[to : to + quarter, :] = (
            keep[start : start + quarter, :].astype(F32) + got[start : start + quarter, :].astype(F32)
        ).astype(BF16)


def second_body(keep, got_a, got_b, both, send_a, send_b):
    part = send_a.shape[0]
    for side, (got, send) in enumerate(((got_a, send_a), (got_b, send_b))):
        base = 2 * part * side
        for out, to, start in ((both, part * side, 0), (send, 0, part)):
            out[to : to + part, :] = (
                keep[base + start : base + start + part, :].astype(F32)
                + got[start : start + part, :].astype(F32)
            ).astype(BF16)


def third_body(keep, got_a, got_b, *outs):
    part = got_a.shape[0]
    size = outs[0].shape[0]
    for place, out in enumerate(outs):
        start = place * size
        got = got_a if start < part else got_b
        within = start % part
        out[...] = (
            keep[start : start + size, :].astype(F32) + got[within : within + size, :].astype(F32)
        ).astype(BF16)


def xor_pairs(count, bit):
    return [(i, i ^ bit) for i in range(count)]


def scatter_sum(keep, send, lon_count):
    lat_count = lax.axis_size("lat")
    rows, cols = keep.shape
    got = lax.ppermute(send, "lat", xor_pairs(lat_count, 1))
    quarter = rows // 4
    shape = lambda n: ((n, cols), BF16)
    both, send_a, send_b = call(
        first_body, "sum_first", [shape(2 * quarter), shape(quarter), shape(quarter)], (keep, got)
    )
    got_a = lax.ppermute(send_a, "lat", xor_pairs(lat_count, 2))
    got_b = lax.ppermute(send_b, "lat", xor_pairs(lat_count, 4))
    part = quarter // 2
    both, send_a, send_b = call(
        second_body, "sum_second", [shape(2 * part), shape(part), shape(part)], (both, got_a, got_b)
    )
    got_a = lax.ppermute(send_a, "lat", xor_pairs(lat_count, 4))
    got_b = lax.ppermute(send_b, "lat", xor_pairs(lat_count, 2))
    size = 2 * part // lon_count
    pieces = call(third_body, "sum_third", [shape(size)] * lon_count, (both, got_a, got_b))
    total = pieces[0].astype(F32)
    arrived = [
        lax.ppermute(pieces[k], "lon", [(i, (i + k) % lon_count) for i in range(lon_count)])
        for k in range(1, lon_count)
    ]
    for item in arrived:
        total = total + item.astype(F32)
    return total


def on_device(tokens, layer_norm_gain, layer_norm_bias, w_qkv, w_out, output_cotangent):
    levels, lat_rows, lon_cols, width = tokens.shape
    inner = w_out.shape[0]
    lat_count, lon_count = lax.axis_size("lat"), lax.axis_size("lon")
    lat_place, lon_place = lax.axis_index("lat"), lax.axis_index("lon")
    cells = levels * lat_rows * lon_cols
    count = cells // 4
    norm_factor = 1.0 / math.sqrt(cells * lat_count * lon_count)

    def moved(lat_step, lon_step):
        pairs = []
        for i in range(lat_count):
            for j in range(lon_count):
                to = ((i + lat_step) % lat_count) * lon_count + (j + lon_step) % lon_count
                pairs.append((i * lon_count + j, to))
        return pairs

    steps = ((0, 1), (1, 0), (1, 1))

    own, *sends = call(
        pack_body, "pack", [((count, 2 * width), BF16)] * 4, (tokens, output_cotangent),
        scratch=[pltpu.VMEM((count, width), F32)],
    )
    quads = [own] + [
        lax.ppermute(item, ("lat", "lon"), moved(-a, -b)) for item, (a, b) in zip(sends, steps)
    ]

    share = width // (lat_count * lon_count)
    hyper = lat_count == 8 and lon_count % 2 == 0 and share % 16 == 0
    if hyper:
        group = share
        order = []
        half_lon = lon_count // 2
        for core in range(2):
            for side in range(2):
                for outer in range(2):
                    for nested in range(2):
                        x_bit, y_bit = (outer, nested) if side == 0 else (nested, outer)
                        block = lat_place ^ (core + 2 * x_bit + 4 * y_bit)
                        for k in range(half_lon):
                            step = (lon_place + side * half_lon + k) % lon_count
                            order.append(block * lon_count + step)
        order = jnp.stack(order).astype(jnp.int32)
    else:
        group = 16
        order = jnp.arange(width // group, dtype=jnp.int32)
    edges = jnp.stack([lat_place == lat_count - 1, lon_place == lon_count - 1]).astype(jnp.int32)

    gain_row = layer_norm_gain.reshape(1, width)
    bias_row = layer_norm_bias.reshape(1, width)
    early, early_send, y_part, grad_proj, normed_t = call(
        functools.partial(attention_body, group),
        "attention",
        [
            ((width // 2, 2 * inner), BF16),
            ((width // 2, 2 * inner), BF16),
            ((4, count, width), BF16),
            ((cells, 3 * inner), BF16),
            ((width, cells), BF16),
        ],
        (order, edges, *quads, gain_row, bias_row, w_qkv, w_out),
        scratch=[
            pltpu.VMEM((cells, width), F32),
            pltpu.VMEM((cells, inner), BF16),
            pltpu.VMEM((width, cells), BF16),
            pltpu.VMEM((width, cells), BF16),
        ],
        smem=2,
    )
    late, late_send, *returns = call(
        functools.partial(gradient_body, group),
        "gradient",
        [((width // 2, 2 * inner + LANES), BF16)] * 2 + [((count, 2 * width), BF16)] * 4,
        (order, *quads, y_part, grad_proj, normed_t, gain_row, w_qkv),
        scratch=[
            pltpu.VMEM((cells, width), F32),
            pltpu.VMEM((width, LANES), F32),
            pltpu.VMEM((width, LANES), F32),
        ],
        smem=1,
    )
    if hyper:
        early_total = scatter_sum(early, early_send, lon_count)
        late_total = scatter_sum(late, late_send, lon_count)
    else:
        def natural(a, b):
            whole = jnp.concatenate([a, b], axis=0).astype(F32)
            whole = lax.psum_scatter(whole, "lat", scatter_dimension=0, tiled=True)
            return lax.psum_scatter(whole, "lon", scatter_dimension=0, tiled=True)

        early_total = natural(early, early_send)
        late_total = natural(late, late_send)
    back = [returns[0]] + [
        lax.ppermute(item, ("lat", "lon"), moved(a, b)) for item, (a, b) in zip(returns[1:], steps)
    ]
    y_out, token_gradient = call(
        unpack_body, "unpack", [(tokens.shape, BF16)] * 2, tuple(back),
        scratch=[pltpu.VMEM((count, width), F32), pltpu.VMEM(tokens.shape, F32)],
    )
    early_total = early_total * norm_factor
    late_total = late_total * norm_factor
    d_out = early_total[:, :inner].T
    d_qkv = jnp.concatenate([late_total[:, : 2 * inner], early_total[:, inner:]], axis=1)
    gain_gradient_scaled = late_total[:, 2 * inner]
    d_bias = late_total[:, 2 * inner + 1]
    return (y_out, token_gradient, d_qkv, d_out, gain_gradient_scaled, d_bias)


def solution(mesh):
    in_specs = (P(None, "lat", "lon", None), P(), P(), P(), P(), P(None, "lat", "lon", None))
    out_specs = (
        P(None, "lat", "lon", None),
        P(None, "lat", "lon", None),
        P(("lat", "lon"), None),
        P(None, ("lat", "lon")),
        P(("lat", "lon")),
        P(("lat", "lon")),
    )
    return jax.shard_map(
        on_device, mesh=mesh, in_specs=in_specs, out_specs=out_specs, check_vma=False
    )
```

```python
import functools
import math

import jax
import jax.numpy as jnp
from jax import lax
from jax.experimental import pallas as pl
from jax.experimental.pallas import tpu as pltpu
from jax.sharding import PartitionSpec as P

HDIM = 64
WLAT = 6
WLON = 12
F32 = jnp.float32
BF16 = jnp.bfloat16
LANES = 128

ANY_SPEC = pl.BlockSpec(memory_space=pl.ANY)
VMEM_SPEC = pl.BlockSpec(memory_space=pltpu.VMEM)
SMEM_SPEC = pl.BlockSpec(memory_space=pltpu.SMEM)


def dot(a, b, contract):
    return lax.dot_general(a, b, ((contract[0], contract[1]), ((), ())), preferred_element_type=F32)


def call(body, name, outs, args, scratch=(), smem=0, cost=None):
    specs = [SMEM_SPEC] * smem + [VMEM_SPEC] * (len(args) - smem)
    return pl.pallas_call(
        body,
        name=name,
        out_shape=[jax.ShapeDtypeStruct(s, d) for s, d in outs],
        in_specs=specs,
        out_specs=[VMEM_SPEC] * len(outs),
        scratch_shapes=list(scratch),
        cost_estimate=cost,
    )(*args)


def corners(rows, cols):
    return ((rows // 2, cols // 2), (rows // 2, 0), (0, cols // 2), (0, 0))


def run_copies(copies):
    for item in copies:
        item.start()
    for item in copies:
        item.wait()


def pack_body(tok_ref, cot_ref, *refs):
    outs, sem = refs[:-1], refs[-1]
    rows, cols = tok_ref.shape[:2]
    copies = []
    for out_ref, (row, col) in zip(outs, corners(rows, cols)[1:]):
        for part, ref in enumerate((tok_ref, cot_ref)):
            copies.append(
                pltpu.make_async_copy(
                    ref.at[pl.ds(row, rows // 2), pl.ds(col, cols // 2)],
                    out_ref.at[part],
                    sem.at[len(copies)],
                )
            )
    run_copies(copies)


def unpack_body(q0, q1, q2, q3, y_ref, grad_ref, sem):
    rows, cols = y_ref.shape[:2]
    copies = []
    for quad, (row, col) in zip((q0, q1, q2, q3), corners(rows, cols)):
        for part, ref in enumerate((y_ref, grad_ref)):
            copies.append(
                pltpu.make_async_copy(
                    quad.at[part],
                    ref.at[pl.ds(row, rows // 2), pl.ds(col, cols // 2)],
                    sem.at[len(copies)],
                )
            )
    run_copies(copies)


def move_cells(body, name, outs, args, count):
    return pl.pallas_call(
        body,
        name=name,
        out_shape=[jax.ShapeDtypeStruct(shape, BF16) for shape in outs],
        in_specs=[ANY_SPEC] * len(args),
        out_specs=[ANY_SPEC] * len(outs),
        scratch_shapes=[pltpu.SemaphoreType.DMA((count,))],
    )(*args)


def gather_window(own, received, part, wide):
    rows, cols, levels, width = own.shape
    count = levels * (rows // 2) * (cols // 2)
    pieces = [own[rows // 2 :, cols // 2 :]] + [item[part] for item in received]
    for place, piece in enumerate(pieces):
        wide[place * count : (place + 1) * count, :] = piece.reshape(count, width).astype(F32)
    return wide[...]


def normalize(tokens_wide):
    average = jnp.mean(tokens_wide, axis=-1, keepdims=True)
    centered = tokens_wide - average
    inverse = lax.rsqrt(jnp.mean(centered * centered, axis=-1, keepdims=True) + 1e-05)
    return centered * inverse, inverse


def reorder(order_ref, source, targets, group, base=0):
    half = source.shape[0] // 2
    for place in range(source.shape[0] // group):
        start = pl.multiple_of(order_ref[place] * group, group)
        at = place * group
        target = targets[at // half]
        at = base + at % half
        target[at : at + group, :] = source[pl.ds(start, group), :]


def attention_body(
    group, order_ref, edge_ref, tok_ref, cot_ref, r1, r2, r3, gain_ref, bias_ref, w_qkv_ref,
    w_out_ref, mine_ref, peer_ref, factor_ref, wide, side,
):
    received = (r1, r2, r3)
    inner, width = w_out_ref.shape
    heads = inner // HDIM
    scale = HDIM ** (-0.5)
    grad = gather_window(cot_ref, received, 1, wide).astype(BF16)
    total = grad.shape[0]
    side[...] = grad.T
    reorder(order_ref, side, (mine_ref, peer_ref), group, width // 2)
    standard, _ = normalize(gather_window(tok_ref, received, 0, wide))
    normed = (standard * gain_ref[...] + bias_ref[...]).astype(BF16)
    side[...] = normed.T
    reorder(order_ref, side, (mine_ref, peer_ref), group)
    projected = dot(normed, w_qkv_ref[...], ((1,), (0,))).astype(BF16)
    grad_att = dot(grad, w_out_ref[...], ((1,), (1,))).astype(BF16)
    count = total // 4
    row_id = lax.broadcasted_iota(jnp.int32, (total, total), 0) // count
    col_id = lax.broadcasted_iota(jnp.int32, (total, total), 1) // count
    apart = jnp.where((row_id >= 2) != (col_id >= 2), edge_ref[0], 0) + jnp.where(
        (row_id % 2) != (col_id % 2), edge_ref[1], 0
    )
    blocked = apart > 0
    for head in range(heads):
        at = head * HDIM
        query = projected[:, at : at + HDIM]
        key = projected[:, inner + at : inner + at + HDIM]
        value = projected[:, 2 * inner + at : 2 * inner + at + HDIM]
        grad_head = grad_att[:, at : at + HDIM]
        scores = dot(query, key, ((1,), (1,))) * scale
        scores = jnp.where(blocked, -1e30, scores)
        exps = jnp.exp(scores - jnp.max(scores, axis=-1, keepdims=True))
        probs = exps / jnp.sum(exps, axis=-1, keepdims=True)
        low = probs.astype(BF16)
        factor_ref[:, at : at + HDIM] = dot(low, value, ((1,), (0,))).astype(BF16)
        grad_prob = dot(grad_head, value, ((1,), (1,)))
        inner_sum = jnp.sum(probs * grad_prob, axis=-1, keepdims=True)
        grad_score = (probs * (grad_prob - inner_sum)).astype(BF16)
        factor_ref[:, inner + at : inner + at + HDIM] = dot(low, grad_head, ((0,), (0,))).astype(
            BF16
        )
        factor_ref[:, 2 * inner + at : 2 * inner + at + HDIM] = (
            dot(grad_score, key, ((1,), (0,))) * scale
        ).astype(BF16)
        factor_ref[:, 3 * inner + at : 3 * inner + at + HDIM] = (
            dot(grad_score, query, ((0,), (0,))) * scale
        ).astype(BF16)


def gradient_body(
    group, order_ref, tok_ref, cot_ref, r1, r2, r3, factor_ref, gain_ref, w_qkv_ref, w_out_ref,
    o0, o1, o2, o3, mine_ref, peer_ref, wide, flat,
):
    received = (r1, r2, r3)
    inner, width = w_out_ref.shape
    outs = (o0, o1, o2, o3)
    quad = o0.shape[1:]
    count = quad[0] * quad[1] * quad[2]
    tokens_wide = gather_window(tok_ref, received, 0, wide)
    standard, inverse = normalize(tokens_wide)
    grad_normed = dot(factor_ref[:, inner : 2 * inner], w_qkv_ref[:, 2 * inner :], ((1,), (1,)))
    grad_normed += dot(factor_ref[:, 2 * inner :], w_qkv_ref[:, : 2 * inner], ((1,), (1,)))
    sums = [
        jnp.sum(grad_normed * standard, axis=0, keepdims=True),
        jnp.sum(grad_normed, axis=0, keepdims=True),
    ]
    line = lax.broadcasted_iota(jnp.int32, (LANES, width), 0)
    flat[...] = jnp.where(line == 0, sums[0], jnp.where(line == 1, sums[1], 0.0)).T
    reorder(order_ref, flat, (mine_ref, peer_ref), group)
    wide[...] = tokens_wide + dot(factor_ref[:, :inner], w_out_ref[...], ((1,), (0,)))
    for place, out in enumerate(outs):
        out[0] = wide[place * count : (place + 1) * count, :].astype(BF16).reshape(quad)
    grad_hat = grad_normed * gain_ref[...]
    first = jnp.mean(grad_hat, axis=-1, keepdims=True)
    second = jnp.mean(grad_hat * standard, axis=-1, keepdims=True)
    change = (grad_hat - first - standard * second) * inverse
    wide[...] = gather_window(cot_ref, received, 1, wide) + change
    for place, out in enumerate(outs):
        out[1] = wide[place * count : (place + 1) * count, :].astype(BF16).reshape(quad)


def split_store(value, outs, cols):
    both, send_a, send_b = outs
    quarter = send_a.shape[0]
    for out, to, start in (
        (both, 0, 0), (send_a, 0, quarter), (both, quarter, 2 * quarter), (send_b, 0, 3 * quarter),
    ):
        out[to : to + quarter, cols] = value[start : start + quarter].astype(BF16)


def early_body(mine, got, factor, factor_got, *outs):
    half = mine.shape[0] // 2
    inner = factor.shape[1] // 4
    for part in range(2):
        rows = slice((1 - part) * half, (2 - part) * half)
        cols = slice(part * inner, (part + 1) * inner)
        value = dot(mine[rows, :], factor[:, cols], ((1,), (0,)))
        value += dot(got[rows, :], factor_got[:, cols], ((1,), (0,)))
        split_store(value, outs, cols)


def late_body(mine, got, factor, factor_got, sums, sums_got, *outs):
    half = mine.shape[0] // 2
    inner = factor.shape[1] // 4
    for part in range(2):
        cols = slice((2 + part) * inner, (3 + part) * inner)
        value = dot(mine[:half, :], factor[:, cols], ((1,), (0,)))
        value += dot(got[:half, :], factor_got[:, cols], ((1,), (0,)))
        split_store(value, outs, slice(part * inner, (part + 1) * inner))
    split_store(sums[...] + sums_got[...], outs, slice(2 * inner, 2 * inner + LANES))


def second_body(keep, got_a, got_b, both, send_a, send_b):
    part = send_a.shape[0]
    for side, (got, send) in enumerate(((got_a, send_a), (got_b, send_b))):
        base = 2 * part * side
        for out, to, start in ((both, part * side, 0), (send, 0, part)):
            out[to : to + part, :] = (
                keep[base + start : base + start + part, :].astype(F32)
                + got[start : start + part, :].astype(F32)
            ).astype(BF16)


def third_body(keep, got_a, got_b, *outs):
    part = got_a.shape[0]
    size = outs[0].shape[0]
    for place, out in enumerate(outs):
        start = place * size
        got = got_a if start < part else got_b
        within = start % part
        out[...] = (
            keep[start : start + size, :].astype(F32) + got[within : within + size, :].astype(F32)
        ).astype(BF16)


def xor_pairs(bit):
    return [(i, i ^ bit) for i in range(lax.axis_size("lat"))]


def swap(value, bit):
    return lax.ppermute(value, "lat", xor_pairs(bit))


def scatter_sum(both, send_a, send_b, lon_count):
    quarter, cols = send_a.shape
    shape = lambda n: ((n, cols), BF16)
    got_a, got_b = swap(send_a, 2), swap(send_b, 4)
    part = quarter // 2
    both, send_a, send_b = call(
        second_body, "sum_second", [shape(2 * part), shape(part), shape(part)], (both, got_a, got_b)
    )
    got_a, got_b = swap(send_a, 4), swap(send_b, 2)
    size = 2 * part // lon_count
    pieces = call(third_body, "sum_third", [shape(size)] * lon_count, (both, got_a, got_b))
    total = pieces[0].astype(F32)
    arrived = [
        lax.ppermute(pieces[k], "lon", [(i, (i + k) % lon_count) for i in range(lon_count)])
        for k in range(1, lon_count)
    ]
    for item in arrived:
        total = total + item.astype(F32)
    return total


def on_device(tokens, layer_norm_gain, layer_norm_bias, w_qkv, w_out, output_cotangent):
    levels, lat_rows, lon_cols, width = tokens.shape
    inner = w_out.shape[0]
    lat_count, lon_count = lax.axis_size("lat"), lax.axis_size("lon")
    lat_place, lon_place = lax.axis_index("lat"), lax.axis_index("lon")
    cells = levels * lat_rows * lon_cols
    norm_factor = 1.0 / math.sqrt(cells * lat_count * lon_count)

    def moved(lat_step, lon_step):
        pairs = []
        for i in range(lat_count):
            for j in range(lon_count):
                to = ((i + lat_step) % lat_count) * lon_count + (j + lon_step) % lon_count
                pairs.append((i * lon_count + j, to))
        return pairs

    steps = ((0, 1), (1, 0), (1, 1))
    grid = (lat_rows, lon_cols, levels, width)
    quad = (2, lat_rows // 2, lon_cols // 2, levels, width)
    tok = tokens.transpose(1, 2, 0, 3)
    cot = output_cotangent.transpose(1, 2, 0, 3)
    sends = move_cells(pack_body, "pack", [quad] * 3, (tok, cot), 6)
    received = [
        lax.ppermute(item, ("lat", "lon"), moved(-a, -b)) for item, (a, b) in zip(sends, steps)
    ]

    share = width // (lat_count * lon_count)
    hyper = lat_count == 8 and lon_count % 2 == 0 and share % 16 == 0
    if hyper:
        group = share
        order = []
        half_lon = lon_count // 2
        for core in range(2):
            for side in range(2):
                for outer in range(2):
                    for nested in range(2):
                        x_bit, y_bit = (outer, nested) if side == 0 else (nested, outer)
                        for k in range(half_lon):
                            order.append((core + 2 * x_bit + 4 * y_bit, side * half_lon + k))
        flips = jnp.array([item[0] for item in order], jnp.int32)
        turns = jnp.array([item[1] for item in order], jnp.int32)
        order = (lat_place ^ flips) * lon_count + (lon_place + turns) % lon_count
    else:
        group = 16
        order = jnp.arange(width // group, dtype=jnp.int32)
    ends = jnp.array([lat_count - 1, lon_count - 1], jnp.int32)
    edges = (jnp.array([1, 0]) * lat_place + jnp.array([0, 1]) * lon_place == ends).astype(jnp.int32)

    gain_row = layer_norm_gain.reshape(1, width)
    bias_row = layer_norm_bias.reshape(1, width)
    mine, peer, factor = call(
        functools.partial(attention_body, group),
        "attention",
        [((width, cells), BF16)] * 2 + [((cells, 4 * inner), BF16)],
        (order, edges, tok, cot, *received, gain_row, bias_row, w_qkv, w_out),
        scratch=[pltpu.VMEM((cells, width), F32), pltpu.VMEM((width, cells), BF16)],
        smem=2,
    )
    q0, q1, q2, q3, sums, sums_peer = call(
        functools.partial(gradient_body, group),
        "gradient",
        [(quad, BF16)] * 4 + [((width // 2, LANES), F32)] * 2,
        (order, tok, cot, *received, factor, gain_row, w_qkv, w_out),
        scratch=[pltpu.VMEM((cells, width), F32), pltpu.VMEM((width, LANES), F32)],
        smem=1,
    )
    if hyper:
        got, factor_got, sums_got = swap(peer, 1), swap(factor, 1), swap(sums_peer, 1)
        quarter = width // 8

        def shapes(cols):
            return [((rows, cols), BF16) for rows in (2 * quarter, quarter, quarter)]

        early = call(early_body, "early", shapes(2 * inner), (mine, got, factor, factor_got))
        late = call(
            late_body, "late", shapes(2 * inner + LANES),
            (mine, got, factor, factor_got, sums, sums_got),
        )
        early_total = scatter_sum(*early, lon_count)
        late_total = scatter_sum(*late, lon_count)
    else:
        half = width // 2
        normed_t = jnp.concatenate([mine[:half], peer[:half]], axis=0)
        cot_t = jnp.concatenate([mine[half:], peer[half:]], axis=0)
        whole = jnp.concatenate(
            [
                dot(cot_t, factor[:, :inner], ((1,), (0,))),
                dot(normed_t, factor[:, inner:], ((1,), (0,))),
                jnp.concatenate([sums, sums_peer], axis=0),
            ],
            axis=1,
        )
        whole = lax.psum_scatter(whole, "lat", scatter_dimension=0, tiled=True)
        whole = lax.psum_scatter(whole, "lon", scatter_dimension=0, tiled=True)
        early_total, late_total = whole[:, : 2 * inner], whole[:, 2 * inner :]
    back = [q0] + [
        lax.ppermute(item, ("lat", "lon"), moved(a, b)) for item, (a, b) in zip((q1, q2, q3), steps)
    ]
    y_out, token_gradient = move_cells(unpack_body, "unpack", [grid] * 2, back, 8)
    early_total = early_total * norm_factor
    late_total = late_total * norm_factor
    d_out = early_total[:, :inner].T
    d_qkv = jnp.concatenate([late_total[:, : 2 * inner], early_total[:, inner:]], axis=1)
    gain_gradient_scaled = late_total[:, 2 * inner]
    d_bias = late_total[:, 2 * inner + 1]
    return (
        y_out.transpose(2, 0, 1, 3),
        token_gradient.transpose(2, 0, 1, 3),
        d_qkv,
        d_out,
        gain_gradient_scaled,
        d_bias,
    )


def solution(mesh):
    in_specs = (P(None, "lat", "lon", None), P(), P(), P(), P(), P(None, "lat", "lon", None))
    out_specs = (
        P(None, "lat", "lon", None),
        P(None, "lat", "lon", None),
        P(("lat", "lon"), None),
        P(None, ("lat", "lon")),
        P(("lat", "lon")),
        P(("lat", "lon")),
    )
    return jax.shard_map(
        on_device, mesh=mesh, in_specs=in_specs, out_specs=out_specs, check_vma=False
    )
```

```python
import functools
import math

import jax
import jax.numpy as jnp
from jax import lax
from jax.experimental import pallas as pl
from jax.experimental.pallas import tpu as pltpu
from jax.sharding import PartitionSpec as P

HDIM = 64
WLAT = 6
WLON = 12
F32 = jnp.float32
BF16 = jnp.bfloat16
LANES = 128

VMEM_SPEC = pl.BlockSpec(memory_space=pltpu.VMEM)
SMEM_SPEC = pl.BlockSpec(memory_space=pltpu.SMEM)


def dot(a, b, contract):
    return lax.dot_general(a, b, ((contract[0], contract[1]), ((), ())), preferred_element_type=F32)


def size_of(shape, dtype):
    rows = 16 if len(shape) > 1 and shape[-2] > 2 else shape[-2] if len(shape) > 1 else 1
    padded = [*shape[:-2], -(-shape[-2] // rows) * rows] if len(shape) > 1 else []
    return math.prod([*padded, -(-shape[-1] // LANES) * LANES]) * jnp.dtype(dtype).itemsize


def call(body, name, outs, args, scratch=(), smem=0, near_in=None, near_out=None, room=4):
    near_in = len(args) - smem if near_in is None else near_in
    near_out = len(outs) if near_out is None else near_out
    far = len(args) - near_in
    held = sum(size_of(a.shape, a.dtype) for a in args[smem:far])
    held += sum(size_of(s, d) for s, d in outs[near_out:])
    held += sum(size_of(m.shape, m.dtype) for m in scratch)
    args = [
        a if i < far else pltpu.with_memory_space_constraint(a, pltpu.VMEM)
        for i, a in enumerate(args)
    ]
    return pl.pallas_call(
        body,
        name=name,
        out_shape=[
            pltpu.VMEM(s, d) if i < near_out else jax.ShapeDtypeStruct(s, d)
            for i, (s, d) in enumerate(outs)
        ],
        in_specs=[SMEM_SPEC] * smem + [VMEM_SPEC] * (len(args) - smem),
        out_specs=[VMEM_SPEC] * len(outs),
        scratch_shapes=list(scratch),
        compiler_params=pltpu.CompilerParams(vmem_limit_bytes=held + room * 2**20),
    )(*args)


def corners(rows, cols):
    return ((rows // 2, cols // 2), (rows // 2, 0), (0, cols // 2), (0, 0))


def pack_body(tok_ref, cot_ref, *outs):
    rows, cols = tok_ref.shape[:2]
    for out_ref, (row, col) in zip(outs, corners(rows, cols)[1:]):
        for part, ref in enumerate((tok_ref, cot_ref)):
            out_ref[part] = ref[row : row + rows // 2, col : col + cols // 2]


def unpack_body(q0, q1, q2, q3, y_ref, grad_ref):
    rows, cols = y_ref.shape[:2]
    for quad, (row, col) in zip((q0, q1, q2, q3), corners(rows, cols)):
        for part, ref in enumerate((y_ref, grad_ref)):
            ref[row : row + rows // 2, col : col + cols // 2] = quad[part]


def gather_window(own, received, part, wide):
    rows, cols, levels, width = own.shape
    count = levels * (rows // 2) * (cols // 2)
    pieces = [own[rows // 2 :, cols // 2 :]] + [item[part] for item in received]
    for place, piece in enumerate(pieces):
        wide[place * count : (place + 1) * count, :] = piece.reshape(count, width).astype(F32)
    return wide[...]


def normalize(tokens_wide):
    average = jnp.mean(tokens_wide, axis=-1, keepdims=True)
    centered = tokens_wide - average
    inverse = lax.rsqrt(jnp.mean(centered * centered, axis=-1, keepdims=True) + 1e-05)
    return centered * inverse, inverse


def reorder(order_ref, source, targets, group, base=0):
    half = source.shape[0] // 2
    for place in range(source.shape[0] // group):
        start = pl.multiple_of(order_ref[place] * group, group)
        at = place * group
        target = targets[at // half]
        at = base + at % half
        target[at : at + group, :] = source[pl.ds(start, group), :]


def attention_body(
    group, order_ref, edge_ref, tok_ref, cot_ref, r1, r2, r3, gain_ref, bias_ref, w_qkv_ref,
    w_out_ref, mine_ref, peer_ref, factor_ref, wide, side,
):
    received = (r1, r2, r3)
    inner, width = w_out_ref.shape
    heads = inner // HDIM
    scale = HDIM ** (-0.5)
    grad = gather_window(cot_ref, received, 1, wide).astype(BF16)
    total = grad.shape[0]
    side[...] = grad.T
    reorder(order_ref, side, (mine_ref, peer_ref), group, width // 2)
    standard, _ = normalize(gather_window(tok_ref, received, 0, wide))
    normed = (standard * gain_ref[...] + bias_ref[...]).astype(BF16)
    side[...] = normed.T
    reorder(order_ref, side, (mine_ref, peer_ref), group)
    projected = dot(normed, w_qkv_ref[...], ((1,), (0,))).astype(BF16)
    grad_att = dot(grad, w_out_ref[...], ((1,), (1,))).astype(BF16)
    count = total // 4
    row_id = lax.broadcasted_iota(jnp.int32, (total, total), 0) // count
    col_id = lax.broadcasted_iota(jnp.int32, (total, total), 1) // count
    apart = jnp.where((row_id >= 2) != (col_id >= 2), edge_ref[0], 0) + jnp.where(
        (row_id % 2) != (col_id % 2), edge_ref[1], 0
    )
    blocked = apart > 0
    for head in range(heads):
        at = head * HDIM
        query = projected[:, at : at + HDIM]
        key = projected[:, inner + at : inner + at + HDIM]
        value = projected[:, 2 * inner + at : 2 * inner + at + HDIM]
        grad_head = grad_att[:, at : at + HDIM]
        scores = dot(query, key, ((1,), (1,))) * scale
        scores = jnp.where(blocked, -1e30, scores)
        exps = jnp.exp(scores - jnp.max(scores, axis=-1, keepdims=True))
        probs = exps / jnp.sum(exps, axis=-1, keepdims=True)
        low = probs.astype(BF16)
        factor_ref[:, at : at + HDIM] = dot(low, value, ((1,), (0,))).astype(BF16)
        grad_prob = dot(grad_head, value, ((1,), (1,)))
        inner_sum = jnp.sum(probs * grad_prob, axis=-1, keepdims=True)
        grad_score = (probs * (grad_prob - inner_sum)).astype(BF16)
        factor_ref[:, inner + at : inner + at + HDIM] = dot(low, grad_head, ((0,), (0,))).astype(
            BF16
        )
        factor_ref[:, 2 * inner + at : 2 * inner + at + HDIM] = (
            dot(grad_score, key, ((1,), (0,))) * scale
        ).astype(BF16)
        factor_ref[:, 3 * inner + at : 3 * inner + at + HDIM] = (
            dot(grad_score, query, ((0,), (0,))) * scale
        ).astype(BF16)


def gradient_body(
    group, order_ref, tok_ref, cot_ref, r1, r2, r3, factor_ref, gain_ref, w_qkv_ref, w_out_ref,
    o0, o1, o2, o3, mine_ref, peer_ref, wide, flat,
):
    received = (r1, r2, r3)
    inner, width = w_out_ref.shape
    outs = (o0, o1, o2, o3)
    quad = o0.shape[1:]
    count = quad[0] * quad[1] * quad[2]
    tokens_wide = gather_window(tok_ref, received, 0, wide)
    standard, inverse = normalize(tokens_wide)
    grad_normed = dot(factor_ref[:, inner : 2 * inner], w_qkv_ref[:, 2 * inner :], ((1,), (1,)))
    grad_normed += dot(factor_ref[:, 2 * inner :], w_qkv_ref[:, : 2 * inner], ((1,), (1,)))
    sums = [
        jnp.sum(grad_normed * standard, axis=0, keepdims=True),
        jnp.sum(grad_normed, axis=0, keepdims=True),
    ]
    line = lax.broadcasted_iota(jnp.int32, (LANES, width), 0)
    flat[...] = jnp.where(line == 0, sums[0], jnp.where(line == 1, sums[1], 0.0)).T
    reorder(order_ref, flat, (mine_ref, peer_ref), group)
    wide[...] = tokens_wide + dot(factor_ref[:, :inner], w_out_ref[...], ((1,), (0,)))
    for place, out in enumerate(outs):
        out[0] = wide[place * count : (place + 1) * count, :].astype(BF16).reshape(quad)
    grad_hat = grad_normed * gain_ref[...]
    first = jnp.mean(grad_hat, axis=-1, keepdims=True)
    second = jnp.mean(grad_hat * standard, axis=-1, keepdims=True)
    change = (grad_hat - first - standard * second) * inverse
    wide[...] = gather_window(cot_ref, received, 1, wide) + change
    for place, out in enumerate(outs):
        out[1] = wide[place * count : (place + 1) * count, :].astype(BF16).reshape(quad)


def split_store(value, outs, cols):
    both, send_a, send_b = outs
    quarter = send_a.shape[0]
    for out, to, start in (
        (both, 0, 0), (send_a, 0, quarter), (both, quarter, 2 * quarter), (send_b, 0, 3 * quarter),
    ):
        out[to : to + quarter, cols] = value[start : start + quarter].astype(BF16)


def early_body(mine, got, factor, factor_got, *outs):
    half = mine.shape[0] // 2
    inner = factor.shape[1] // 4
    for part in range(2):
        rows = slice((1 - part) * half, (2 - part) * half)
        cols = slice(part * inner, (part + 1) * inner)
        value = dot(mine[rows, :], factor[:, cols], ((1,), (0,)))
        value += dot(got[rows, :], factor_got[:, cols], ((1,), (0,)))
        split_store(value, outs, cols)


def late_body(mine, got, factor, factor_got, sums, sums_got, *outs):
    half = mine.shape[0] // 2
    inner = factor.shape[1] // 4
    for part in range(2):
        cols = slice((2 + part) * inner, (3 + part) * inner)
        value = dot(mine[:half, :], factor[:, cols], ((1,), (0,)))
        value += dot(got[:half, :], factor_got[:, cols], ((1,), (0,)))
        split_store(value, outs, slice(part * inner, (part + 1) * inner))
    split_store(sums[...] + sums_got[...], outs, slice(2 * inner, 2 * inner + LANES))


def second_body(keep, got_a, got_b, both, send_a, send_b):
    part = send_a.shape[0]
    for side, (got, send) in enumerate(((got_a, send_a), (got_b, send_b))):
        base = 2 * part * side
        for out, to, start in ((both, part * side, 0), (send, 0, part)):
            out[to : to + part, :] = (
                keep[base + start : base + start + part, :].astype(F32)
                + got[start : start + part, :].astype(F32)
            ).astype(BF16)


def third_body(keep, got_a, got_b, *outs):
    part = got_a.shape[0]
    size = outs[0].shape[0]
    for place, out in enumerate(outs):
        start = place * size
        got = got_a if start < part else got_b
        within = start % part
        out[...] = (
            keep[start : start + size, :].astype(F32) + got[within : within + size, :].astype(F32)
        ).astype(BF16)


def xor_pairs(bit):
    return [(i, i ^ bit) for i in range(lax.axis_size("lat"))]


def swap(value, bit):
    return lax.ppermute(value, "lat", xor_pairs(bit))


def scatter_sum(both, send_a, send_b, lon_count):
    quarter, cols = send_a.shape
    shape = lambda n: ((n, cols), BF16)
    got_a, got_b = swap(send_a, 2), swap(send_b, 4)
    part = quarter // 2
    both, send_a, send_b = call(
        second_body, "sum_second", [shape(2 * part), shape(part), shape(part)], (both, got_a, got_b)
    )
    got_a, got_b = swap(send_a, 4), swap(send_b, 2)
    size = 2 * part // lon_count
    pieces = call(third_body, "sum_third", [shape(size)] * lon_count, (both, got_a, got_b))
    total = pieces[0].astype(F32)
    arrived = [
        lax.ppermute(pieces[k], "lon", [(i, (i + k) % lon_count) for i in range(lon_count)])
        for k in range(1, lon_count)
    ]
    for item in arrived:
        total = total + item.astype(F32)
    return total


def on_device(tokens, layer_norm_gain, layer_norm_bias, w_qkv, w_out, output_cotangent):
    levels, lat_rows, lon_cols, width = tokens.shape
    inner = w_out.shape[0]
    lat_count, lon_count = lax.axis_size("lat"), lax.axis_size("lon")
    lat_place, lon_place = lax.axis_index("lat"), lax.axis_index("lon")
    cells = levels * lat_rows * lon_cols
    norm_factor = 1.0 / math.sqrt(cells * lat_count * lon_count)

    def moved(lat_step, lon_step):
        pairs = []
        for i in range(lat_count):
            for j in range(lon_count):
                to = ((i + lat_step) % lat_count) * lon_count + (j + lon_step) % lon_count
                pairs.append((i * lon_count + j, to))
        return pairs

    steps = ((0, 1), (1, 0), (1, 1))
    grid = (lat_rows, lon_cols, levels, width)
    quad = (2, lat_rows // 2, lon_cols // 2, levels, width)
    tok = tokens.transpose(1, 2, 0, 3)
    cot = output_cotangent.transpose(1, 2, 0, 3)
    sends = call(pack_body, "pack", [(quad, BF16)] * 3, (tok, cot), near_in=0)
    received = [
        lax.ppermute(item, ("lat", "lon"), moved(-a, -b)) for item, (a, b) in zip(sends, steps)
    ]

    share = width // (lat_count * lon_count)
    hyper = lat_count == 8 and lon_count % 2 == 0 and share % 16 == 0
    if hyper:
        group = share
        order = []
        half_lon = lon_count // 2
        for core in range(2):
            for side in range(2):
                for outer in range(2):
                    for nested in range(2):
                        x_bit, y_bit = (outer, nested) if side == 0 else (nested, outer)
                        for k in range(half_lon):
                            order.append((core + 2 * x_bit + 4 * y_bit, side * half_lon + k))
        flips = jnp.array([item[0] for item in order], jnp.int32)
        turns = jnp.array([item[1] for item in order], jnp.int32)
        order = (lat_place ^ flips) * lon_count + (lon_place + turns) % lon_count
    else:
        group = 16
        order = jnp.arange(width // group, dtype=jnp.int32)
    ends = jnp.array([lat_count - 1, lon_count - 1], jnp.int32)
    edges = (jnp.array([1, 0]) * lat_place + jnp.array([0, 1]) * lon_place == ends).astype(jnp.int32)

    gain_row = layer_norm_gain.reshape(1, width)
    bias_row = layer_norm_bias.reshape(1, width)
    mine, peer, factor = call(
        functools.partial(attention_body, group),
        "attention",
        [((width, cells), BF16)] * 2 + [((cells, 4 * inner), BF16)],
        (order, edges, tok, cot, *received, gain_row, bias_row, w_qkv, w_out),
        scratch=[pltpu.VMEM((cells, width), F32), pltpu.VMEM((width, cells), BF16)],
        smem=2,
    )
    q0, q1, q2, q3, sums, sums_peer = call(
        functools.partial(gradient_body, group),
        "gradient",
        [(quad, BF16)] * 4 + [((width // 2, LANES), F32)] * 2,
        (order, tok, cot, *received, factor, gain_row, w_qkv, w_out),
        scratch=[pltpu.VMEM((cells, width), F32), pltpu.VMEM((width, LANES), F32)],
        smem=1,
    )
    if hyper:
        got, factor_got, sums_got = swap(peer, 1), swap(factor, 1), swap(sums_peer, 1)
        quarter = width // 8

        def shapes(cols):
            return [((rows, cols), BF16) for rows in (2 * quarter, quarter, quarter)]

        early = call(early_body, "early", shapes(2 * inner), (mine, got, factor, factor_got))
        late = call(
            late_body, "late", shapes(2 * inner + LANES),
            (mine, got, factor, factor_got, sums, sums_got),
        )
        early_total = scatter_sum(*early, lon_count)
        late_total = scatter_sum(*late, lon_count)
    else:
        half = width // 2
        normed_t = jnp.concatenate([mine[:half], peer[:half]], axis=0)
        cot_t = jnp.concatenate([mine[half:], peer[half:]], axis=0)
        whole = jnp.concatenate(
            [
                dot(cot_t, factor[:, :inner], ((1,), (0,))),
                dot(normed_t, factor[:, inner:], ((1,), (0,))),
                jnp.concatenate([sums, sums_peer], axis=0),
            ],
            axis=1,
        )
        whole = lax.psum_scatter(whole, "lat", scatter_dimension=0, tiled=True)
        whole = lax.psum_scatter(whole, "lon", scatter_dimension=0, tiled=True)
        early_total, late_total = whole[:, : 2 * inner], whole[:, 2 * inner :]
    back = [q0] + [
        lax.ppermute(item, ("lat", "lon"), moved(a, b)) for item, (a, b) in zip((q1, q2, q3), steps)
    ]
    y_out, token_gradient = call(unpack_body, "unpack", [(grid, BF16)] * 2, back, near_out=0)
    early_total = early_total * norm_factor
    late_total = late_total * norm_factor
    d_out = early_total[:, :inner].T
    d_qkv = jnp.concatenate([late_total[:, : 2 * inner], early_total[:, inner:]], axis=1)
    gain_gradient_scaled = late_total[:, 2 * inner]
    d_bias = late_total[:, 2 * inner + 1]
    return (
        y_out.transpose(2, 0, 1, 3),
        token_gradient.transpose(2, 0, 1, 3),
        d_qkv,
        d_out,
        gain_gradient_scaled,
        d_bias,
    )


def solution(mesh):
    in_specs = (P(None, "lat", "lon", None), P(), P(), P(), P(), P(None, "lat", "lon", None))
    out_specs = (
        P(None, "lat", "lon", None),
        P(None, "lat", "lon", None),
        P(("lat", "lon"), None),
        P(None, ("lat", "lon")),
        P(("lat", "lon")),
        P(("lat", "lon")),
    )
    return jax.shard_map(
        on_device, mesh=mesh, in_specs=in_specs, out_specs=out_specs, check_vma=False
    )
```

```python
import functools
import itertools
import math

import jax
import jax.numpy as jnp
from jax import lax
from jax.experimental import pallas as pl
from jax.experimental.pallas import tpu as pltpu
from jax.sharding import PartitionSpec as P


HDIM = 64
F32 = jnp.float32
BF16 = jnp.bfloat16
LANES = 128

HBM_SPEC = pl.BlockSpec(memory_space=pltpu.HBM)

VMEM_SPEC = pl.BlockSpec(memory_space=pltpu.VMEM)
SMEM_SPEC = pl.BlockSpec(memory_space=pltpu.SMEM)


def dot(a, b, contract):
    return lax.dot_general(a, b, ((contract[0], contract[1]), ((), ())), preferred_element_type=F32)


def size_of(shape, dtype):
    rows = 16 if len(shape) > 1 and shape[-2] > 2 else shape[-2] if len(shape) > 1 else 1
    padded = [*shape[:-2], -(-shape[-2] // rows) * rows] if len(shape) > 1 else []
    return math.prod([*padded, -(-shape[-1] // LANES) * LANES]) * jnp.dtype(dtype).itemsize


def call(body, outs, args, scratch=(), smem=0, far=0, near_out=None, room=4):
    near_out = len(outs) if near_out is None else near_out
    near_at = smem + far
    held = sum(size_of(s, d) for s, d in outs[near_out:])
    held += sum(size_of(m.shape, m.dtype) for m in scratch if m.dtype in (F32, BF16))
    spaces = [None] * smem + [pltpu.HBM] * far + [pltpu.VMEM] * (len(args) - near_at)
    args = [
        a if space is None else pltpu.with_memory_space_constraint(a, space)
        for a, space in zip(args, spaces)
    ]
    return pl.pallas_call(
        body,
        out_shape=[
            pltpu.VMEM(s, d) if i < near_out else jax.ShapeDtypeStruct(s, d)
            for i, (s, d) in enumerate(outs)
        ],
        in_specs=[SMEM_SPEC] * smem + [HBM_SPEC] * far + [VMEM_SPEC] * (len(args) - near_at),
        out_specs=[VMEM_SPEC] * len(outs),
        scratch_shapes=list(scratch),
        compiler_params=pltpu.CompilerParams(vmem_limit_bytes=held + room * 2**20),
    )(*args)


def corners(rows, cols):
    return ((rows // 2, cols // 2), (rows // 2, 0), (0, cols // 2), (0, 0))


def run_copies(pairs, sem):
    copies = [
        pltpu.make_async_copy(source, target, sem.at[place])
        for place, (source, target) in enumerate(pairs)
    ]
    for item in copies:
        item.start()
    for item in copies:
        item.wait()


def pack_body(tok_ref, cot_ref, *refs):
    outs, sem = refs[:-1], refs[-1]
    rows, cols = tok_ref.shape[:2]
    pairs = []
    for out_ref, (row, col) in zip(outs, corners(rows, cols)):
        for part, ref in enumerate((tok_ref, cot_ref)):
            source = ref.at[pl.ds(row, rows // 2), pl.ds(col, cols // 2)]
            pairs.append((source, out_ref.at[part]))
    run_copies(pairs, sem)


def fetch_body(*refs):
    count = len(refs) // 2
    run_copies(list(zip(refs[:count], refs[count:-1])), refs[-1])


def unpack_body(q0, q1, q2, q3, y_ref, grad_ref):
    rows, cols = y_ref.shape[:2]
    for quad, (row, col) in zip((q0, q1, q2, q3), corners(rows, cols)):
        for part, ref in enumerate((y_ref, grad_ref)):
            ref[row : row + rows // 2, col : col + cols // 2] = quad[part]


def gather_window(quads, part, wide):
    levels, width = quads[0].shape[-2:]
    count = levels * quads[0].shape[1] * quads[0].shape[2]
    for place, item in enumerate(quads):
        wide[place * count : (place + 1) * count, :] = (
            item[part].reshape(count, width).astype(F32)
        )
    return wide[...]


def normalize(tokens_wide):
    average = jnp.mean(tokens_wide, axis=-1, keepdims=True)
    centered = tokens_wide - average
    inverse = lax.rsqrt(jnp.mean(centered * centered, axis=-1, keepdims=True) + 1e-05)
    return centered * inverse, inverse


def reorder(plan, places_ref, source, targets, base=0):
    group, counts, steps = plan
    half = source.shape[0] // 2
    for place in range(source.shape[0] // group):
        start = place * group
        if steps:
            block = places_ref[0] ^ steps[place][0]
            turned = lax.rem(places_ref[1] + steps[place][1], counts[1])
            start = pl.multiple_of((block * counts[1] + turned) * group, group)
        at = place * group
        target = targets[at // half]
        at = base + at % half
        target[at : at + group, :] = source[pl.ds(start, group), :]


def attention_body(
    plan, places_ref, r0, r1, r2, r3, w_qkv_ref, w_out_ref, gain_ref, bias_ref,
    mine_ref, peer_ref, factor_ref, wide, side,
):
    quads = (r0, r1, r2, r3)
    inner, width = w_out_ref.shape
    heads = inner // HDIM
    scale = HDIM ** (-0.5)
    grad = gather_window(quads, 1, wide).astype(BF16)
    total = grad.shape[0]
    side[...] = grad.T
    reorder(plan, places_ref, side, (mine_ref, peer_ref), width // 2)
    standard, _ = normalize(gather_window(quads, 0, wide))
    normed = (standard * gain_ref[...] + bias_ref[...]).astype(BF16)
    side[...] = normed.T
    reorder(plan, places_ref, side, (mine_ref, peer_ref))
    projected = dot(normed, w_qkv_ref[...], ((1,), (0,))).astype(BF16)
    grad_att = dot(grad, w_out_ref[...], ((1,), (1,))).astype(BF16)
    count = total // 4
    row_id = lax.broadcasted_iota(jnp.int32, (total, total), 0) // count
    col_id = lax.broadcasted_iota(jnp.int32, (total, total), 1) // count
    last_lat, last_lon = ((places_ref[i] == n - 1).astype(jnp.int32) for i, n in enumerate(plan[1]))
    apart = jnp.where((row_id >= 2) != (col_id >= 2), last_lat, 0) + jnp.where(
        (row_id % 2) != (col_id % 2), last_lon, 0
    )
    blocked = apart > 0
    for head in range(heads):
        at = head * HDIM
        query = projected[:, at : at + HDIM]
        key = projected[:, inner + at : inner + at + HDIM]
        value = projected[:, 2 * inner + at : 2 * inner + at + HDIM]
        grad_head = grad_att[:, at : at + HDIM]
        scores = dot(query, key, ((1,), (1,))) * scale
        scores = jnp.where(blocked, -1e30, scores)
        exps = jnp.exp(scores - jnp.max(scores, axis=-1, keepdims=True))
        probs = exps / jnp.sum(exps, axis=-1, keepdims=True)
        low = probs.astype(BF16)
        factor_ref[:, at : at + HDIM] = dot(low, value, ((1,), (0,))).astype(BF16)
        grad_prob = dot(grad_head, value, ((1,), (1,)))
        inner_sum = jnp.sum(probs * grad_prob, axis=-1, keepdims=True)
        grad_score = (probs * (grad_prob - inner_sum)).astype(BF16)
        factor_ref[:, inner + at : inner + at + HDIM] = dot(low, grad_head, ((0,), (0,))).astype(
            BF16
        )
        factor_ref[:, 2 * inner + at : 2 * inner + at + HDIM] = (
            dot(grad_score, key, ((1,), (0,))) * scale
        ).astype(BF16)
        factor_ref[:, 3 * inner + at : 3 * inner + at + HDIM] = (
            dot(grad_score, query, ((0,), (0,))) * scale
        ).astype(BF16)


def gradient_body(
    plan, places_ref, r0, r1, r2, r3, factor_ref, w_qkv_ref, w_out_ref, gain_ref,
    o0, o1, o2, o3, mine_ref, peer_ref, wide, flat,
):
    quads = (r0, r1, r2, r3)
    inner, width = w_out_ref.shape
    outs = (o0, o1, o2, o3)
    quad = o0.shape[1:]
    count = quad[0] * quad[1] * quad[2]
    tokens_wide = gather_window(quads, 0, wide)
    standard, inverse = normalize(tokens_wide)
    grad_normed = dot(factor_ref[:, inner : 2 * inner], w_qkv_ref[:, 2 * inner :], ((1,), (1,)))
    grad_normed += dot(factor_ref[:, 2 * inner :], w_qkv_ref[:, : 2 * inner], ((1,), (1,)))
    sums = [
        jnp.sum(grad_normed * standard, axis=0, keepdims=True),
        jnp.sum(grad_normed, axis=0, keepdims=True),
    ]
    line = lax.broadcasted_iota(jnp.int32, (LANES, width), 0)
    flat[...] = jnp.where(line == 0, sums[0], jnp.where(line == 1, sums[1], 0.0)).T
    reorder(plan, places_ref, flat, (mine_ref, peer_ref))
    wide[...] = tokens_wide + dot(factor_ref[:, :inner], w_out_ref[...], ((1,), (0,)))
    for place, out in enumerate(outs):
        out[0] = wide[place * count : (place + 1) * count, :].astype(BF16).reshape(quad)
    grad_hat = grad_normed * gain_ref[...]
    first = jnp.mean(grad_hat, axis=-1, keepdims=True)
    second = jnp.mean(grad_hat * standard, axis=-1, keepdims=True)
    change = (grad_hat - first - standard * second) * inverse
    wide[...] = gather_window(quads, 1, wide) + change
    for place, out in enumerate(outs):
        out[1] = wide[place * count : (place + 1) * count, :].astype(BF16).reshape(quad)


def split_store(value, outs, cols):
    both, send_a, send_b = outs
    quarter = send_a.shape[0]
    for out, to, start in (
        (both, 0, 0), (send_a, 0, quarter), (both, quarter, 2 * quarter), (send_b, 0, 3 * quarter),
    ):
        out[to : to + quarter, cols] = value[start : start + quarter].astype(BF16)


def early_body(mine, got, factor, factor_got, *outs):
    half = mine.shape[0] // 2
    inner = factor.shape[1] // 4
    for part in range(2):
        rows = slice((1 - part) * half, (2 - part) * half)
        cols = slice(part * inner, (part + 1) * inner)
        value = dot(mine[rows, :], factor[:, cols], ((1,), (0,)))
        value += dot(got[rows, :], factor_got[:, cols], ((1,), (0,)))
        split_store(value, outs, cols)


def late_body(mine, got, factor, factor_got, sums, sums_got, *outs):
    half = mine.shape[0] // 2
    inner = factor.shape[1] // 4
    for part in range(2):
        cols = slice((2 + part) * inner, (3 + part) * inner)
        value = dot(mine[:half, :], factor[:, cols], ((1,), (0,)))
        value += dot(got[:half, :], factor_got[:, cols], ((1,), (0,)))
        split_store(value, outs, slice(part * inner, (part + 1) * inner))
    split_store(sums[...] + sums_got[...], outs, slice(2 * inner, 2 * inner + LANES))


def added(*refs):
    total = refs[0].astype(F32)
    for ref in refs[1:]:
        total += ref.astype(F32)
    return total


def second_body(keep, got_a, got_b, both, send_a, send_b):
    part = send_a.shape[0]
    for side, (got, send) in enumerate(((got_a, send_a), (got_b, send_b))):
        at = 2 * part * side
        both[part * side : part * (side + 1), :] = added(
            keep[at : at + part, :], got[:part, :]
        ).astype(BF16)
        send[...] = added(keep[at + part : at + 2 * part, :], got[part:, :]).astype(BF16)


def third_body(keep, got_a, got_b, *outs):
    part = got_a.shape[0]
    size = outs[0].shape[0]
    for place, out in enumerate(outs):
        start = place * size
        got = got_a if start < part else got_b
        within = start % part
        out[...] = added(keep[start : start + size, :], got[within : within + size, :]).astype(BF16)


def turn_body(keep, got_a, got_b, *outs):
    part = got_a.shape[0]
    size = outs[0].shape[0] // 2
    per_side = len(outs) // 2
    for place, out in enumerate(outs):
        got, base = (got_a, 0) if place < per_side else (got_b, part)
        for nested in range(2):
            at = nested * (part // 2) + (place % per_side) * size
            out[nested * size : (nested + 1) * size, :] = added(
                keep[base + at : base + at + size, :], got[at : at + size, :]
            ).astype(BF16)


def meet_body(*refs):
    pieces, (base, send_a, send_b) = refs[:-3], refs[-3:]
    size = base.shape[0]
    per_side = len(pieces) // 2
    base[...] = added(*(item[:size, :] for item in pieces))
    send_a[...] = added(*(item[size:, :] for item in pieces[:per_side])).astype(BF16)
    send_b[...] = added(*(item[size:, :] for item in pieces[per_side:])).astype(BF16)


def early_end_body(factor, base, got_a, got_b, value_ref, out_ref):
    total = added(base[...], got_a[...], got_b[...]) * factor
    inner = out_ref.shape[1]
    out_ref[...] = total[:, :inner]
    value_ref[...] = total[:, inner:]


def late_end_body(factor, value_ref, *refs):
    pieces, (qkv_ref, gain_ref, bias_ref) = refs[:-3], refs[-3:]
    total = added(*(item[...] for item in pieces)) * factor
    cols = total.shape[1] - LANES
    qkv_ref[:, :cols] = total[:, :cols]
    qkv_ref[:, cols:] = value_ref[...]
    rows = total.shape[0]
    flat = jnp.concatenate([total[:, cols:], jnp.zeros((LANES - rows, LANES), F32)], axis=0).T
    gain_ref[...] = flat[0:1, :rows]
    bias_ref[...] = flat[1:2, :rows]


def xor_pairs(bit):
    return [(i, i ^ bit) for i in range(lax.axis_size("lat"))]


def swap(value, bit):
    return lax.ppermute(value, "lat", xor_pairs(bit))


def turn(pieces):
    count = len(pieces)
    return [pieces[0]] + [
        lax.ppermute(pieces[k], "lon", [(i, (i + k) % count) for i in range(count)])
        for k in range(1, count)
    ]


def sum_early(both, send_a, send_b, lon_count, factor):
    quarter, cols = send_a.shape
    size = quarter // lon_count
    got_a, got_b = swap(send_a, 2), swap(send_b, 4)
    pieces = call(turn_body, [((2 * size, cols), BF16)] * lon_count, (both, got_a, got_b))
    pieces = turn(pieces)
    base, send_a, send_b = call(
        meet_body, [((size, cols), F32)] + [((size, cols), BF16)] * 2, pieces
    )
    got_a, got_b = swap(send_a, 4), swap(send_b, 2)
    shape = ((size, cols // 2), F32)
    return call(
        functools.partial(early_end_body, factor), [shape] * 2,
        (base, got_a, got_b), near_out=1,
    )


def sum_late(both, send_a, send_b, value, lon_count, factor):
    quarter, cols = send_a.shape
    part = quarter // 2
    size = 2 * part // lon_count
    got_a, got_b = swap(send_a, 2), swap(send_b, 4)
    both, send_a, send_b = call(
        second_body, [((n * part, cols), BF16) for n in (2, 1, 1)], (both, got_a, got_b)
    )
    got_a, got_b = swap(send_a, 4), swap(send_b, 2)
    pieces = call(third_body, [((size, cols), BF16)] * lon_count, (both, got_a, got_b))
    pieces = turn(pieces)
    return call(
        functools.partial(late_end_body, factor),
        [((size, cols - LANES + value.shape[1]), F32)] + [((1, size), F32)] * 2,
        (value, *pieces), near_out=0,
    )


def device_step(tokens, layer_norm_gain, layer_norm_bias, w_qkv, w_out, output_cotangent):
    levels, lat_rows, lon_cols, width = tokens.shape
    inner = w_out.shape[0]
    lat_count, lon_count = lax.axis_size("lat"), lax.axis_size("lon")
    lat_place, lon_place = lax.axis_index("lat"), lax.axis_index("lon")
    cells = levels * lat_rows * lon_cols
    norm_factor = 1.0 / math.sqrt(cells * lat_count * lon_count)

    def moved(lat_step, lon_step):
        pairs = []
        for i in range(lat_count):
            for j in range(lon_count):
                to = ((i + lat_step) % lat_count) * lon_count + (j + lon_step) % lon_count
                pairs.append((i * lon_count + j, to))
        return pairs

    steps = ((0, 1), (1, 0), (1, 1))
    grid = (lat_rows, lon_cols, levels, width)
    quad = (2, lat_rows // 2, lon_cols // 2, levels, width)
    tok = tokens.transpose(1, 2, 0, 3)
    cot = output_cotangent.transpose(1, 2, 0, 3)
    own, *sends = call(
        pack_body, [(quad, BF16)] * 4, (tok, cot), far=2,
        scratch=[pltpu.SemaphoreType.DMA((8,))],
    )
    quads = [own] + [
        lax.ppermute(item, ("lat", "lon"), moved(-a, -b)) for item, (a, b) in zip(sends, steps)
    ]
    params = (w_qkv, w_out, layer_norm_gain.reshape(1, width), layer_norm_bias.reshape(1, width))
    params = call(
        fetch_body, [(item.shape, item.dtype) for item in params], params, far=4,
        scratch=[pltpu.SemaphoreType.DMA((4,))],
    )

    share = width // (lat_count * lon_count)
    hyper = lat_count == 8 and lon_count % 2 == 0 and share % 16 == 0
    order = []
    if hyper:
        half_lon = lon_count // 2
        for core, side, outer, nested, k in itertools.product(
            range(2), range(2), range(2), range(2), range(half_lon)
        ):
            x_bit, y_bit = (outer, nested) if side == 0 else (nested, outer)
            order.append((core + 2 * x_bit + 4 * y_bit, side * half_lon + k))
    plan = (share if hyper else 16, (lat_count, lon_count), tuple(order))
    places = jnp.where(jnp.arange(2) == 0, lat_place, lon_place).astype(jnp.int32)
    mine, peer, factor = call(
        functools.partial(attention_body, plan),
        [((width, cells), BF16)] * 2 + [((cells, 4 * inner), BF16)],
        (places, *quads, *params),
        scratch=[pltpu.VMEM((cells, width), F32), pltpu.VMEM((width, cells), BF16)],
        smem=1,
    )
    q0, q1, q2, q3, sums, sums_peer = call(
        functools.partial(gradient_body, plan),
        [(quad, BF16)] * 4 + [((width // 2, LANES), F32)] * 2,
        (places, *quads, factor, *params[:3]),
        scratch=[pltpu.VMEM((cells, width), F32), pltpu.VMEM((width, LANES), F32)],
        smem=1,
    )
    if hyper:
        factor_got = swap(factor, 1)
        got = swap(peer, 1)
        sums_got = swap(sums_peer, 1)
        quarter = width // 8

        def shapes(cols):
            return [((rows, cols), BF16) for rows in (2 * quarter, quarter, quarter)]

        early = call(early_body, shapes(2 * inner), (mine, got, factor, factor_got))
        late = call(
            late_body, shapes(2 * inner + LANES),
            (mine, got, factor, factor_got, sums, sums_got),
        )
        value, d_out = sum_early(*early, lon_count, norm_factor)
        d_qkv, gain, bias = sum_late(*late, value, lon_count, norm_factor)
    else:
        half = width // 2
        normed_t = jnp.concatenate([mine[:half], peer[:half]], axis=0)
        cot_t = jnp.concatenate([mine[half:], peer[half:]], axis=0)
        whole = jnp.concatenate(
            [
                dot(cot_t, factor[:, :inner], ((1,), (0,))),
                dot(normed_t, factor[:, inner:], ((1,), (0,))),
                jnp.concatenate([sums, sums_peer], axis=0),
            ],
            axis=1,
        )
        whole = lax.psum_scatter(whole, "lat", scatter_dimension=0, tiled=True)
        whole = lax.psum_scatter(whole, "lon", scatter_dimension=0, tiled=True)
        whole = whole * norm_factor
        d_out = whole[:, :inner]
        d_qkv = jnp.concatenate([whole[:, 2 * inner : 4 * inner], whole[:, inner : 2 * inner]], axis=1)
        gain, bias = whole[:, 4 * inner], whole[:, 4 * inner + 1]
    back = [q0] + [
        lax.ppermute(item, ("lat", "lon"), moved(a, b))
        for item, (a, b) in zip((q1, q2, q3), steps)
    ]
    y_out, token_gradient = call(unpack_body, [(grid, BF16)] * 2, back, near_out=0)
    return (
        y_out.transpose(2, 0, 1, 3),
        token_gradient.transpose(2, 0, 1, 3),
        d_qkv,
        d_out.T,
        gain.reshape(share),
        bias.reshape(share),
    )


def solution(mesh):
    in_specs = (P(None, "lat", "lon", None), P(), P(), P(), P(), P(None, "lat", "lon", None))
    out_specs = (
        P(None, "lat", "lon", None),
        P(None, "lat", "lon", None),
        P(("lat", "lon"), None),
        P(None, ("lat", "lon")),
        P(("lat", "lon")),
        P(("lat", "lon")),
    )
    return jax.shard_map(
        device_step, mesh=mesh, in_specs=in_specs, out_specs=out_specs, check_vma=False
    )
```

```python
import functools
import itertools
import math

import jax
import jax.numpy as jnp
from jax import lax
from jax.experimental import pallas as pl
from jax.experimental.pallas import tpu as pltpu
from jax.sharding import PartitionSpec as P


HDIM = 64
F32 = jnp.float32
BF16 = jnp.bfloat16
LANES = 128

HBM_SPEC = pl.BlockSpec(memory_space=pltpu.HBM)

VMEM_SPEC = pl.BlockSpec(memory_space=pltpu.VMEM)
SMEM_SPEC = pl.BlockSpec(memory_space=pltpu.SMEM)


def dot(a, b, contract):
    return lax.dot_general(a, b, ((contract[0], contract[1]), ((), ())), preferred_element_type=F32)


def size_of(shape, dtype):
    rows = 16 if len(shape) > 1 and shape[-2] > 2 else shape[-2] if len(shape) > 1 else 1
    padded = [*shape[:-2], -(-shape[-2] // rows) * rows] if len(shape) > 1 else []
    return math.prod([*padded, -(-shape[-1] // LANES) * LANES]) * jnp.dtype(dtype).itemsize


def call(body, outs, args, scratch=(), smem=0, far=0, near_out=None, room=4):
    near_out = len(outs) if near_out is None else near_out
    near_at = smem + far
    held = sum(size_of(s, d) for s, d in outs[near_out:])
    held += sum(size_of(m.shape, m.dtype) for m in scratch if m.dtype in (F32, BF16))
    spaces = [None] * smem + [pltpu.HBM] * far + [pltpu.VMEM] * (len(args) - near_at)
    args = [
        a if space is None else pltpu.with_memory_space_constraint(a, space)
        for a, space in zip(args, spaces)
    ]
    return pl.pallas_call(
        body,
        out_shape=[
            pltpu.VMEM(s, d) if i < near_out else jax.ShapeDtypeStruct(s, d)
            for i, (s, d) in enumerate(outs)
        ],
        in_specs=[SMEM_SPEC] * smem + [HBM_SPEC] * far + [VMEM_SPEC] * (len(args) - near_at),
        out_specs=[VMEM_SPEC] * len(outs),
        scratch_shapes=list(scratch),
        compiler_params=pltpu.CompilerParams(vmem_limit_bytes=held + room * 2**20),
    )(*args)


def corners(rows, cols):
    return ((rows // 2, cols // 2), (rows // 2, 0), (0, cols // 2), (0, 0))


def run_copies(pairs, sem):
    copies = [
        pltpu.make_async_copy(source, target, sem.at[place])
        for place, (source, target) in enumerate(pairs)
    ]
    for item in copies:
        item.start()
    for item in copies:
        item.wait()


def pack_body(tok_ref, cot_ref, *refs):
    outs, sem = refs[:-1], refs[-1]
    rows, cols = tok_ref.shape[:2]
    pairs = []
    for out_ref, (row, col) in zip(outs, corners(rows, cols)):
        for part, ref in enumerate((tok_ref, cot_ref)):
            source = ref.at[pl.ds(row, rows // 2), pl.ds(col, cols // 2)]
            pairs.append((source, out_ref.at[part]))
    run_copies(pairs, sem)


def fetch_body(*refs):
    count = len(refs) // 2
    run_copies(list(zip(refs[:count], refs[count:-1])), refs[-1])


def unpack_body(q0, q1, q2, q3, y_ref, grad_ref):
    rows, cols = y_ref.shape[:2]
    for quad, (row, col) in zip((q0, q1, q2, q3), corners(rows, cols)):
        for part, ref in enumerate((y_ref, grad_ref)):
            ref[row : row + rows // 2, col : col + cols // 2] = quad[part]


def gather_window(quads, part, wide):
    levels, width = quads[0].shape[-2:]
    count = levels * quads[0].shape[1] * quads[0].shape[2]
    for place, item in enumerate(quads):
        wide[place * count : (place + 1) * count, :] = (
            item[part].reshape(count, width).astype(F32)
        )
    return wide[...]


def normalize(tokens_wide):
    average = jnp.mean(tokens_wide, axis=-1, keepdims=True)
    centered = tokens_wide - average
    inverse = lax.rsqrt(jnp.mean(centered * centered, axis=-1, keepdims=True) + 1e-05)
    return centered * inverse, inverse


def reorder(plan, places_ref, source, targets, base=0):
    group, counts, steps = plan
    half = source.shape[0] // 2
    for place in range(source.shape[0] // group):
        start = place * group
        if steps:
            block = places_ref[0] ^ steps[place][0]
            turned = lax.rem(places_ref[1] + steps[place][1], counts[1])
            start = pl.multiple_of((block * counts[1] + turned) * group, group)
        at = place * group
        target = targets[at // half]
        at = base + at % half
        target[at : at + group, :] = source[pl.ds(start, group), :]


def pair_tools(total):
    lane = lax.broadcasted_iota(jnp.int32, (total, LANES), 1)
    first = lane < HDIM

    def alone(value, head):
        return jnp.where(first if head == 0 else ~first, value, jnp.zeros_like(value))

    def pick(results):
        return jnp.where(first, results[0], results[1])

    return alone, pick


def forward_body(
    plan, places_ref, r0, r1, r2, r3, w_qkv_ref, w_out_ref, gain_ref, bias_ref,
    mine_ref, peer_ref, factor_ref, query_ref, pair_ref, probs_ref, wide, side, bias_of,
):
    quads = (r0, r1, r2, r3)
    inner, width = w_out_ref.shape
    grad = gather_window(quads, 1, wide).astype(BF16)
    total = grad.shape[0]
    count = total // 4
    row_id = lax.broadcasted_iota(jnp.int32, (total, total), 0) // count
    col_id = lax.broadcasted_iota(jnp.int32, (total, total), 1) // count
    last_lat, last_lon = ((places_ref[i] == n - 1).astype(jnp.int32) for i, n in enumerate(plan[1]))
    apart = jnp.where((row_id >= 2) != (col_id >= 2), last_lat, 0) + jnp.where(
        (row_id % 2) != (col_id % 2), last_lon, 0
    )
    bias_of[...] = jnp.where(apart > 0, -1e30, 0.0)
    side[...] = grad.T
    reorder(plan, places_ref, side, (mine_ref, peer_ref), width // 2)
    pair_ref[:, 2 * inner :] = dot(grad, w_out_ref[...], ((1,), (1,))).astype(BF16)
    standard, _ = normalize(gather_window(quads, 0, wide))
    normed = (standard * gain_ref[...] + bias_ref[...]).astype(BF16)
    side[...] = normed.T
    reorder(plan, places_ref, side, (mine_ref, peer_ref))
    scale = jnp.asarray(HDIM ** (-0.5), BF16)
    query_ref[...] = dot(normed, w_qkv_ref[:, :inner], ((1,), (0,))).astype(BF16) * scale
    pair_ref[:, : 2 * inner] = dot(normed, w_qkv_ref[:, inner:], ((1,), (0,))).astype(BF16)
    alone, pick = pair_tools(total)
    for pair in range(inner // LANES):
        cols = slice(pair * LANES, (pair + 1) * LANES)
        query = query_ref[:, cols]
        key = pair_ref[:, cols]
        value = pair_ref[:, inner + pair * LANES : inner + (pair + 1) * LANES]
        grad_pair = pair_ref[:, 2 * inner + pair * LANES : 2 * inner + (pair + 1) * LANES]
        lows = []
        for head in range(2):
            scores = dot(alone(query, head), key, ((1,), (1,))) + bias_of[...]
            exps = jnp.exp(scores - jnp.max(scores, axis=-1, keepdims=True))
            probs = exps / jnp.sum(exps, axis=-1, keepdims=True)
            probs_ref[2 * pair + head] = probs
            lows.append(probs.astype(BF16))
        factor_ref[:, cols] = pick([dot(low, value, ((1,), (0,))) for low in lows]).astype(BF16)
        factor_ref[:, inner + pair * LANES : inner + (pair + 1) * LANES] = pick(
            [dot(low, grad_pair, ((0,), (0,))) for low in lows]
        ).astype(BF16)


def backward_body(query_ref, pair_ref, probs_ref, factor_ref):
    inner = query_ref.shape[1]
    scale = HDIM ** (-0.5)
    alone, pick = pair_tools(query_ref.shape[0])
    for pair in range(inner // LANES):
        cols = slice(pair * LANES, (pair + 1) * LANES)
        query = query_ref[:, cols]
        key = pair_ref[:, cols]
        value = pair_ref[:, inner + pair * LANES : inner + (pair + 1) * LANES]
        grad_pair = pair_ref[:, 2 * inner + pair * LANES : 2 * inner + (pair + 1) * LANES]
        lows = []
        for head in range(2):
            probs = probs_ref[2 * pair + head]
            grad_prob = dot(alone(grad_pair, head), value, ((1,), (1,)))
            inner_sum = jnp.sum(probs * grad_prob, axis=-1, keepdims=True)
            lows.append((probs * (grad_prob - inner_sum)).astype(BF16))
        factor_ref[:, cols] = (
            pick([dot(low, key, ((1,), (0,))) for low in lows]) * scale
        ).astype(BF16)
        factor_ref[:, inner + pair * LANES : inner + (pair + 1) * LANES] = pick(
            [dot(low, query, ((0,), (0,))) for low in lows]
        ).astype(BF16)


def gradient_body(
    plan, places_ref, r0, r1, r2, r3, factor_ref, late_ref, w_qkv_ref, w_out_ref, gain_ref,
    o0, o1, o2, o3, mine_ref, peer_ref, wide, flat,
):
    quads = (r0, r1, r2, r3)
    inner, width = w_out_ref.shape
    outs = (o0, o1, o2, o3)
    quad = o0.shape[1:]
    count = quad[0] * quad[1] * quad[2]
    tokens_wide = gather_window(quads, 0, wide)
    standard, inverse = normalize(tokens_wide)
    grad_normed = dot(factor_ref[:, inner:], w_qkv_ref[:, 2 * inner :], ((1,), (1,)))
    grad_normed += dot(late_ref[...], w_qkv_ref[:, : 2 * inner], ((1,), (1,)))
    sums = [
        jnp.sum(grad_normed * standard, axis=0, keepdims=True),
        jnp.sum(grad_normed, axis=0, keepdims=True),
    ]
    line = lax.broadcasted_iota(jnp.int32, (LANES, width), 0)
    flat[...] = jnp.where(line == 0, sums[0], jnp.where(line == 1, sums[1], 0.0)).T
    reorder(plan, places_ref, flat, (mine_ref, peer_ref))
    wide[...] = tokens_wide + dot(factor_ref[:, :inner], w_out_ref[...], ((1,), (0,)))
    for place, out in enumerate(outs):
        out[0] = wide[place * count : (place + 1) * count, :].astype(BF16).reshape(quad)
    grad_hat = grad_normed * gain_ref[...]
    first = jnp.mean(grad_hat, axis=-1, keepdims=True)
    second = jnp.mean(grad_hat * standard, axis=-1, keepdims=True)
    change = (grad_hat - first - standard * second) * inverse
    wide[...] = gather_window(quads, 1, wide) + change
    for place, out in enumerate(outs):
        out[1] = wide[place * count : (place + 1) * count, :].astype(BF16).reshape(quad)


def split_store(value, outs, cols):
    both, send_a, send_b = outs
    quarter = send_a.shape[0]
    for out, to, start in (
        (both, 0, 0), (send_a, 0, quarter), (both, quarter, 2 * quarter), (send_b, 0, 3 * quarter),
    ):
        out[to : to + quarter, cols] = value[start : start + quarter].astype(BF16)


def early_body(mine, got, factor, factor_got, *outs):
    half = mine.shape[0] // 2
    inner = factor.shape[1] // 2
    for part in range(2):
        rows = slice((1 - part) * half, (2 - part) * half)
        cols = slice(part * inner, (part + 1) * inner)
        value = dot(mine[rows, :], factor[:, cols], ((1,), (0,)))
        value += dot(got[rows, :], factor_got[:, cols], ((1,), (0,)))
        split_store(value, outs, cols)


def late_body(mine, got, factor, factor_got, sums, sums_got, *outs):
    half = mine.shape[0] // 2
    inner = factor.shape[1] // 2
    for part in range(2):
        cols = slice(part * inner, (part + 1) * inner)
        value = dot(mine[:half, :], factor[:, cols], ((1,), (0,)))
        value += dot(got[:half, :], factor_got[:, cols], ((1,), (0,)))
        split_store(value, outs, cols)
    split_store(sums[...] + sums_got[...], outs, slice(2 * inner, 2 * inner + LANES))


def added(*refs):
    total = refs[0].astype(F32)
    for ref in refs[1:]:
        total += ref.astype(F32)
    return total


def second_body(keep, got_a, got_b, both, send_a, send_b):
    part = send_a.shape[0]
    for side, (got, send) in enumerate(((got_a, send_a), (got_b, send_b))):
        at = 2 * part * side
        both[part * side : part * (side + 1), :] = added(
            keep[at : at + part, :], got[:part, :]
        ).astype(BF16)
        send[...] = added(keep[at + part : at + 2 * part, :], got[part:, :]).astype(BF16)


def third_body(keep, got_a, got_b, *outs):
    part = got_a.shape[0]
    size = outs[0].shape[0]
    for place, out in enumerate(outs):
        start = place * size
        got = got_a if start < part else got_b
        within = start % part
        out[...] = added(keep[start : start + size, :], got[within : within + size, :]).astype(BF16)


def turn_body(keep, got_a, got_b, *outs):
    part = got_a.shape[0]
    size = outs[0].shape[0] // 2
    per_side = len(outs) // 2
    for place, out in enumerate(outs):
        got, base = (got_a, 0) if place < per_side else (got_b, part)
        for nested in range(2):
            at = nested * (part // 2) + (place % per_side) * size
            out[nested * size : (nested + 1) * size, :] = added(
                keep[base + at : base + at + size, :], got[at : at + size, :]
            ).astype(BF16)


def meet_body(*refs):
    pieces, (base, send_a, send_b) = refs[:-3], refs[-3:]
    size = base.shape[0]
    per_side = len(pieces) // 2
    base[...] = added(*(item[:size, :] for item in pieces))
    send_a[...] = added(*(item[size:, :] for item in pieces[:per_side])).astype(BF16)
    send_b[...] = added(*(item[size:, :] for item in pieces[per_side:])).astype(BF16)


def early_end_body(factor, base, got_a, got_b, value_ref, out_ref):
    total = added(base[...], got_a[...], got_b[...]) * factor
    inner = out_ref.shape[1]
    out_ref[...] = total[:, :inner]
    value_ref[...] = total[:, inner:]


def late_end_body(factor, value_ref, *refs):
    pieces, (qkv_ref, gain_ref, bias_ref) = refs[:-3], refs[-3:]
    total = added(*(item[...] for item in pieces)) * factor
    cols = total.shape[1] - LANES
    qkv_ref[:, :cols] = total[:, :cols]
    qkv_ref[:, cols:] = value_ref[...]
    rows = total.shape[0]
    flat = jnp.concatenate([total[:, cols:], jnp.zeros((LANES - rows, LANES), F32)], axis=0).T
    gain_ref[...] = flat[0:1, :rows]
    bias_ref[...] = flat[1:2, :rows]


def xor_pairs(bit):
    return [(i, i ^ bit) for i in range(lax.axis_size("lat"))]


def swap(value, bit):
    return lax.ppermute(value, "lat", xor_pairs(bit))


def turn(pieces):
    count = len(pieces)
    return [pieces[0]] + [
        lax.ppermute(pieces[k], "lon", [(i, (i + k) % count) for i in range(count)])
        for k in range(1, count)
    ]


def sum_early(both, send_a, send_b, lon_count, factor):
    quarter, cols = send_a.shape
    size = quarter // lon_count
    got_a, got_b = swap(send_a, 2), swap(send_b, 4)
    pieces = call(turn_body, [((2 * size, cols), BF16)] * lon_count, (both, got_a, got_b))
    pieces = turn(pieces)
    base, send_a, send_b = call(
        meet_body, [((size, cols), F32)] + [((size, cols), BF16)] * 2, pieces
    )
    got_a, got_b = swap(send_a, 4), swap(send_b, 2)
    shape = ((size, cols // 2), F32)
    return call(
        functools.partial(early_end_body, factor), [shape] * 2,
        (base, got_a, got_b), near_out=1,
    )


def sum_late(both, send_a, send_b, value, lon_count, factor):
    quarter, cols = send_a.shape
    part = quarter // 2
    size = 2 * part // lon_count
    got_a, got_b = swap(send_a, 2), swap(send_b, 4)
    both, send_a, send_b = call(
        second_body, [((n * part, cols), BF16) for n in (2, 1, 1)], (both, got_a, got_b)
    )
    got_a, got_b = swap(send_a, 4), swap(send_b, 2)
    pieces = call(third_body, [((size, cols), BF16)] * lon_count, (both, got_a, got_b))
    pieces = turn(pieces)
    return call(
        functools.partial(late_end_body, factor),
        [((size, cols - LANES + value.shape[1]), F32)] + [((1, size), F32)] * 2,
        (value, *pieces), near_out=0,
    )


def device_step(tokens, layer_norm_gain, layer_norm_bias, w_qkv, w_out, output_cotangent):
    levels, lat_rows, lon_cols, width = tokens.shape
    inner = w_out.shape[0]
    lat_count, lon_count = lax.axis_size("lat"), lax.axis_size("lon")
    lat_place, lon_place = lax.axis_index("lat"), lax.axis_index("lon")
    cells = levels * lat_rows * lon_cols
    norm_factor = 1.0 / math.sqrt(cells * lat_count * lon_count)

    def moved(lat_step, lon_step):
        pairs = []
        for i in range(lat_count):
            for j in range(lon_count):
                to = ((i + lat_step) % lat_count) * lon_count + (j + lon_step) % lon_count
                pairs.append((i * lon_count + j, to))
        return pairs

    steps = ((0, 1), (1, 0), (1, 1))
    by_turn = (0, 2, 1)

    def moved_all(items, sign):
        moves = {}
        for place in by_turn:
            a, b = steps[place]
            moves[place] = lax.ppermute(items[place], ("lat", "lon"), moved(sign * a, sign * b))
        return [moves[place] for place in range(3)]

    grid = (lat_rows, lon_cols, levels, width)
    quad = (2, lat_rows // 2, lon_cols // 2, levels, width)
    tok = tokens.transpose(1, 2, 0, 3)
    cot = output_cotangent.transpose(1, 2, 0, 3)
    own, *sends = call(
        pack_body, [(quad, BF16)] * 4, (tok, cot), far=2,
        scratch=[pltpu.SemaphoreType.DMA((8,))],
    )
    quads = [own, *moved_all(sends, -1)]
    params = (w_qkv, w_out, layer_norm_gain.reshape(1, width), layer_norm_bias.reshape(1, width))
    params = call(
        fetch_body, [(item.shape, item.dtype) for item in params], params, far=4,
        scratch=[pltpu.SemaphoreType.DMA((4,))],
    )

    share = width // (lat_count * lon_count)
    hyper = lat_count == 8 and lon_count % 2 == 0 and share % 16 == 0
    order = []
    if hyper:
        half_lon = lon_count // 2
        for core, side, outer, nested, k in itertools.product(
            range(2), range(2), range(2), range(2), range(half_lon)
        ):
            x_bit, y_bit = (outer, nested) if side == 0 else (nested, outer)
            order.append((core + 2 * x_bit + 4 * y_bit, side * half_lon + k))
    plan = (share if hyper else 16, (lat_count, lon_count), tuple(order))
    places = jnp.where(jnp.arange(2) == 0, lat_place, lon_place).astype(jnp.int32)
    heads = inner // HDIM
    mine, peer, factor, query, pairs, probs = call(
        functools.partial(forward_body, plan),
        [((width, cells), BF16)] * 2
        + [((cells, n * inner), BF16) for n in (2, 1, 3)]
        + [((heads, cells, cells), F32)],
        (places, *quads, *params),
        scratch=[
            pltpu.VMEM((cells, width), F32),
            pltpu.VMEM((width, cells), BF16),
            pltpu.VMEM((cells, cells), F32),
        ],
        smem=1,
    )
    (factor_late,) = call(backward_body, [((cells, 2 * inner), BF16)], (query, pairs, probs))
    q0, q1, q2, q3, sums, sums_peer = call(
        functools.partial(gradient_body, plan),
        [(quad, BF16)] * 4 + [((width // 2, LANES), F32)] * 2,
        (places, *quads, factor, factor_late, *params[:3]),
        scratch=[pltpu.VMEM((cells, width), F32), pltpu.VMEM((width, LANES), F32)],
        smem=1,
    )
    if hyper:
        factor_got = swap(factor, 1)
        late_got = swap(factor_late, 1)
        got = swap(peer, 1)
        sums_got = swap(sums_peer, 1)
        quarter = width // 8

        def shapes(cols):
            return [((rows, cols), BF16) for rows in (2 * quarter, quarter, quarter)]

        early = call(early_body, shapes(2 * inner), (mine, got, factor, factor_got))
        late = call(
            late_body, shapes(2 * inner + LANES),
            (mine, got, factor_late, late_got, sums, sums_got),
        )
        value, d_out = sum_early(*early, lon_count, norm_factor)
        d_qkv, gain, bias = sum_late(*late, value, lon_count, norm_factor)
    else:
        half = width // 2
        normed_t = jnp.concatenate([mine[:half], peer[:half]], axis=0)
        cot_t = jnp.concatenate([mine[half:], peer[half:]], axis=0)
        whole = jnp.concatenate(
            [
                dot(cot_t, factor[:, :inner], ((1,), (0,))),
                dot(normed_t, factor[:, inner:], ((1,), (0,))),
                dot(normed_t, factor_late, ((1,), (0,))),
                jnp.concatenate([sums, sums_peer], axis=0),
            ],
            axis=1,
        )
        whole = lax.psum_scatter(whole, "lat", scatter_dimension=0, tiled=True)
        whole = lax.psum_scatter(whole, "lon", scatter_dimension=0, tiled=True)
        whole = whole * norm_factor
        d_out = whole[:, :inner]
        d_qkv = jnp.concatenate([whole[:, 2 * inner : 4 * inner], whole[:, inner : 2 * inner]], axis=1)
        gain, bias = whole[:, 4 * inner], whole[:, 4 * inner + 1]
    back = [q0, *moved_all((q1, q2, q3), 1)]
    y_out, token_gradient = call(unpack_body, [(grid, BF16)] * 2, back, near_out=0)
    return (
        y_out.transpose(2, 0, 1, 3),
        token_gradient.transpose(2, 0, 1, 3),
        d_qkv,
        d_out.T,
        gain.reshape(share),
        bias.reshape(share),
    )


def solution(mesh):
    in_specs = (P(None, "lat", "lon", None), P(), P(), P(), P(), P(None, "lat", "lon", None))
    out_specs = (
        P(None, "lat", "lon", None),
        P(None, "lat", "lon", None),
        P(("lat", "lon"), None),
        P(None, ("lat", "lon")),
        P(("lat", "lon")),
        P(("lat", "lon")),
    )
    return jax.shard_map(
        device_step, mesh=mesh, in_specs=in_specs, out_specs=out_specs, check_vma=False
    )
```

```python
import functools
import itertools
import math

import jax
import jax.numpy as jnp
from jax import lax
from jax.experimental import pallas as pl
from jax.experimental.pallas import tpu as pltpu
from jax.sharding import PartitionSpec as P


HDIM = 64
F32 = jnp.float32
EARLY = (0, 1)
LATE = (2, 3)
BF16 = jnp.bfloat16
LANES = 128

HBM_SPEC = pl.BlockSpec(memory_space=pltpu.HBM)

VMEM_SPEC = pl.BlockSpec(memory_space=pltpu.VMEM)
SMEM_SPEC = pl.BlockSpec(memory_space=pltpu.SMEM)


def dot(a, b, contract):
    return lax.dot_general(a, b, ((contract[0], contract[1]), ((), ())), preferred_element_type=F32)


def size_of(shape, dtype):
    rows = 16 if len(shape) > 1 and shape[-2] > 2 else shape[-2] if len(shape) > 1 else 1
    padded = [*shape[:-2], -(-shape[-2] // rows) * rows] if len(shape) > 1 else []
    return math.prod([*padded, -(-shape[-1] // LANES) * LANES]) * jnp.dtype(dtype).itemsize


def call(body, outs, args, scratch=(), smem=0, far=0, near_out=None, room=4):
    near_out = len(outs) if near_out is None else near_out
    near_at = smem + far
    held = sum(size_of(s, d) for s, d in outs[near_out:])
    held += sum(size_of(m.shape, m.dtype) for m in scratch if m.dtype in (F32, BF16))
    spaces = [None] * smem + [pltpu.HBM] * far + [pltpu.VMEM] * (len(args) - near_at)
    args = [
        a if space is None else pltpu.with_memory_space_constraint(a, space)
        for a, space in zip(args, spaces)
    ]
    return pl.pallas_call(
        body,
        out_shape=[
            pltpu.VMEM(s, d) if i < near_out else jax.ShapeDtypeStruct(s, d)
            for i, (s, d) in enumerate(outs)
        ],
        in_specs=[SMEM_SPEC] * smem + [HBM_SPEC] * far + [VMEM_SPEC] * (len(args) - near_at),
        out_specs=[VMEM_SPEC] * len(outs),
        scratch_shapes=list(scratch),
        compiler_params=pltpu.CompilerParams(vmem_limit_bytes=held + room * 2**20),
    )(*args)


def corners(rows, cols):
    return ((rows // 2, cols // 2), (rows // 2, 0), (0, cols // 2), (0, 0))


def run_copies(pairs, sem):
    copies = [
        pltpu.make_async_copy(source, target, sem.at[place])
        for place, (source, target) in enumerate(pairs)
    ]
    for item in copies:
        item.start()
    for item in copies:
        item.wait()


def pack_body(tok_ref, cot_ref, *refs):
    outs, sem = refs[:-1], refs[-1]
    rows, cols = tok_ref.shape[:2]
    pairs = []
    for out_ref, (row, col) in zip(outs, corners(rows, cols)):
        for part, ref in enumerate((tok_ref, cot_ref)):
            source = ref.at[pl.ds(row, rows // 2), pl.ds(col, cols // 2)]
            pairs.append((source, out_ref.at[part]))
    run_copies(pairs, sem)


def fetch_body(*refs):
    count = len(refs) // 2
    run_copies(list(zip(refs[:count], refs[count:-1])), refs[-1])


def unpack_body(q0, q1, q2, q3, tok_ref, w_out_ref, y_ref, grad_ref, att):
    rows, cols, levels, width = y_ref.shape
    inner = att.shape[-1]
    for quad, (row, col) in zip((q0, q1, q2, q3), corners(rows, cols)):
        at = (slice(row, row + rows // 2), slice(col, col + cols // 2))
        att[at] = quad[:, :, :, :inner]
        grad_ref[at] = quad[:, :, :, inner:]
    flat = att[...].reshape(rows * cols * levels, inner)
    mixed = dot(flat, w_out_ref[...], ((1,), (0,)))
    total = tok_ref[...].reshape(rows * cols * levels, width).astype(F32) + mixed
    y_ref[...] = total.astype(BF16).reshape(y_ref.shape)


def gather_window(quads, part, wide):
    levels, width = quads[0].shape[-2:]
    count = levels * quads[0].shape[1] * quads[0].shape[2]
    for place, item in enumerate(quads):
        wide[place * count : (place + 1) * count, :] = (
            item[part].reshape(count, width).astype(F32)
        )
    return wide[...]


def normalize(tokens_wide):
    average = jnp.mean(tokens_wide, axis=-1, keepdims=True)
    centered = tokens_wide - average
    inverse = lax.rsqrt(jnp.mean(centered * centered, axis=-1, keepdims=True) + 1e-05)
    return centered * inverse, inverse


def reorder(plan, places_ref, source, targets, base=0):
    group, counts, steps = plan
    half = source.shape[0] // 2
    for place in range(source.shape[0] // group):
        start = place * group
        if steps:
            block = places_ref[0] ^ steps[place][0]
            turned = places_ref[1] ^ steps[place][1]
            start = pl.multiple_of((block * counts[1] + turned) * group, group)
        at = place * group
        target = targets[at // half]
        at = base + at % half
        target[at : at + group, :] = source[pl.ds(start, group), :]


def pair_tools(total):
    lane = lax.broadcasted_iota(jnp.int32, (total, LANES), 1)
    first = lane < HDIM

    def alone(value, head):
        return jnp.where(first if head == 0 else ~first, value, jnp.zeros_like(value))

    def pick(results):
        return jnp.where(first, results[0], results[1])

    return alone, pick


def forward_body(
    plan, places_ref, r0, r1, r2, r3, w_qkv_ref, w_out_ref, gain_ref, bias_ref,
    mine_ref, peer_ref, factor_ref, query_ref, pair_ref, probs_ref, wide, side, bias_of,
):
    quads = (r0, r1, r2, r3)
    inner, width = w_out_ref.shape
    grad = gather_window(quads, 1, wide).astype(BF16)
    total = grad.shape[0]
    count = total // 4
    row_id = lax.broadcasted_iota(jnp.int32, (total, total), 0) // count
    col_id = lax.broadcasted_iota(jnp.int32, (total, total), 1) // count
    last_lat, last_lon = ((places_ref[i] == n - 1).astype(jnp.int32) for i, n in enumerate(plan[1]))
    apart = jnp.where((row_id >= 2) != (col_id >= 2), last_lat, 0) + jnp.where(
        (row_id % 2) != (col_id % 2), last_lon, 0
    )
    bias_of[...] = jnp.where(apart > 0, -1e30, 0.0)
    side[...] = grad.T
    reorder(plan, places_ref, side, (mine_ref, peer_ref), width // 2)
    pair_ref[:, 2 * inner :] = dot(grad, w_out_ref[...], ((1,), (1,))).astype(BF16)
    standard, _ = normalize(gather_window(quads, 0, wide))
    normed = (standard * gain_ref[...] + bias_ref[...]).astype(BF16)
    side[...] = normed.T
    reorder(plan, places_ref, side, (mine_ref, peer_ref))
    scale = jnp.asarray(HDIM ** (-0.5), BF16)
    query_ref[...] = dot(normed, w_qkv_ref[:, :inner], ((1,), (0,))).astype(BF16) * scale
    pair_ref[:, : 2 * inner] = dot(normed, w_qkv_ref[:, inner:], ((1,), (0,))).astype(BF16)
    alone, pick = pair_tools(total)
    for pair in range(inner // LANES):
        cols = slice(pair * LANES, (pair + 1) * LANES)
        query = query_ref[:, cols]
        key = pair_ref[:, cols]
        value = pair_ref[:, inner + pair * LANES : inner + (pair + 1) * LANES]
        grad_pair = pair_ref[:, 2 * inner + pair * LANES : 2 * inner + (pair + 1) * LANES]
        lows = []
        for head in range(2):
            scores = dot(alone(query, head), key, ((1,), (1,))) + bias_of[...]
            exps = jnp.exp(scores - jnp.max(scores, axis=-1, keepdims=True))
            probs = exps / jnp.sum(exps, axis=-1, keepdims=True)
            probs_ref[2 * pair + head] = probs
            lows.append(probs.astype(BF16))
        factor_ref[:, cols] = pick([dot(low, value, ((1,), (0,))) for low in lows]).astype(BF16)
        factor_ref[:, inner + pair * LANES : inner + (pair + 1) * LANES] = pick(
            [dot(low, grad_pair, ((0,), (0,))) for low in lows]
        ).astype(BF16)


def backward_body(query_ref, pair_ref, probs_ref, factor_ref):
    inner = query_ref.shape[1]
    scale = HDIM ** (-0.5)
    alone, pick = pair_tools(query_ref.shape[0])
    for pair in range(inner // LANES):
        cols = slice(pair * LANES, (pair + 1) * LANES)
        query = query_ref[:, cols]
        key = pair_ref[:, cols]
        value = pair_ref[:, inner + pair * LANES : inner + (pair + 1) * LANES]
        grad_pair = pair_ref[:, 2 * inner + pair * LANES : 2 * inner + (pair + 1) * LANES]
        lows = []
        for head in range(2):
            probs = probs_ref[2 * pair + head]
            grad_prob = dot(alone(grad_pair, head), value, ((1,), (1,)))
            inner_sum = jnp.sum(probs * grad_prob, axis=-1, keepdims=True)
            lows.append((probs * (grad_prob - inner_sum)).astype(BF16))
        factor_ref[:, cols] = (
            pick([dot(low, key, ((1,), (0,))) for low in lows]) * scale
        ).astype(BF16)
        factor_ref[:, inner + pair * LANES : inner + (pair + 1) * LANES] = pick(
            [dot(low, query, ((0,), (0,))) for low in lows]
        ).astype(BF16)


def gradient_body(
    plan, places_ref, r0, r1, r2, r3, factor_ref, late_ref, w_qkv_ref, gain_ref,
    o0, o1, o2, o3, mine_ref, peer_ref, wide, flat,
):
    quads = (r0, r1, r2, r3)
    inner, width = late_ref.shape[1] // 2, wide.shape[1]
    outs = (o0, o1, o2, o3)
    quad = o0.shape[:3]
    count = quad[0] * quad[1] * quad[2]
    tokens_wide = gather_window(quads, 0, wide)
    standard, inverse = normalize(tokens_wide)
    grad_normed = dot(factor_ref[:, inner:], w_qkv_ref[:, 2 * inner :], ((1,), (1,)))
    grad_normed += dot(late_ref[...], w_qkv_ref[:, : 2 * inner], ((1,), (1,)))
    sums = [
        jnp.sum(grad_normed * standard, axis=0, keepdims=True),
        jnp.sum(grad_normed, axis=0, keepdims=True),
    ]
    line = lax.broadcasted_iota(jnp.int32, (LANES, width), 0)
    flat[...] = jnp.where(line == 0, sums[0], jnp.where(line == 1, sums[1], 0.0)).T
    reorder(plan, places_ref, flat, (mine_ref, peer_ref))
    wide[:, :inner] = factor_ref[:, :inner].astype(F32)
    for place, out in enumerate(outs):
        rows = wide[place * count : (place + 1) * count, :inner]
        out[:, :, :, :inner] = rows.astype(BF16).reshape(*quad, inner)
    grad_hat = grad_normed * gain_ref[...]
    first = jnp.mean(grad_hat, axis=-1, keepdims=True)
    second = jnp.mean(grad_hat * standard, axis=-1, keepdims=True)
    change = (grad_hat - first - standard * second) * inverse
    wide[...] = gather_window(quads, 1, wide) + change
    for place, out in enumerate(outs):
        rows = wide[place * count : (place + 1) * count, :]
        out[:, :, :, inner:] = rows.astype(BF16).reshape(*quad, width)


def split_store(value, outs, cols):
    both, send_a, send_b = outs
    quarter = send_a.shape[0]
    for out, to, start in (
        (both, 0, 0), (send_a, 0, quarter), (both, quarter, 2 * quarter), (send_b, 0, 3 * quarter),
    ):
        out[to : to + quarter, cols] = value[start : start + quarter].astype(BF16)


def multiply(mine, got, factors, blocks, outs):
    half = mine.shape[0] // 2
    inner = factors[0].shape[1] // 2
    for place, block in enumerate(blocks):
        rows = slice(half, 2 * half) if block == 0 else slice(0, half)
        pair = 2 * (block // 2)
        at = block % 2 * inner
        value = dot(mine[rows, :], factors[pair][:, at : at + inner], ((1,), (0,)))
        value += dot(got[rows, :], factors[pair + 1][:, at : at + inner], ((1,), (0,)))
        split_store(value, outs, slice(place * inner, (place + 1) * inner))
    return len(blocks) * inner


def early_body(mine, got, *refs):
    multiply(mine, got, refs[:-3], EARLY, refs[-3:])


def late_body(mine, got, *refs):
    factors, (sums, sums_got), outs = refs[:-5], refs[-5:-3], refs[-3:]
    at = multiply(mine, got, factors, LATE, outs)
    split_store(sums[...] + sums_got[...], outs, slice(at, at + LANES))


def added(*refs):
    total = refs[0].astype(F32)
    for ref in refs[1:]:
        total += ref.astype(F32)
    return total


def second_body(keep, got_a, got_b, both, send_a, send_b):
    part = send_a.shape[0]
    for side, (got, send) in enumerate(((got_a, send_a), (got_b, send_b))):
        at = 2 * part * side
        both[part * side : part * (side + 1), :] = added(
            keep[at : at + part, :], got[:part, :]
        ).astype(BF16)
        send[...] = added(keep[at + part : at + 2 * part, :], got[part:, :]).astype(BF16)


def third_body(keep, got_a, got_b, *outs):
    part = got_a.shape[0]
    size = outs[0].shape[0]
    for place, out in enumerate(outs):
        start = place * size
        got = got_a if start < part else got_b
        within = start % part
        out[...] = added(keep[start : start + size, :], got[within : within + size, :]).astype(BF16)


def turn_body(keep, got_a, got_b, *outs):
    part = got_a.shape[0]
    size = outs[0].shape[0] // 2
    per_side = len(outs) // 2
    for place, out in enumerate(outs):
        got, base = (got_a, 0) if place < per_side else (got_b, part)
        for nested in range(2):
            at = nested * (part // 2) + (place % per_side) * size
            out[nested * size : (nested + 1) * size, :] = added(
                keep[base + at : base + at + size, :], got[at : at + size, :]
            ).astype(BF16)


def meet_body(*refs):
    pieces, (base, send_a, send_b) = refs[:-3], refs[-3:]
    size = base.shape[0]
    per_side = len(pieces) // 2
    base[...] = added(*(item[:size, :] for item in pieces))
    send_a[...] = added(*(item[size:, :] for item in pieces[:per_side])).astype(BF16)
    send_b[...] = added(*(item[size:, :] for item in pieces[per_side:])).astype(BF16)


def early_end_body(factor, base, got_a, got_b, value_ref, out_ref):
    total = added(base[...], got_a[...], got_b[...]) * factor
    inner = out_ref.shape[1]
    out_ref[...] = total[:, :inner]
    value_ref[...] = total[:, inner:]


def late_end_body(factor, value_ref, *refs):
    pieces, (qkv_ref, gain_ref, bias_ref) = refs[:-3], refs[-3:]
    total = added(*(item[...] for item in pieces)) * factor
    cols = total.shape[1] - LANES
    inner = cols // len(LATE)
    sources = {block: value_ref[:, i * inner : (i + 1) * inner] for i, block in enumerate(EARLY[1:])}
    sources |= {block: total[:, i * inner : (i + 1) * inner] for i, block in enumerate(LATE)}
    for place, block in enumerate((2, 3, 1)):
        qkv_ref[:, place * inner : (place + 1) * inner] = sources[block]
    rows = total.shape[0]
    flat = jnp.concatenate([total[:, cols:], jnp.zeros((LANES - rows, LANES), F32)], axis=0).T
    gain_ref[...] = flat[0:1, :rows]
    bias_ref[...] = flat[1:2, :rows]


def xor_pairs(bit):
    return [(i, i ^ bit) for i in range(lax.axis_size("lat"))]


def swap(value, bit):
    return lax.ppermute(value, "lat", xor_pairs(bit))


def turn(pieces):
    count = len(pieces)
    return [pieces[0]] + [
        lax.ppermute(pieces[k], "lon", [(i, i ^ k) for i in range(count)])
        for k in range(1, count)
    ]


def sum_early(both, send_a, send_b, lon_count, factor):
    quarter, cols = send_a.shape
    size = quarter // lon_count
    got_a, got_b = swap(send_a, 2), swap(send_b, 4)
    pieces = call(turn_body, [((2 * size, cols), BF16)] * lon_count, (both, got_a, got_b))
    pieces = turn(pieces)
    base, send_a, send_b = call(
        meet_body, [((size, cols), F32)] + [((size, cols), BF16)] * 2, pieces
    )
    got_a, got_b = swap(send_a, 4), swap(send_b, 2)
    return call(
        functools.partial(early_end_body, factor),
        [((size, cols - cols // len(EARLY)), F32), ((size, cols // len(EARLY)), F32)],
        (base, got_a, got_b), near_out=1,
    )


def sum_late(both, send_a, send_b, value, lon_count, factor):
    quarter, cols = send_a.shape
    part = quarter // 2
    size = 2 * part // lon_count
    got_a, got_b = swap(send_a, 2), swap(send_b, 4)
    both, send_a, send_b = call(
        second_body, [((n * part, cols), BF16) for n in (2, 1, 1)], (both, got_a, got_b)
    )
    got_a, got_b = swap(send_a, 4), swap(send_b, 2)
    pieces = call(third_body, [((size, cols), BF16)] * lon_count, (both, got_a, got_b))
    pieces = turn(pieces)
    return call(
        functools.partial(late_end_body, factor),
        [((size, cols - LANES + value.shape[1]), F32)] + [((1, size), F32)] * 2,
        (value, *pieces), near_out=0,
    )


def device_step(tokens, layer_norm_gain, layer_norm_bias, w_qkv, w_out, output_cotangent):
    levels, lat_rows, lon_cols, width = tokens.shape
    inner = w_out.shape[0]
    lat_count, lon_count = lax.axis_size("lat"), lax.axis_size("lon")
    lat_place, lon_place = lax.axis_index("lat"), lax.axis_index("lon")
    cells = levels * lat_rows * lon_cols
    norm_factor = 1.0 / math.sqrt(cells * lat_count * lon_count)

    def moved(lat_step, lon_step):
        pairs = []
        for i in range(lat_count):
            for j in range(lon_count):
                to = ((i + lat_step) % lat_count) * lon_count + (j + lon_step) % lon_count
                pairs.append((i * lon_count + j, to))
        return pairs

    steps = ((0, 1), (1, 0), (1, 1))
    by_turn = (0, 2, 1)

    def moved_all(items, sign):
        moves = {}
        for place in by_turn:
            a, b = steps[place]
            moves[place] = lax.ppermute(items[place], ("lat", "lon"), moved(sign * a, sign * b))
        return [moves[place] for place in range(3)]

    grid = (lat_rows, lon_cols, levels, width)
    quad = (2, lat_rows // 2, lon_cols // 2, levels, width)
    tok = tokens.transpose(1, 2, 0, 3)
    cot = output_cotangent.transpose(1, 2, 0, 3)
    own, *sends = call(
        pack_body, [(quad, BF16)] * 4, (tok, cot), far=2,
        scratch=[pltpu.SemaphoreType.DMA((8,))],
    )
    quads = [own, *moved_all(sends, -1)]
    params = (w_qkv, w_out, layer_norm_gain.reshape(1, width), layer_norm_bias.reshape(1, width))
    params = (*params, tok)
    *params, tok = call(
        fetch_body, [(item.shape, item.dtype) for item in params], params, far=5,
        scratch=[pltpu.SemaphoreType.DMA((5,))],
    )

    share = width // (lat_count * lon_count)
    hyper = lat_count == 8 and lon_count in (2, 4, 8) and share % 16 == 0
    order = []
    if hyper:
        half_lon = lon_count // 2
        for core, side, outer, nested, k in itertools.product(
            range(2), range(2), range(2), range(2), range(half_lon)
        ):
            x_bit, y_bit = (outer, nested) if side == 0 else (nested, outer)
            order.append((core + 2 * x_bit + 4 * y_bit, side * half_lon + k))
    plan = (share if hyper else 16, (lat_count, lon_count), tuple(order))
    places = jnp.where(jnp.arange(2) == 0, lat_place, lon_place).astype(jnp.int32)
    heads = inner // HDIM
    mine, peer, factor, query, pairs, probs = call(
        functools.partial(forward_body, plan),
        [((width, cells), BF16)] * 2
        + [((cells, n * inner), BF16) for n in (2, 1, 3)]
        + [((heads, cells, cells), F32)],
        (places, *quads, *params),
        scratch=[
            pltpu.VMEM((cells, width), F32),
            pltpu.VMEM((width, cells), BF16),
            pltpu.VMEM((cells, cells), F32),
        ],
        smem=1,
    )
    (factor_late,) = call(backward_body, [((cells, 2 * inner), BF16)], (query, pairs, probs))
    q0, q1, q2, q3, sums, sums_peer = call(
        functools.partial(gradient_body, plan),
        [((*quad[1:-1], inner + width), BF16)] * 4 + [((width // 2, LANES), F32)] * 2,
        (places, *quads, factor, factor_late, params[0], params[2]),
        scratch=[pltpu.VMEM((cells, width), F32), pltpu.VMEM((width, LANES), F32)],
        smem=1,
    )
    if hyper:
        factor_got = swap(factor, 1)
        late_got = swap(factor_late, 1)
        got = swap(peer, 1)
        sums_got = swap(sums_peer, 1)
        quarter = width // 8

        def shapes(cols):
            return [((rows, cols), BF16) for rows in (2 * quarter, quarter, quarter)]

        factors = (factor, factor_got, factor_late, late_got)
        early = call(
            early_body, shapes(len(EARLY) * inner),
            (mine, got, *factors[: 2 * (EARLY[-1] // 2 + 1)]),
        )
        late = call(
            late_body, shapes(len(LATE) * inner + LANES),
            (mine, got, *factors, sums, sums_got),
        )
        value, d_out = sum_early(*early, lon_count, norm_factor)
        d_qkv, gain, bias = sum_late(*late, value, lon_count, norm_factor)
    else:
        half = width // 2
        normed_t = jnp.concatenate([mine[:half], peer[:half]], axis=0)
        cot_t = jnp.concatenate([mine[half:], peer[half:]], axis=0)
        whole = jnp.concatenate(
            [
                dot(cot_t, factor[:, :inner], ((1,), (0,))),
                dot(normed_t, factor[:, inner:], ((1,), (0,))),
                dot(normed_t, factor_late, ((1,), (0,))),
                jnp.concatenate([sums, sums_peer], axis=0),
            ],
            axis=1,
        )
        whole = lax.psum_scatter(whole, "lat", scatter_dimension=0, tiled=True)
        whole = lax.psum_scatter(whole, "lon", scatter_dimension=0, tiled=True)
        whole = whole * norm_factor
        d_out = whole[:, :inner]
        d_qkv = jnp.concatenate([whole[:, 2 * inner : 4 * inner], whole[:, inner : 2 * inner]], axis=1)
        gain, bias = whole[:, 4 * inner], whole[:, 4 * inner + 1]
    back = [q0, *moved_all((q1, q2, q3), 1)]
    y_out, token_gradient = call(
        unpack_body, [(grid, BF16)] * 2, (*back, tok, params[1]), near_out=0,
        scratch=[pltpu.VMEM((*grid[:-1], inner), BF16)],
    )
    return (
        y_out.transpose(2, 0, 1, 3),
        token_gradient.transpose(2, 0, 1, 3),
        d_qkv,
        d_out.T,
        gain.reshape(share),
        bias.reshape(share),
    )


def solution(mesh):
    in_specs = (P(None, "lat", "lon", None), P(), P(), P(), P(), P(None, "lat", "lon", None))
    out_specs = (
        P(None, "lat", "lon", None),
        P(None, "lat", "lon", None),
        P(("lat", "lon"), None),
        P(None, ("lat", "lon")),
        P(("lat", "lon")),
        P(("lat", "lon")),
    )
    return jax.shard_map(
        device_step, mesh=mesh, in_specs=in_specs, out_specs=out_specs, check_vma=False
    )
```

```python
import functools
import itertools
import math

import jax
import jax.numpy as jnp
from jax import lax
from jax.experimental import pallas as pl
from jax.experimental.pallas import tpu as pltpu
from jax.sharding import PartitionSpec as P


HDIM = 64
F32 = jnp.float32
EARLY = (0, 1)
LATE = (2, 3)
BF16 = jnp.bfloat16
LANES = 128

HBM_SPEC = pl.BlockSpec(memory_space=pltpu.HBM)

VMEM_SPEC = pl.BlockSpec(memory_space=pltpu.VMEM)
SMEM_SPEC = pl.BlockSpec(memory_space=pltpu.SMEM)


def dot(a, b, contract):
    return lax.dot_general(a, b, ((contract[0], contract[1]), ((), ())), preferred_element_type=F32)


def size_of(shape, dtype):
    rows = 16 if len(shape) > 1 and shape[-2] > 2 else shape[-2] if len(shape) > 1 else 1
    padded = [*shape[:-2], -(-shape[-2] // rows) * rows] if len(shape) > 1 else []
    return math.prod([*padded, -(-shape[-1] // LANES) * LANES]) * jnp.dtype(dtype).itemsize


def call(body, outs, args, scratch=(), smem=0, far=0, near_out=None, room=4):
    near_out = len(outs) if near_out is None else near_out
    near_at = smem + far
    held = sum(size_of(s, d) for s, d in outs[near_out:])
    held += sum(size_of(m.shape, m.dtype) for m in scratch if m.dtype in (F32, BF16))
    spaces = [None] * smem + [pltpu.HBM] * far + [pltpu.VMEM] * (len(args) - near_at)
    args = [
        a if space is None else pltpu.with_memory_space_constraint(a, space)
        for a, space in zip(args, spaces)
    ]
    return pl.pallas_call(
        body,
        out_shape=[
            pltpu.VMEM(s, d) if i < near_out else jax.ShapeDtypeStruct(s, d)
            for i, (s, d) in enumerate(outs)
        ],
        in_specs=[SMEM_SPEC] * smem + [HBM_SPEC] * far + [VMEM_SPEC] * (len(args) - near_at),
        out_specs=[VMEM_SPEC] * len(outs),
        scratch_shapes=list(scratch),
        compiler_params=pltpu.CompilerParams(vmem_limit_bytes=held + room * 2**20),
    )(*args)


def corners(rows, cols):
    return ((rows // 2, cols // 2), (rows // 2, 0), (0, cols // 2), (0, 0))


def run_copies(pairs, sem):
    copies = [
        pltpu.make_async_copy(source, target, sem.at[place])
        for place, (source, target) in enumerate(pairs)
    ]
    for item in copies:
        item.start()
    for item in copies:
        item.wait()


def pack_body(tok_ref, cot_ref, *refs):
    outs, sem = refs[:-1], refs[-1]
    rows, cols = tok_ref.shape[:2]
    pairs = []
    for out_ref, (row, col) in zip(outs, corners(rows, cols)):
        for part, ref in enumerate((tok_ref, cot_ref)):
            source = ref.at[pl.ds(row, rows // 2), pl.ds(col, cols // 2)]
            pairs.append((source, out_ref.at[part]))
    run_copies(pairs, sem)


def fetch_body(*refs):
    count = len(refs) // 2
    run_copies(list(zip(refs[:count], refs[count:-1])), refs[-1])


def unpack_body(q0, q1, q2, q3, tok_ref, w_out_ref, y_ref, grad_ref, att):
    rows, cols, levels, width = y_ref.shape
    inner = att.shape[-1]
    for quad, (row, col) in zip((q0, q1, q2, q3), corners(rows, cols)):
        at = (slice(row, row + rows // 2), slice(col, col + cols // 2))
        att[at] = quad[:, :, :, :inner]
        grad_ref[at] = quad[:, :, :, inner:]
    flat = att[...].reshape(rows * cols * levels, inner)
    mixed = dot(flat, w_out_ref[...], ((1,), (0,)))
    total = tok_ref[...].reshape(rows * cols * levels, width).astype(F32) + mixed
    y_ref[...] = total.astype(BF16).reshape(y_ref.shape)


def gather_window(quads, part, wide):
    levels, width = quads[0].shape[-2:]
    count = levels * quads[0].shape[1] * quads[0].shape[2]
    for place, item in enumerate(quads):
        wide[place * count : (place + 1) * count, :] = (
            item[part].reshape(count, width).astype(F32)
        )
    return wide[...]


def normalize(tokens_wide):
    average = jnp.mean(tokens_wide, axis=-1, keepdims=True)
    centered = tokens_wide - average
    inverse = lax.rsqrt(jnp.mean(centered * centered, axis=-1, keepdims=True) + 1e-05)
    return centered * inverse, inverse


def reorder(plan, places_ref, source, targets, base=0):
    group, counts, steps = plan
    half = source.shape[0] // 2
    for place in range(source.shape[0] // group):
        start = place * group
        if steps:
            block = places_ref[0] ^ steps[place][0]
            turned = places_ref[1] ^ steps[place][1]
            start = pl.multiple_of((block * counts[1] + turned) * group, group)
        at = place * group
        target = targets[at // half]
        at = base + at % half
        target[at : at + group, :] = source[pl.ds(start, group), :]


def pair_tools(total):
    lane = lax.broadcasted_iota(jnp.int32, (total, LANES), 1)
    first = lane < HDIM

    def alone(value, head):
        return jnp.where(first if head == 0 else ~first, value, jnp.zeros_like(value))

    def pick(results):
        return jnp.where(first, results[0], results[1])

    return alone, pick


def forward_body(
    plan, places_ref, r0, r1, r2, r3, w_qkv_ref, w_out_ref, gain_ref, bias_ref,
    mine_ref, peer_ref, factor_ref, query_ref, pair_ref, probs_ref, wide, side, bias_of,
):
    quads = (r0, r1, r2, r3)
    inner, width = w_out_ref.shape
    grad = gather_window(quads, 1, wide).astype(BF16)
    total = grad.shape[0]
    count = total // 4
    row_id = lax.broadcasted_iota(jnp.int32, (total, total), 0) // count
    col_id = lax.broadcasted_iota(jnp.int32, (total, total), 1) // count
    last_lat, last_lon = ((places_ref[i] == n - 1).astype(jnp.int32) for i, n in enumerate(plan[1]))
    apart = jnp.where((row_id >= 2) != (col_id >= 2), last_lat, 0) + jnp.where(
        (row_id % 2) != (col_id % 2), last_lon, 0
    )
    bias_of[...] = jnp.where(apart > 0, -1e30, 0.0)
    side[...] = grad.T
    reorder(plan, places_ref, side, (mine_ref, peer_ref), width // 2)
    pair_ref[:, 2 * inner :] = dot(grad, w_out_ref[...], ((1,), (1,))).astype(BF16)
    standard, _ = normalize(gather_window(quads, 0, wide))
    normed = (standard * gain_ref[...] + bias_ref[...]).astype(BF16)
    side[...] = normed.T
    reorder(plan, places_ref, side, (mine_ref, peer_ref))
    scale = jnp.asarray(HDIM ** (-0.5), BF16)
    query_ref[...] = dot(normed, w_qkv_ref[:, :inner], ((1,), (0,))).astype(BF16) * scale
    pair_ref[:, : 2 * inner] = dot(normed, w_qkv_ref[:, inner:], ((1,), (0,))).astype(BF16)
    alone, pick = pair_tools(total)
    for pair in range(inner // LANES):
        cols = slice(pair * LANES, (pair + 1) * LANES)
        query = query_ref[:, cols]
        key = pair_ref[:, cols]
        value = pair_ref[:, inner + pair * LANES : inner + (pair + 1) * LANES]
        grad_pair = pair_ref[:, 2 * inner + pair * LANES : 2 * inner + (pair + 1) * LANES]
        lows = []
        for head in range(2):
            scores = dot(alone(query, head), key, ((1,), (1,))) + bias_of[...]
            exps = jnp.exp(scores - jnp.max(scores, axis=-1, keepdims=True))
            probs = exps / jnp.sum(exps, axis=-1, keepdims=True)
            probs_ref[2 * pair + head] = probs
            lows.append(probs.astype(BF16))
        factor_ref[:, cols] = pick([dot(low, value, ((1,), (0,))) for low in lows]).astype(BF16)
        factor_ref[:, inner + pair * LANES : inner + (pair + 1) * LANES] = pick(
            [dot(low, grad_pair, ((0,), (0,))) for low in lows]
        ).astype(BF16)


def backward_body(query_ref, pair_ref, probs_ref, factor_ref):
    inner = query_ref.shape[1]
    scale = HDIM ** (-0.5)
    alone, pick = pair_tools(query_ref.shape[0])
    for pair in range(inner // LANES):
        cols = slice(pair * LANES, (pair + 1) * LANES)
        query = query_ref[:, cols]
        key = pair_ref[:, cols]
        value = pair_ref[:, inner + pair * LANES : inner + (pair + 1) * LANES]
        grad_pair = pair_ref[:, 2 * inner + pair * LANES : 2 * inner + (pair + 1) * LANES]
        lows = []
        for head in range(2):
            probs = probs_ref[2 * pair + head]
            grad_prob = dot(alone(grad_pair, head), value, ((1,), (1,)))
            inner_sum = jnp.sum(probs * grad_prob, axis=-1, keepdims=True)
            lows.append((probs * (grad_prob - inner_sum)).astype(BF16))
        factor_ref[:, cols] = (
            pick([dot(low, key, ((1,), (0,))) for low in lows]) * scale
        ).astype(BF16)
        factor_ref[:, inner + pair * LANES : inner + (pair + 1) * LANES] = pick(
            [dot(low, query, ((0,), (0,))) for low in lows]
        ).astype(BF16)


def gradient_body(
    plan, places_ref, r0, r1, r2, r3, factor_ref, late_ref, w_qkv_ref, gain_ref,
    o0, o1, o2, o3, mine_ref, peer_ref, wide, flat,
):
    quads = (r0, r1, r2, r3)
    inner, width = late_ref.shape[1] // 2, wide.shape[1]
    outs = (o0, o1, o2, o3)
    quad = o0.shape[:3]
    count = quad[0] * quad[1] * quad[2]
    tokens_wide = gather_window(quads, 0, wide)
    standard, inverse = normalize(tokens_wide)
    grad_normed = dot(factor_ref[:, inner:], w_qkv_ref[:, 2 * inner :], ((1,), (1,)))
    grad_normed += dot(late_ref[...], w_qkv_ref[:, : 2 * inner], ((1,), (1,)))
    sums = [
        jnp.sum(grad_normed * standard, axis=0, keepdims=True),
        jnp.sum(grad_normed, axis=0, keepdims=True),
    ]
    line = lax.broadcasted_iota(jnp.int32, (LANES, width), 0)
    flat[...] = jnp.where(line == 0, sums[0], jnp.where(line == 1, sums[1], 0.0)).T
    reorder(plan, places_ref, flat, (mine_ref, peer_ref))
    wide[:, :inner] = factor_ref[:, :inner].astype(F32)
    for place, out in enumerate(outs):
        rows = wide[place * count : (place + 1) * count, :inner]
        out[:, :, :, :inner] = rows.astype(BF16).reshape(*quad, inner)
    grad_hat = grad_normed * gain_ref[...]
    first = jnp.mean(grad_hat, axis=-1, keepdims=True)
    second = jnp.mean(grad_hat * standard, axis=-1, keepdims=True)
    change = (grad_hat - first - standard * second) * inverse
    wide[...] = gather_window(quads, 1, wide) + change
    for place, out in enumerate(outs):
        rows = wide[place * count : (place + 1) * count, :]
        out[:, :, :, inner:] = rows.astype(BF16).reshape(*quad, width)


def split_store(value, outs, cols):
    both, send_a, send_b = outs
    quarter = send_a.shape[0]
    for out, to, start in (
        (both, 0, 0), (send_a, 0, quarter), (both, quarter, 2 * quarter), (send_b, 0, 3 * quarter),
    ):
        out[to : to + quarter, cols] = value[start : start + quarter].astype(BF16)


def multiply(mine, got, factors, blocks, outs):
    half = mine.shape[0] // 2
    inner = factors[0].shape[1] // 2
    for place, block in enumerate(blocks):
        rows = slice(half, 2 * half) if block == 0 else slice(0, half)
        pair = 2 * (block // 2)
        at = block % 2 * inner
        value = dot(mine[rows, :], factors[pair][:, at : at + inner], ((1,), (0,)))
        value += dot(got[rows, :], factors[pair + 1][:, at : at + inner], ((1,), (0,)))
        split_store(value, outs, slice(place * inner, (place + 1) * inner))
    return len(blocks) * inner


def early_body(mine, got, *refs):
    multiply(mine, got, refs[:-3], EARLY, refs[-3:])


def late_body(mine, got, *refs):
    factors, (sums, sums_got), outs = refs[:-5], refs[-5:-3], refs[-3:]
    at = multiply(mine, got, factors, LATE, outs)
    split_store(sums[...] + sums_got[...], outs, slice(at, at + LANES))


def added(*refs):
    total = refs[0].astype(F32)
    for ref in refs[1:]:
        total += ref.astype(F32)
    return total


def second_body(keep, got_a, got_b, both, send_a, send_b):
    part = send_a.shape[0]
    for side, (got, send) in enumerate(((got_a, send_a), (got_b, send_b))):
        at = 2 * part * side
        both[part * side : part * (side + 1), :] = added(
            keep[at : at + part, :], got[:part, :]
        ).astype(BF16)
        send[...] = added(keep[at + part : at + 2 * part, :], got[part:, :]).astype(BF16)


def third_body(keep, got_a, got_b, *outs):
    part = got_a.shape[0]
    size = outs[0].shape[0]
    for place, out in enumerate(outs):
        start = place * size
        got = got_a if start < part else got_b
        within = start % part
        out[...] = added(keep[start : start + size, :], got[within : within + size, :]).astype(BF16)


def turn_body(keep, got_a, got_b, *outs):
    part = got_a.shape[0]
    size = outs[0].shape[0] // 2
    per_side = len(outs) // 2
    for place, out in enumerate(outs):
        got, base = (got_a, 0) if place < per_side else (got_b, part)
        for nested in range(2):
            at = nested * (part // 2) + (place % per_side) * size
            out[nested * size : (nested + 1) * size, :] = added(
                keep[base + at : base + at + size, :], got[at : at + size, :]
            ).astype(BF16)


def meet_body(*refs):
    pieces, (base, send_a, send_b) = refs[:-3], refs[-3:]
    size = base.shape[0]
    per_side = len(pieces) // 2
    base[...] = added(*(item[:size, :] for item in pieces))
    send_a[...] = added(*(item[size:, :] for item in pieces[:per_side])).astype(BF16)
    send_b[...] = added(*(item[size:, :] for item in pieces[per_side:])).astype(BF16)


def end_body(factor, base, got_a, got_b, *refs):
    pieces, (qkv_ref, out_ref, gain_ref, bias_ref) = refs[:-4], refs[-4:]
    early = added(base[...], got_a[...], got_b[...]) * factor
    total = added(*(item[...] for item in pieces)) * factor
    cols = total.shape[1] - LANES
    inner = cols // len(LATE)
    sources = {block: early[:, i * inner : (i + 1) * inner] for i, block in enumerate(EARLY)}
    out_ref[...] = sources[0]
    sources |= {block: total[:, i * inner : (i + 1) * inner] for i, block in enumerate(LATE)}
    for place, block in enumerate((2, 3, 1)):
        qkv_ref[:, place * inner : (place + 1) * inner] = sources[block]
    rows = total.shape[0]
    flat = jnp.concatenate([total[:, cols:], jnp.zeros((LANES - rows, LANES), F32)], axis=0).T
    gain_ref[...] = flat[0:1, :rows]
    bias_ref[...] = flat[1:2, :rows]


def xor_pairs(bit):
    return [(i, i ^ bit) for i in range(lax.axis_size("lat"))]


def swap(value, bit):
    return lax.ppermute(value, "lat", xor_pairs(bit))


def turn(pieces):
    count = len(pieces)
    return [pieces[0]] + [
        lax.ppermute(pieces[k], "lon", [(i, i ^ k) for i in range(count)])
        for k in range(1, count)
    ]


def sum_early(both, send_a, send_b, lon_count):
    quarter, cols = send_a.shape
    size = quarter // lon_count
    got_a, got_b = swap(send_a, 2), swap(send_b, 4)
    pieces = call(turn_body, [((2 * size, cols), BF16)] * lon_count, (both, got_a, got_b))
    pieces = turn(pieces)
    base, send_a, send_b = call(
        meet_body, [((size, cols), F32)] + [((size, cols), BF16)] * 2, pieces
    )
    got_a, got_b = swap(send_a, 4), swap(send_b, 2)
    return base, got_a, got_b


def sum_late(both, send_a, send_b, lon_count):
    quarter, cols = send_a.shape
    part = quarter // 2
    size = 2 * part // lon_count
    got_a, got_b = swap(send_a, 2), swap(send_b, 4)
    both, send_a, send_b = call(
        second_body, [((n * part, cols), BF16) for n in (2, 1, 1)], (both, got_a, got_b)
    )
    got_a, got_b = swap(send_a, 4), swap(send_b, 2)
    pieces = call(third_body, [((size, cols), BF16)] * lon_count, (both, got_a, got_b))
    pieces = turn(pieces)
    return pieces


def device_step(tokens, layer_norm_gain, layer_norm_bias, w_qkv, w_out, output_cotangent):
    levels, lat_rows, lon_cols, width = tokens.shape
    inner = w_out.shape[0]
    lat_count, lon_count = lax.axis_size("lat"), lax.axis_size("lon")
    lat_place, lon_place = lax.axis_index("lat"), lax.axis_index("lon")
    cells = levels * lat_rows * lon_cols
    norm_factor = 1.0 / math.sqrt(cells * lat_count * lon_count)

    def moved(lat_step, lon_step):
        pairs = []
        for i in range(lat_count):
            for j in range(lon_count):
                to = ((i + lat_step) % lat_count) * lon_count + (j + lon_step) % lon_count
                pairs.append((i * lon_count + j, to))
        return pairs

    steps = ((0, 1), (1, 0), (1, 1))
    by_turn = (0, 2, 1)

    def moved_all(items, sign):
        moves = {}
        for place in by_turn:
            a, b = steps[place]
            moves[place] = lax.ppermute(
                items[place], ("lat", "lon"), moved(sign * a, sign * b)
            )
        return [moves[place] for place in range(3)]

    grid = (lat_rows, lon_cols, levels, width)
    quad = (2, lat_rows // 2, lon_cols // 2, levels, width)
    tok = tokens.transpose(1, 2, 0, 3)
    cot = output_cotangent.transpose(1, 2, 0, 3)
    own, *sends = call(
        pack_body, [(quad, BF16)] * 4, (tok, cot), far=2,
        scratch=[pltpu.SemaphoreType.DMA((8,))],
    )
    quads = [own, *moved_all(sends, -1)]
    params = (w_qkv, w_out, layer_norm_gain.reshape(1, width), layer_norm_bias.reshape(1, width))
    params = (*params, tok)
    *params, tok = call(
        fetch_body, [(item.shape, item.dtype) for item in params], params, far=5,
        scratch=[pltpu.SemaphoreType.DMA((5,))],
    )

    share = width // (lat_count * lon_count)
    hyper = lat_count == 8 and lon_count in (2, 4, 8) and share % 16 == 0
    order = []
    if hyper:
        half_lon = lon_count // 2
        for core, side, outer, nested, k in itertools.product(
            range(2), range(2), range(2), range(2), range(half_lon)
        ):
            x_bit, y_bit = (outer, nested) if side == 0 else (nested, outer)
            order.append((core + 2 * x_bit + 4 * y_bit, side * half_lon + k))
    plan = (share if hyper else 16, (lat_count, lon_count), tuple(order))
    places = jnp.where(jnp.arange(2) == 0, lat_place, lon_place).astype(jnp.int32)
    heads = inner // HDIM
    mine, peer, factor, query, pairs, probs = call(
        functools.partial(forward_body, plan),
        [((width, cells), BF16)] * 2
        + [((cells, n * inner), BF16) for n in (2, 1, 3)]
        + [((heads, cells, cells), F32)],
        (places, *quads, *params),
        scratch=[
            pltpu.VMEM((cells, width), F32),
            pltpu.VMEM((width, cells), BF16),
            pltpu.VMEM((cells, cells), F32),
        ],
        smem=1,
    )
    (factor_late,) = call(backward_body, [((cells, 2 * inner), BF16)], (query, pairs, probs))
    q0, q1, q2, q3, sums, sums_peer = call(
        functools.partial(gradient_body, plan),
        [((*quad[1:-1], inner + width), BF16)] * 4 + [((width // 2, LANES), F32)] * 2,
        (places, *quads, factor, factor_late, params[0], params[2]),
        scratch=[pltpu.VMEM((cells, width), F32), pltpu.VMEM((width, LANES), F32)],
        smem=1,
    )
    if hyper:
        factor_got = swap(factor, 1)
        late_got = swap(factor_late, 1)
        got = swap(peer, 1)
        sums_got = swap(sums_peer, 1)
        quarter = width // 8

        def shapes(cols):
            return [((rows, cols), BF16) for rows in (2 * quarter, quarter, quarter)]

        factors = (factor, factor_got, factor_late, late_got)
        early = call(
            early_body, shapes(len(EARLY) * inner),
            (mine, got, *factors[: 2 * (EARLY[-1] // 2 + 1)]),
        )
        late = call(
            late_body, shapes(len(LATE) * inner + LANES),
            (mine, got, *factors, sums, sums_got),
        )
        parts = (*sum_early(*early, lon_count), *sum_late(*late, lon_count))
        d_qkv, d_out, gain, bias = call(
            functools.partial(end_body, norm_factor),
            [((share, n * inner), F32) for n in (3, 1)] + [((1, share), F32)] * 2,
            parts, near_out=0,
        )
    else:
        half = width // 2
        normed_t = jnp.concatenate([mine[:half], peer[:half]], axis=0)
        cot_t = jnp.concatenate([mine[half:], peer[half:]], axis=0)
        whole = jnp.concatenate(
            [
                dot(cot_t, factor[:, :inner], ((1,), (0,))),
                dot(normed_t, factor[:, inner:], ((1,), (0,))),
                dot(normed_t, factor_late, ((1,), (0,))),
                jnp.concatenate([sums, sums_peer], axis=0),
            ],
            axis=1,
        )
        whole = lax.psum_scatter(whole, "lat", scatter_dimension=0, tiled=True)
        whole = lax.psum_scatter(whole, "lon", scatter_dimension=0, tiled=True)
        whole = whole * norm_factor
        d_out = whole[:, :inner]
        d_qkv = jnp.concatenate([whole[:, 2 * inner : 4 * inner], whole[:, inner : 2 * inner]], axis=1)
        gain, bias = whole[:, 4 * inner], whole[:, 4 * inner + 1]
    back = [q0, *moved_all((q1, q2, q3), 1)]
    y_out, token_gradient = call(
        unpack_body, [(grid, BF16)] * 2, (*back, tok, params[1]), near_out=0,
        scratch=[pltpu.VMEM((*grid[:-1], inner), BF16)],
    )
    return (
        y_out.transpose(2, 0, 1, 3),
        token_gradient.transpose(2, 0, 1, 3),
        d_qkv,
        d_out.T,
        gain.reshape(share),
        bias.reshape(share),
    )


def solution(mesh):
    in_specs = (P(None, "lat", "lon", None), P(), P(), P(), P(), P(None, "lat", "lon", None))
    out_specs = (
        P(None, "lat", "lon", None),
        P(None, "lat", "lon", None),
        P(("lat", "lon"), None),
        P(None, ("lat", "lon")),
        P(("lat", "lon")),
        P(("lat", "lon")),
    )
    return jax.shard_map(
        device_step, mesh=mesh, in_specs=in_specs, out_specs=out_specs, check_vma=False
    )
```

```python
import functools
import itertools
import math

import jax
import jax.numpy as jnp
from jax import lax
from jax.experimental import pallas as pl
from jax.experimental.pallas import tpu as pltpu
from jax.sharding import PartitionSpec as P


HDIM = 64
F32 = jnp.float32
EARLY = (0, 1)
LATE = (2, 3)
BF16 = jnp.bfloat16
LANES = 128

HBM_SPEC = pl.BlockSpec(memory_space=pltpu.HBM)

VMEM_SPEC = pl.BlockSpec(memory_space=pltpu.VMEM)
SMEM_SPEC = pl.BlockSpec(memory_space=pltpu.SMEM)


def dot(a, b, contract):
    return lax.dot_general(a, b, ((contract[0], contract[1]), ((), ())), preferred_element_type=F32)


def size_of(shape, dtype):
    rows = 16 if len(shape) > 1 and shape[-2] > 2 else shape[-2] if len(shape) > 1 else 1
    padded = [*shape[:-2], -(-shape[-2] // rows) * rows] if len(shape) > 1 else []
    return math.prod([*padded, -(-shape[-1] // LANES) * LANES]) * jnp.dtype(dtype).itemsize


def call(body, outs, args, scratch=(), smem=0, far=0, near_out=None, room=4):
    near_out = len(outs) if near_out is None else near_out
    near_at = smem + far
    held = sum(size_of(s, d) for s, d in outs[near_out:])
    held += sum(size_of(m.shape, m.dtype) for m in scratch if m.dtype in (F32, BF16))
    spaces = [None] * smem + [pltpu.HBM] * far + [pltpu.VMEM] * (len(args) - near_at)
    args = [
        a if space is None else pltpu.with_memory_space_constraint(a, space)
        for a, space in zip(args, spaces)
    ]
    return pl.pallas_call(
        body,
        out_shape=[
            pltpu.VMEM(s, d) if i < near_out else jax.ShapeDtypeStruct(s, d)
            for i, (s, d) in enumerate(outs)
        ],
        in_specs=[SMEM_SPEC] * smem + [HBM_SPEC] * far + [VMEM_SPEC] * (len(args) - near_at),
        out_specs=[VMEM_SPEC] * len(outs),
        scratch_shapes=list(scratch),
        compiler_params=pltpu.CompilerParams(vmem_limit_bytes=held + room * 2**20),
    )(*args)


def corners(rows, cols):
    return ((rows // 2, cols // 2), (rows // 2, 0), (0, cols // 2), (0, 0))


def run_copies(pairs, sem):
    copies = [
        pltpu.make_async_copy(source, target, sem.at[place])
        for place, (source, target) in enumerate(pairs)
    ]
    for item in copies:
        item.start()
    for item in copies:
        item.wait()


def pack_body(tok_ref, cot_ref, *refs):
    outs, sem = refs[:-1], refs[-1]
    rows, cols = tok_ref.shape[:2]
    pairs = []
    for out_ref, (row, col) in zip(outs, corners(rows, cols)):
        for part, ref in enumerate((tok_ref, cot_ref)):
            source = ref.at[pl.ds(row, rows // 2), pl.ds(col, cols // 2)]
            pairs.append((source, out_ref.at[part]))
    run_copies(pairs, sem)


def fetch_body(*refs):
    count = len(refs) // 2
    run_copies(list(zip(refs[:count], refs[count:-1])), refs[-1])


def join_body(north_ref, east_ref, both_ref):
    both_ref[0] = north_ref[...]
    both_ref[1] = east_ref[1]


def unpack_body(stay_ref, east_ref, both_ref, tok_ref, w_out_ref, y_ref, grad_ref, att):
    rows, cols, levels, width = y_ref.shape
    inner = att.shape[-1]
    for quad, (row, col) in zip(
        (stay_ref, east_ref.at[0], both_ref.at[0], both_ref.at[1]), corners(rows, cols)
    ):
        at = (slice(row, row + rows // 2), slice(col, col + cols // 2))
        att[at] = quad[:, :, :, :inner]
        grad_ref[at] = quad[:, :, :, inner:]
    flat = att[...].reshape(rows * cols * levels, inner)
    mixed = dot(flat, w_out_ref[...], ((1,), (0,)))
    total = tok_ref[...].reshape(rows * cols * levels, width).astype(F32) + mixed
    y_ref[...] = total.astype(BF16).reshape(y_ref.shape)


def gather_window(quads, part, wide):
    levels, width = quads[0].shape[-2:]
    count = levels * quads[0].shape[1] * quads[0].shape[2]
    for place, item in enumerate(quads):
        wide[place * count : (place + 1) * count, :] = (
            item[part].reshape(count, width).astype(F32)
        )
    return wide[...]


def normalize(tokens_wide):
    average = jnp.mean(tokens_wide, axis=-1, keepdims=True)
    centered = tokens_wide - average
    inverse = lax.rsqrt(jnp.mean(centered * centered, axis=-1, keepdims=True) + 1e-05)
    return centered * inverse, inverse


def reorder(plan, places_ref, source, targets, base=0):
    group, counts, steps = plan
    half = source.shape[0] // 2
    for place in range(source.shape[0] // group):
        start = place * group
        if steps:
            block = places_ref[0] ^ steps[place][0]
            turned = places_ref[1] ^ steps[place][1]
            start = pl.multiple_of((block * counts[1] + turned) * group, group)
        at = place * group
        target = targets[at // half]
        at = base + at % half
        target[at : at + group, :] = source[pl.ds(start, group), :]


def pair_tools(total):
    lane = lax.broadcasted_iota(jnp.int32, (total, LANES), 1)
    first = lane < HDIM

    def alone(value, head):
        return jnp.where(first if head == 0 else ~first, value, jnp.zeros_like(value))

    def pick(results):
        return jnp.where(first, results[0], results[1])

    return alone, pick


def forward_body(
    plan, places_ref, r0, r1, r2, r3, w_qkv_ref, w_out_ref, gain_ref, bias_ref,
    mine_ref, peer_ref, factor_ref, query_ref, pair_ref, probs_ref, wide, side, bias_of,
):
    quads = (r0, r1, r2, r3)
    inner, width = w_out_ref.shape
    grad = gather_window(quads, 1, wide).astype(BF16)
    total = grad.shape[0]
    count = total // 4
    row_id = lax.broadcasted_iota(jnp.int32, (total, 1), 0)
    col_id = lax.broadcasted_iota(jnp.int32, (1, total), 1)
    row_side, col_side = ((i >= 2 * count).astype(jnp.int32) for i in (row_id, col_id))
    row_turn, col_turn = (
        ((i >= count) & (i < 2 * count) | (i >= 3 * count)).astype(jnp.int32)
        for i in (row_id, col_id)
    )
    last_lat, last_lon = ((places_ref[i] == n - 1).astype(jnp.int32) for i, n in enumerate(plan[1]))
    apart = (row_side ^ col_side) * last_lat + (row_turn ^ col_turn) * last_lon
    bias_of[...] = jnp.where(apart > 0, -1e30, 0.0)
    side[...] = grad.T
    reorder(plan, places_ref, side, (mine_ref, peer_ref), width // 2)
    pair_ref[:, 2 * inner :] = dot(grad, w_out_ref[...], ((1,), (1,))).astype(BF16)
    standard, _ = normalize(gather_window(quads, 0, wide))
    normed = (standard * gain_ref[...] + bias_ref[...]).astype(BF16)
    side[...] = normed.T
    reorder(plan, places_ref, side, (mine_ref, peer_ref))
    scale = jnp.asarray(HDIM ** (-0.5), BF16)
    query_ref[...] = dot(normed, w_qkv_ref[:, :inner], ((1,), (0,))).astype(BF16) * scale
    pair_ref[:, : 2 * inner] = dot(normed, w_qkv_ref[:, inner:], ((1,), (0,))).astype(BF16)
    alone, pick = pair_tools(total)
    for pair in range(inner // LANES):
        cols = slice(pair * LANES, (pair + 1) * LANES)
        query = query_ref[:, cols]
        key = pair_ref[:, cols]
        value = pair_ref[:, inner + pair * LANES : inner + (pair + 1) * LANES]
        grad_pair = pair_ref[:, 2 * inner + pair * LANES : 2 * inner + (pair + 1) * LANES]
        lows = []
        for head in range(2):
            scores = dot(alone(query, head), key, ((1,), (1,))) + bias_of[...]
            exps = jnp.exp(scores - jnp.max(scores, axis=-1, keepdims=True))
            probs = exps / jnp.sum(exps, axis=-1, keepdims=True)
            probs_ref[2 * pair + head] = probs
            lows.append(probs.astype(BF16))
        factor_ref[:, cols] = pick([dot(low, value, ((1,), (0,))) for low in lows]).astype(BF16)
        factor_ref[:, inner + pair * LANES : inner + (pair + 1) * LANES] = pick(
            [dot(low, grad_pair, ((0,), (0,))) for low in lows]
        ).astype(BF16)


def backward_body(query_ref, pair_ref, probs_ref, factor_ref):
    inner = query_ref.shape[1]
    scale = HDIM ** (-0.5)
    alone, pick = pair_tools(query_ref.shape[0])
    for pair in range(inner // LANES):
        cols = slice(pair * LANES, (pair + 1) * LANES)
        query = query_ref[:, cols]
        key = pair_ref[:, cols]
        value = pair_ref[:, inner + pair * LANES : inner + (pair + 1) * LANES]
        grad_pair = pair_ref[:, 2 * inner + pair * LANES : 2 * inner + (pair + 1) * LANES]
        lows = []
        for head in range(2):
            probs = probs_ref[2 * pair + head]
            grad_prob = dot(alone(grad_pair, head), value, ((1,), (1,)))
            inner_sum = jnp.sum(probs * grad_prob, axis=-1, keepdims=True)
            lows.append((probs * (grad_prob - inner_sum)).astype(BF16))
        factor_ref[:, cols] = (
            pick([dot(low, key, ((1,), (0,))) for low in lows]) * scale
        ).astype(BF16)
        factor_ref[:, inner + pair * LANES : inner + (pair + 1) * LANES] = pick(
            [dot(low, query, ((0,), (0,))) for low in lows]
        ).astype(BF16)


def gradient_body(
    plan, places_ref, r0, r1, r2, r3, factor_ref, late_ref, w_qkv_ref, gain_ref,
    stay_ref, east_ref, north_ref, mine_ref, peer_ref, wide, flat,
):
    quads = (r0, r1, r2, r3)
    inner, width = late_ref.shape[1] // 2, wide.shape[1]
    outs = (stay_ref, east_ref.at[0], north_ref, east_ref.at[1])
    quad = stay_ref.shape[:3]
    count = quad[0] * quad[1] * quad[2]
    tokens_wide = gather_window(quads, 0, wide)
    standard, inverse = normalize(tokens_wide)
    grad_normed = dot(factor_ref[:, inner:], w_qkv_ref[:, 2 * inner :], ((1,), (1,)))
    grad_normed += dot(late_ref[...], w_qkv_ref[:, : 2 * inner], ((1,), (1,)))
    sums = [
        jnp.sum(grad_normed * standard, axis=0, keepdims=True),
        jnp.sum(grad_normed, axis=0, keepdims=True),
    ]
    line = lax.broadcasted_iota(jnp.int32, (LANES, width), 0)
    flat[...] = jnp.where(line == 0, sums[0], jnp.where(line == 1, sums[1], 0.0)).T
    reorder(plan, places_ref, flat, (mine_ref, peer_ref))
    wide[:, :inner] = factor_ref[:, :inner].astype(F32)
    for place, out in enumerate(outs):
        rows = wide[place * count : (place + 1) * count, :inner]
        out[:, :, :, :inner] = rows.astype(BF16).reshape(*quad, inner)
    grad_hat = grad_normed * gain_ref[...]
    first = jnp.mean(grad_hat, axis=-1, keepdims=True)
    second = jnp.mean(grad_hat * standard, axis=-1, keepdims=True)
    change = (grad_hat - first - standard * second) * inverse
    wide[...] = gather_window(quads, 1, wide) + change
    for place, out in enumerate(outs):
        rows = wide[place * count : (place + 1) * count, :]
        out[:, :, :, inner:] = rows.astype(BF16).reshape(*quad, width)


def split_store(value, outs, cols):
    both, send_a, send_b = outs
    quarter = send_a.shape[0]
    for out, to, start in (
        (both, 0, 0), (send_a, 0, quarter), (both, quarter, 2 * quarter), (send_b, 0, 3 * quarter),
    ):
        out[to : to + quarter, cols] = value[start : start + quarter].astype(BF16)


def multiply(mine, got, factors, blocks, outs):
    half = mine.shape[0] // 2
    inner = factors[0].shape[1] // 2
    for place, block in enumerate(blocks):
        rows = slice(half, 2 * half) if block == 0 else slice(0, half)
        pair = 2 * (block // 2)
        at = block % 2 * inner
        value = dot(mine[rows, :], factors[pair][:, at : at + inner], ((1,), (0,)))
        value += dot(got[rows, :], factors[pair + 1][:, at : at + inner], ((1,), (0,)))
        split_store(value, outs, slice(place * inner, (place + 1) * inner))
    return len(blocks) * inner


def early_body(mine, got, *refs):
    multiply(mine, got, refs[:-3], EARLY, refs[-3:])


def late_body(mine, got, *refs):
    factors, (sums, sums_got), outs = refs[:-5], refs[-5:-3], refs[-3:]
    at = multiply(mine, got, factors, LATE, outs)
    split_store(sums[...] + sums_got[...], outs, slice(at, at + LANES))


def added(*refs):
    total = refs[0].astype(F32)
    for ref in refs[1:]:
        total += ref.astype(F32)
    return total


def second_body(keep, got_a, got_b, both, send_a, send_b):
    part = send_a.shape[0]
    for side, (got, send) in enumerate(((got_a, send_a), (got_b, send_b))):
        at = 2 * part * side
        both[part * side : part * (side + 1), :] = added(
            keep[at : at + part, :], got[:part, :]
        ).astype(BF16)
        send[...] = added(keep[at + part : at + 2 * part, :], got[part:, :]).astype(BF16)


def third_body(keep, got_a, got_b, *outs):
    part = got_a.shape[0]
    size = outs[0].shape[0]
    for place, out in enumerate(outs):
        start = place * size
        got = got_a if start < part else got_b
        within = start % part
        out[...] = added(keep[start : start + size, :], got[within : within + size, :]).astype(BF16)


def turn_body(keep, got_a, got_b, *outs):
    part = got_a.shape[0]
    size = outs[0].shape[0] // 2
    per_side = len(outs) // 2
    for place, out in enumerate(outs):
        got, base = (got_a, 0) if place < per_side else (got_b, part)
        for nested in range(2):
            at = nested * (part // 2) + (place % per_side) * size
            out[nested * size : (nested + 1) * size, :] = added(
                keep[base + at : base + at + size, :], got[at : at + size, :]
            ).astype(BF16)


def meet_body(*refs):
    pieces, (base, send_a, send_b) = refs[:-3], refs[-3:]
    size = base.shape[0]
    per_side = len(pieces) // 2
    base[...] = added(*(item[:size, :] for item in pieces))
    send_a[...] = added(*(item[size:, :] for item in pieces[:per_side])).astype(BF16)
    send_b[...] = added(*(item[size:, :] for item in pieces[per_side:])).astype(BF16)


def end_body(factor, base, got_a, got_b, *refs):
    pieces, (qkv_ref, out_ref, gain_ref, bias_ref) = refs[:-4], refs[-4:]
    early = added(base[...], got_a[...], got_b[...]) * factor
    total = added(*(item[...] for item in pieces)) * factor
    cols = total.shape[1] - LANES
    inner = cols // len(LATE)
    sources = {block: early[:, i * inner : (i + 1) * inner] for i, block in enumerate(EARLY)}
    out_ref[...] = sources[0]
    sources |= {block: total[:, i * inner : (i + 1) * inner] for i, block in enumerate(LATE)}
    for place, block in enumerate((2, 3, 1)):
        qkv_ref[:, place * inner : (place + 1) * inner] = sources[block]
    rows = total.shape[0]
    flat = jnp.concatenate([total[:, cols:], jnp.zeros((LANES - rows, LANES), F32)], axis=0).T
    gain_ref[...] = flat[0:1, :rows]
    bias_ref[...] = flat[1:2, :rows]


def xor_pairs(bit):
    return [(i, i ^ bit) for i in range(lax.axis_size("lat"))]


def swap(value, bit):
    return lax.ppermute(value, "lat", xor_pairs(bit))


def turn(pieces):
    pairs = lambda k: [(i, i ^ k) for i in range(len(pieces))]
    moved = pieces[:1]
    for k in range(1, len(pieces)):
        moved.append(lax.ppermute(pieces[k], "lon", pairs(k)))
    return moved


def sum_early(both, send_a, send_b, lon_count):
    quarter, cols = send_a.shape
    size = quarter // lon_count
    got_a, got_b = swap(send_a, 2), swap(send_b, 4)
    pieces = call(turn_body, [((2 * size, cols), BF16)] * lon_count, (both, got_a, got_b))
    pieces = turn(list(pieces))
    base, send_a, send_b = call(
        meet_body, [((size, cols), F32)] + [((size, cols), BF16)] * 2, pieces
    )
    got_a, got_b = swap(send_a, 4), swap(send_b, 2)
    return base, got_a, got_b


def sum_late(both, send_a, send_b, lon_count):
    quarter, cols = send_a.shape
    part = quarter // 2
    size = 2 * part // lon_count
    got_a, got_b = swap(send_a, 2), swap(send_b, 4)
    both, send_a, send_b = call(
        second_body, [((n * part, cols), BF16) for n in (2, 1, 1)], (both, got_a, got_b)
    )
    got_a, got_b = swap(send_a, 4), swap(send_b, 2)
    pieces = call(third_body, [((size, cols), BF16)] * lon_count, (both, got_a, got_b))
    pieces = turn(list(pieces))
    return pieces


def device_step(tokens, layer_norm_gain, layer_norm_bias, w_qkv, w_out, output_cotangent):
    levels, lat_rows, lon_cols, width = tokens.shape
    inner = w_out.shape[0]
    lat_count, lon_count = lax.axis_size("lat"), lax.axis_size("lon")
    lat_place, lon_place = lax.axis_index("lat"), lax.axis_index("lon")
    cells = levels * lat_rows * lon_cols
    norm_factor = 1.0 / math.sqrt(cells * lat_count * lon_count)

    def moved(lat_step, lon_step):
        pairs = []
        for i in range(lat_count):
            for j in range(lon_count):
                to = ((i + lat_step) % lat_count) * lon_count + (j + lon_step) % lon_count
                pairs.append((i * lon_count + j, to))
        return pairs

    steps = ((0, 1), (1, 0), (1, 1))
    by_turn = (0, 2, 1)

    def moved_all(items, sign):
        moves = {}
        for place in by_turn:
            a, b = steps[place]
            moves[place] = lax.ppermute(
                items[place], ("lat", "lon"), moved(sign * a, sign * b)
            )
        return [moves[place] for place in range(3)]

    grid = (lat_rows, lon_cols, levels, width)
    quad = (2, lat_rows // 2, lon_cols // 2, levels, width)
    tok = tokens.transpose(1, 2, 0, 3)
    cot = output_cotangent.transpose(1, 2, 0, 3)
    own, *sends = call(
        pack_body, [(quad, BF16)] * 4, (tok, cot), far=2,
        scratch=[pltpu.SemaphoreType.DMA((8,))],
    )
    quads = [own, *moved_all(sends, -1)]
    params = (w_qkv, w_out, layer_norm_gain.reshape(1, width), layer_norm_bias.reshape(1, width))
    params = (*params, tok)
    *params, tok = call(
        fetch_body, [(item.shape, item.dtype) for item in params], params, far=5,
        scratch=[pltpu.SemaphoreType.DMA((5,))],
    )

    share = width // (lat_count * lon_count)
    hyper = lat_count == 8 and lon_count in (2, 4, 8) and share % 16 == 0
    order = []
    if hyper:
        half_lon = lon_count // 2
        for core, side, outer, nested, k in itertools.product(
            range(2), range(2), range(2), range(2), range(half_lon)
        ):
            x_bit, y_bit = (outer, nested) if side == 0 else (nested, outer)
            order.append((core + 2 * x_bit + 4 * y_bit, side * half_lon + k))
    plan = (share if hyper else 16, (lat_count, lon_count), tuple(order))
    places = jnp.where(jnp.arange(2) == 0, lat_place, lon_place).astype(jnp.int32)
    heads = inner // HDIM
    mine, peer, factor, query, pairs, probs = call(
        functools.partial(forward_body, plan),
        [((width, cells), BF16)] * 2
        + [((cells, n * inner), BF16) for n in (2, 1, 3)]
        + [((heads, cells, cells), F32)],
        (places, *quads, *params),
        scratch=[
            pltpu.VMEM((cells, width), F32),
            pltpu.VMEM((width, cells), BF16),
            pltpu.VMEM((cells, cells), F32),
        ],
        smem=1,
    )
    (factor_late,) = call(backward_body, [((cells, 2 * inner), BF16)], (query, pairs, probs))
    part = (*quad[1:-1], inner + width)
    stay, east, north, sums, sums_peer = call(
        functools.partial(gradient_body, plan),
        [(shape, BF16) for shape in (part, (2, *part), part)] + [((width // 2, LANES), F32)] * 2,
        (places, *quads, factor, factor_late, params[0], params[2]),
        scratch=[pltpu.VMEM((cells, width), F32), pltpu.VMEM((width, LANES), F32)],
        smem=1,
    )
    if hyper:
        factor_got = swap(factor, 1)
        late_got = swap(factor_late, 1)
        got = swap(peer, 1)
        sums_got = swap(sums_peer, 1)
        quarter = width // 8

        def shapes(cols):
            return [((rows, cols), BF16) for rows in (2 * quarter, quarter, quarter)]

        factors = (factor, factor_got, factor_late, late_got)
        early = call(
            early_body, shapes(len(EARLY) * inner),
            (mine, got, *factors[: 2 * (EARLY[-1] // 2 + 1)]),
        )
        late = call(
            late_body, shapes(len(LATE) * inner + LANES),
            (mine, got, *factors, sums, sums_got),
        )
        parts = (*sum_early(*early, lon_count), *sum_late(*late, lon_count))
        d_qkv, d_out, gain, bias = call(
            functools.partial(end_body, norm_factor),
            [((share, n * inner), F32) for n in (3, 1)] + [((1, share), F32)] * 2,
            parts, near_out=0,
        )
    else:
        half = width // 2
        normed_t = jnp.concatenate([mine[:half], peer[:half]], axis=0)
        cot_t = jnp.concatenate([mine[half:], peer[half:]], axis=0)
        whole = jnp.concatenate(
            [
                dot(cot_t, factor[:, :inner], ((1,), (0,))),
                dot(normed_t, factor[:, inner:], ((1,), (0,))),
                dot(normed_t, factor_late, ((1,), (0,))),
                jnp.concatenate([sums, sums_peer], axis=0),
            ],
            axis=1,
        )
        whole = lax.psum_scatter(whole, "lat", scatter_dimension=0, tiled=True)
        whole = lax.psum_scatter(whole, "lon", scatter_dimension=0, tiled=True)
        whole = whole * norm_factor
        d_out = whole[:, :inner]
        d_qkv = jnp.concatenate([whole[:, 2 * inner : 4 * inner], whole[:, inner : 2 * inner]], axis=1)
        gain, bias = whole[:, 4 * inner], whole[:, 4 * inner + 1]
    east = lax.ppermute(east, ("lat", "lon"), moved(0, 1))
    (both,) = call(join_body, [((2, *part), BF16)], (north, east))
    both = lax.ppermute(both, ("lat", "lon"), moved(1, 0))
    y_out, token_gradient = call(
        unpack_body, [(grid, BF16)] * 2, (stay, east, both, tok, params[1]), near_out=0,
        scratch=[pltpu.VMEM((*grid[:-1], inner), BF16)],
    )
    return (
        y_out.transpose(2, 0, 1, 3),
        token_gradient.transpose(2, 0, 1, 3),
        d_qkv,
        d_out.T,
        gain.reshape(share),
        bias.reshape(share),
    )


def solution(mesh):
    in_specs = (P(None, "lat", "lon", None), P(), P(), P(), P(), P(None, "lat", "lon", None))
    out_specs = (
        P(None, "lat", "lon", None),
        P(None, "lat", "lon", None),
        P(("lat", "lon"), None),
        P(None, ("lat", "lon")),
        P(("lat", "lon")),
        P(("lat", "lon")),
    )
    return jax.shard_map(
        device_step, mesh=mesh, in_specs=in_specs, out_specs=out_specs, check_vma=False
    )
```

```python
import functools
import itertools
import math

import jax
import jax.numpy as jnp
from jax import lax
from jax.experimental import pallas as pl
from jax.experimental.pallas import tpu as pltpu
from jax.sharding import PartitionSpec as P


HDIM = 64
F32 = jnp.float32
EARLY = (0, 1)
LATE = (2, 3)
BF16 = jnp.bfloat16
LANES = 128

HBM_SPEC = pl.BlockSpec(memory_space=pltpu.HBM)

VMEM_SPEC = pl.BlockSpec(memory_space=pltpu.VMEM)
SMEM_SPEC = pl.BlockSpec(memory_space=pltpu.SMEM)


def dot(a, b, contract):
    return lax.dot_general(a, b, ((contract[0], contract[1]), ((), ())), preferred_element_type=F32)


def size_of(shape, dtype):
    rows = 16 if len(shape) > 1 and shape[-2] > 2 else shape[-2] if len(shape) > 1 else 1
    padded = [*shape[:-2], -(-shape[-2] // rows) * rows] if len(shape) > 1 else []
    return math.prod([*padded, -(-shape[-1] // LANES) * LANES]) * jnp.dtype(dtype).itemsize


def call(body, outs, args, scratch=(), smem=0, far=0, near_out=None, room=4):
    near_out = len(outs) if near_out is None else near_out
    near_at = smem + far
    held = sum(size_of(s, d) for s, d in outs[near_out:])
    held += sum(size_of(m.shape, m.dtype) for m in scratch if m.dtype in (F32, BF16))
    spaces = [None] * smem + [pltpu.HBM] * far + [pltpu.VMEM] * (len(args) - near_at)
    args = [
        a if space is None else pltpu.with_memory_space_constraint(a, space)
        for a, space in zip(args, spaces)
    ]
    return pl.pallas_call(
        body,
        out_shape=[
            pltpu.VMEM(s, d) if i < near_out else jax.ShapeDtypeStruct(s, d)
            for i, (s, d) in enumerate(outs)
        ],
        in_specs=[SMEM_SPEC] * smem + [HBM_SPEC] * far + [VMEM_SPEC] * (len(args) - near_at),
        out_specs=[VMEM_SPEC] * len(outs),
        scratch_shapes=list(scratch),
        compiler_params=pltpu.CompilerParams(vmem_limit_bytes=held + room * 2**20),
    )(*args)


def corners(rows, cols):
    return ((rows // 2, cols // 2), (rows // 2, 0), (0, cols // 2), (0, 0))


def run_copies(pairs, sem):
    copies = [
        pltpu.make_async_copy(source, target, sem.at[place])
        for place, (source, target) in enumerate(pairs)
    ]
    for item in copies:
        item.start()
    for item in copies:
        item.wait()


def pack_body(tok_ref, cot_ref, *refs):
    outs, sem = refs[:-1], refs[-1]
    rows, cols = tok_ref.shape[:2]
    pairs = []
    for out_ref, (row, col) in zip(outs, corners(rows, cols)):
        for part, ref in enumerate((tok_ref, cot_ref)):
            source = ref.at[pl.ds(row, rows // 2), pl.ds(col, cols // 2)]
            pairs.append((source, out_ref.at[part]))
    run_copies(pairs, sem)


def fetch_body(*refs):
    count = len(refs) // 2
    run_copies(list(zip(refs[:count], refs[count:-1])), refs[-1])


def join_body(north_ref, east_ref, both_ref):
    both_ref[0] = north_ref[...]
    both_ref[1] = east_ref[1]


def unpack_body(stay_ref, east_ref, both_ref, tok_ref, w_out_ref, y_ref, grad_ref, att):
    rows, cols, levels, width = y_ref.shape
    inner = att.shape[-1]
    for quad, (row, col) in zip(
        (stay_ref, east_ref.at[0], both_ref.at[0], both_ref.at[1]), corners(rows, cols)
    ):
        at = (slice(row, row + rows // 2), slice(col, col + cols // 2))
        att[at] = quad[:, :, :, :inner]
        grad_ref[at] = quad[:, :, :, inner:]
    flat = att[...].reshape(rows * cols * levels, inner)
    mixed = dot(flat, w_out_ref[...], ((1,), (0,)))
    total = tok_ref[...].reshape(rows * cols * levels, width).astype(F32) + mixed
    y_ref[...] = total.astype(BF16).reshape(y_ref.shape)


def gather_window(quads, part, wide):
    levels, width = quads[0].shape[-2:]
    count = levels * quads[0].shape[1] * quads[0].shape[2]
    for place, item in enumerate(quads):
        wide[place * count : (place + 1) * count, :] = (
            item[part].reshape(count, width).astype(F32)
        )
    return wide[...]


def normalize(tokens_wide):
    average = jnp.mean(tokens_wide, axis=-1, keepdims=True)
    centered = tokens_wide - average
    inverse = lax.rsqrt(jnp.mean(centered * centered, axis=-1, keepdims=True) + 1e-05)
    return centered * inverse, inverse


def reorder(plan, places_ref, source, targets, base=0):
    group, counts, steps = plan
    half = source.shape[0] // 2
    for place in range(source.shape[0] // group):
        start = place * group
        if steps:
            block = places_ref[0] ^ steps[place][0]
            turned = places_ref[1] ^ steps[place][1]
            start = pl.multiple_of((block * counts[1] + turned) * group, group)
        at = place * group
        target = targets[at // half]
        at = base + at % half
        target[at : at + group, :] = source[pl.ds(start, group), :]


def pair_tools(total):
    lane = lax.broadcasted_iota(jnp.int32, (total, LANES), 1)
    first = lane < HDIM

    def alone(value, head):
        return jnp.where(first if head == 0 else ~first, value, jnp.zeros_like(value))

    def pick(results):
        return jnp.where(first, results[0], results[1])

    return alone, pick


def forward_body(
    plan, places_ref, r0, r1, r2, r3, w_qkv_ref, w_out_ref, gain_ref, bias_ref,
    mine_ref, peer_ref, factor_ref, query_ref, pair_ref, probs_ref, standard_ref, inverse_ref,
    wide, side, bias_of,
):
    quads = (r0, r1, r2, r3)
    inner, width = w_out_ref.shape
    grad = gather_window(quads, 1, wide).astype(BF16)
    total = grad.shape[0]
    count = total // 4
    row_id = lax.broadcasted_iota(jnp.int32, (total, 1), 0)
    col_id = lax.broadcasted_iota(jnp.int32, (1, total), 1)
    row_side, col_side = ((i >= 2 * count).astype(jnp.int32) for i in (row_id, col_id))
    row_turn, col_turn = (
        ((i >= count) & (i < 2 * count) | (i >= 3 * count)).astype(jnp.int32)
        for i in (row_id, col_id)
    )
    last_lat, last_lon = ((places_ref[i] == n - 1).astype(jnp.int32) for i, n in enumerate(plan[1]))
    apart = (row_side ^ col_side) * last_lat + (row_turn ^ col_turn) * last_lon
    bias_of[...] = jnp.where(apart > 0, -1e30, 0.0)
    side[...] = grad.T
    reorder(plan, places_ref, side, (mine_ref, peer_ref), width // 2)
    pair_ref[:, 2 * inner :] = dot(grad, w_out_ref[...], ((1,), (1,))).astype(BF16)
    standard, inverse = normalize(gather_window(quads, 0, wide))
    standard_ref[...] = standard
    inverse_ref[...] = jnp.broadcast_to(inverse, inverse_ref.shape)
    normed = (standard * gain_ref[...] + bias_ref[...]).astype(BF16)
    side[...] = normed.T
    reorder(plan, places_ref, side, (mine_ref, peer_ref))
    scale = jnp.asarray(HDIM ** (-0.5), BF16)
    query_ref[...] = dot(normed, w_qkv_ref[:, :inner], ((1,), (0,))).astype(BF16) * scale
    pair_ref[:, : 2 * inner] = dot(normed, w_qkv_ref[:, inner:], ((1,), (0,))).astype(BF16)
    alone, pick = pair_tools(total)
    for pair in range(inner // LANES):
        cols = slice(pair * LANES, (pair + 1) * LANES)
        query = query_ref[:, cols]
        key = pair_ref[:, cols]
        value = pair_ref[:, inner + pair * LANES : inner + (pair + 1) * LANES]
        grad_pair = pair_ref[:, 2 * inner + pair * LANES : 2 * inner + (pair + 1) * LANES]
        lows = []
        for head in range(2):
            scores = dot(alone(query, head), key, ((1,), (1,))) + bias_of[...]
            exps = jnp.exp(scores - jnp.max(scores, axis=-1, keepdims=True))
            probs = exps / jnp.sum(exps, axis=-1, keepdims=True)
            probs_ref[2 * pair + head] = probs
            lows.append(probs.astype(BF16))
        factor_ref[:, cols] = pick([dot(low, value, ((1,), (0,))) for low in lows]).astype(BF16)
        factor_ref[:, inner + pair * LANES : inner + (pair + 1) * LANES] = pick(
            [dot(low, grad_pair, ((0,), (0,))) for low in lows]
        ).astype(BF16)


def backward_body(query_ref, pair_ref, probs_ref, factor_ref):
    inner = query_ref.shape[1]
    scale = HDIM ** (-0.5)
    alone, pick = pair_tools(query_ref.shape[0])
    for pair in range(inner // LANES):
        cols = slice(pair * LANES, (pair + 1) * LANES)
        query = query_ref[:, cols]
        key = pair_ref[:, cols]
        value = pair_ref[:, inner + pair * LANES : inner + (pair + 1) * LANES]
        grad_pair = pair_ref[:, 2 * inner + pair * LANES : 2 * inner + (pair + 1) * LANES]
        lows = []
        for head in range(2):
            probs = probs_ref[2 * pair + head]
            grad_prob = dot(alone(grad_pair, head), value, ((1,), (1,)))
            inner_sum = jnp.sum(probs * grad_prob, axis=-1, keepdims=True)
            lows.append((probs * (grad_prob - inner_sum)).astype(BF16))
        factor_ref[:, cols] = (
            pick([dot(low, key, ((1,), (0,))) for low in lows]) * scale
        ).astype(BF16)
        factor_ref[:, inner + pair * LANES : inner + (pair + 1) * LANES] = pick(
            [dot(low, query, ((0,), (0,))) for low in lows]
        ).astype(BF16)


def gradient_body(
    plan, places_ref, r0, r1, r2, r3, standard_ref, inverse_ref, factor_ref, late_ref, w_qkv_ref,
    gain_ref,
    stay_ref, east_ref, north_ref, mine_ref, peer_ref, wide, flat,
):
    quads = (r0, r1, r2, r3)
    inner, width = late_ref.shape[1] // 2, wide.shape[1]
    outs = (stay_ref, east_ref.at[0], north_ref, east_ref.at[1])
    quad = stay_ref.shape[:3]
    count = quad[0] * quad[1] * quad[2]
    standard, inverse = standard_ref[...], inverse_ref[:, 0:1]
    grad_normed = dot(factor_ref[:, inner:], w_qkv_ref[:, 2 * inner :], ((1,), (1,)))
    grad_normed += dot(late_ref[...], w_qkv_ref[:, : 2 * inner], ((1,), (1,)))
    sums = [
        jnp.sum(grad_normed * standard, axis=0, keepdims=True),
        jnp.sum(grad_normed, axis=0, keepdims=True),
    ]
    line = lax.broadcasted_iota(jnp.int32, (LANES, width), 0)
    flat[...] = jnp.where(line == 0, sums[0], jnp.where(line == 1, sums[1], 0.0)).T
    reorder(plan, places_ref, flat, (mine_ref, peer_ref))
    wide[:, :inner] = factor_ref[:, :inner].astype(F32)
    for place, out in enumerate(outs):
        rows = wide[place * count : (place + 1) * count, :inner]
        out[:, :, :, :inner] = rows.astype(BF16).reshape(*quad, inner)
    grad_hat = grad_normed * gain_ref[...]
    first = jnp.mean(grad_hat, axis=-1, keepdims=True)
    second = jnp.mean(grad_hat * standard, axis=-1, keepdims=True)
    change = (grad_hat - first - standard * second) * inverse
    wide[...] = gather_window(quads, 1, wide) + change
    for place, out in enumerate(outs):
        rows = wide[place * count : (place + 1) * count, :]
        out[:, :, :, inner:] = rows.astype(BF16).reshape(*quad, width)


def split_store(value, outs, cols):
    both, send_a, send_b = outs
    quarter = send_a.shape[0]
    for out, to, start in (
        (both, 0, 0), (send_a, 0, quarter), (both, quarter, 2 * quarter), (send_b, 0, 3 * quarter),
    ):
        out[to : to + quarter, cols] = value[start : start + quarter].astype(BF16)


def multiply(mine, got, factors, blocks, outs):
    half = mine.shape[0] // 2
    inner = factors[0].shape[1] // 2
    for place, block in enumerate(blocks):
        rows = slice(half, 2 * half) if block == 0 else slice(0, half)
        pair = 2 * (block // 2)
        at = block % 2 * inner
        value = dot(mine[rows, :], factors[pair][:, at : at + inner], ((1,), (0,)))
        value += dot(got[rows, :], factors[pair + 1][:, at : at + inner], ((1,), (0,)))
        split_store(value, outs, slice(place * inner, (place + 1) * inner))
    return len(blocks) * inner


def early_body(mine, got, *refs):
    multiply(mine, got, refs[:-3], EARLY, refs[-3:])


def late_body(mine, got, *refs):
    factors, (sums, sums_got), outs = refs[:-5], refs[-5:-3], refs[-3:]
    at = multiply(mine, got, factors, LATE, outs)
    split_store(sums[...] + sums_got[...], outs, slice(at, at + LANES))


def added(*refs):
    total = refs[0].astype(F32)
    for ref in refs[1:]:
        total += ref.astype(F32)
    return total


def second_body(keep, got_a, got_b, both, send_a, send_b):
    part = send_a.shape[0]
    for side, (got, send) in enumerate(((got_a, send_a), (got_b, send_b))):
        at = 2 * part * side
        both[part * side : part * (side + 1), :] = added(
            keep[at : at + part, :], got[:part, :]
        ).astype(BF16)
        send[...] = added(keep[at + part : at + 2 * part, :], got[part:, :]).astype(BF16)


def third_body(keep, got_a, got_b, *outs):
    part = got_a.shape[0]
    size = outs[0].shape[0]
    for place, out in enumerate(outs):
        start = place * size
        got = got_a if start < part else got_b
        within = start % part
        out[...] = added(keep[start : start + size, :], got[within : within + size, :]).astype(BF16)


def turn_body(keep, got_a, got_b, *outs):
    part = got_a.shape[0]
    size = outs[0].shape[0] // 2
    per_side = len(outs) // 2
    for place, out in enumerate(outs):
        got, base = (got_a, 0) if place < per_side else (got_b, part)
        for nested in range(2):
            at = nested * (part // 2) + (place % per_side) * size
            out[nested * size : (nested + 1) * size, :] = added(
                keep[base + at : base + at + size, :], got[at : at + size, :]
            ).astype(BF16)


def meet_body(*refs):
    pieces, (base, send_a, send_b) = refs[:-3], refs[-3:]
    size = base.shape[0]
    per_side = len(pieces) // 2
    base[...] = added(*(item[:size, :] for item in pieces))
    send_a[...] = added(*(item[size:, :] for item in pieces[:per_side])).astype(BF16)
    send_b[...] = added(*(item[size:, :] for item in pieces[per_side:])).astype(BF16)


def end_body(factor, base, got_a, got_b, *refs):
    pieces, (qkv_ref, out_ref, gain_ref, bias_ref) = refs[:-4], refs[-4:]
    early = added(base[...], got_a[...], got_b[...]) * factor
    total = added(*(item[...] for item in pieces)) * factor
    cols = total.shape[1] - LANES
    inner = cols // len(LATE)
    sources = {block: early[:, i * inner : (i + 1) * inner] for i, block in enumerate(EARLY)}
    out_ref[...] = sources[0]
    sources |= {block: total[:, i * inner : (i + 1) * inner] for i, block in enumerate(LATE)}
    for place, block in enumerate((2, 3, 1)):
        qkv_ref[:, place * inner : (place + 1) * inner] = sources[block]
    rows = total.shape[0]
    flat = jnp.concatenate([total[:, cols:], jnp.zeros((LANES - rows, LANES), F32)], axis=0).T
    gain_ref[...] = flat[0:1, :rows]
    bias_ref[...] = flat[1:2, :rows]


def xor_pairs(bit):
    return [(i, i ^ bit) for i in range(lax.axis_size("lat"))]


def swap(value, bit):
    return lax.ppermute(value, "lat", xor_pairs(bit))


def turn(pieces):
    pairs = lambda k: [(i, i ^ k) for i in range(len(pieces))]
    moved = pieces[:1]
    for k in range(1, len(pieces)):
        moved.append(lax.ppermute(pieces[k], "lon", pairs(k)))
    return moved


def sum_early(both, send_a, send_b, lon_count):
    quarter, cols = send_a.shape
    size = quarter // lon_count
    got_a, got_b = swap(send_a, 2), swap(send_b, 4)
    pieces = call(turn_body, [((2 * size, cols), BF16)] * lon_count, (both, got_a, got_b))
    pieces = turn(list(pieces))
    base, send_a, send_b = call(
        meet_body, [((size, cols), F32)] + [((size, cols), BF16)] * 2, pieces
    )
    got_a, got_b = swap(send_a, 4), swap(send_b, 2)
    return base, got_a, got_b


def sum_late(both, send_a, send_b, lon_count):
    quarter, cols = send_a.shape
    part = quarter // 2
    size = 2 * part // lon_count
    got_a, got_b = swap(send_a, 2), swap(send_b, 4)
    both, send_a, send_b = call(
        second_body, [((n * part, cols), BF16) for n in (2, 1, 1)], (both, got_a, got_b)
    )
    got_a, got_b = swap(send_a, 4), swap(send_b, 2)
    pieces = call(third_body, [((size, cols), BF16)] * lon_count, (both, got_a, got_b))
    pieces = turn(list(pieces))
    return pieces


def device_step(tokens, layer_norm_gain, layer_norm_bias, w_qkv, w_out, output_cotangent):
    levels, lat_rows, lon_cols, width = tokens.shape
    inner = w_out.shape[0]
    lat_count, lon_count = lax.axis_size("lat"), lax.axis_size("lon")
    lat_place, lon_place = lax.axis_index("lat"), lax.axis_index("lon")
    cells = levels * lat_rows * lon_cols
    norm_factor = 1.0 / math.sqrt(cells * lat_count * lon_count)

    def moved(lat_step, lon_step):
        pairs = []
        for i in range(lat_count):
            for j in range(lon_count):
                to = ((i + lat_step) % lat_count) * lon_count + (j + lon_step) % lon_count
                pairs.append((i * lon_count + j, to))
        return pairs

    steps = ((0, 1), (1, 0), (1, 1))
    by_turn = (0, 2, 1)

    def moved_all(items, sign):
        moves = {}
        for place in by_turn:
            a, b = steps[place]
            moves[place] = lax.ppermute(
                items[place], ("lat", "lon"), moved(sign * a, sign * b)
            )
        return [moves[place] for place in range(3)]

    grid = (lat_rows, lon_cols, levels, width)
    quad = (2, lat_rows // 2, lon_cols // 2, levels, width)
    tok = tokens.transpose(1, 2, 0, 3)
    cot = output_cotangent.transpose(1, 2, 0, 3)
    own, *sends = call(
        pack_body, [(quad, BF16)] * 4, (tok, cot), far=2,
        scratch=[pltpu.SemaphoreType.DMA((8,))],
    )
    quads = [own, *moved_all(sends, -1)]
    params = (w_qkv, w_out, layer_norm_gain.reshape(1, width), layer_norm_bias.reshape(1, width))
    params = (*params, tok)
    *params, tok = call(
        fetch_body, [(item.shape, item.dtype) for item in params], params, far=5,
        scratch=[pltpu.SemaphoreType.DMA((5,))],
    )

    share = width // (lat_count * lon_count)
    hyper = lat_count == 8 and lon_count in (2, 4, 8) and share % 16 == 0
    order = []
    if hyper:
        half_lon = lon_count // 2
        for core, side, outer, nested, k in itertools.product(
            range(2), range(2), range(2), range(2), range(half_lon)
        ):
            x_bit, y_bit = (outer, nested) if side == 0 else (nested, outer)
            order.append((core + 2 * x_bit + 4 * y_bit, side * half_lon + k))
    plan = (share if hyper else 16, (lat_count, lon_count), tuple(order))
    places = jnp.where(jnp.arange(2) == 0, lat_place, lon_place).astype(jnp.int32)
    heads = inner // HDIM
    mine, peer, factor, query, pairs, probs, standard, inverse = call(
        functools.partial(forward_body, plan),
        [((width, cells), BF16)] * 2
        + [((cells, n * inner), BF16) for n in (2, 1, 3)]
        + [(shape, F32) for shape in ((heads, cells, cells), (cells, width), (cells, LANES))],
        (places, *quads, *params),
        scratch=[
            pltpu.VMEM((cells, width), F32),
            pltpu.VMEM((width, cells), BF16),
            pltpu.VMEM((cells, cells), F32),
        ],
        smem=1,
    )
    (factor_late,) = call(backward_body, [((cells, 2 * inner), BF16)], (query, pairs, probs))
    part = (*quad[1:-1], inner + width)
    stay, east, north, sums, sums_peer = call(
        functools.partial(gradient_body, plan),
        [(shape, BF16) for shape in (part, (2, *part), part)] + [((width // 2, LANES), F32)] * 2,
        (places, *quads, standard, inverse, factor, factor_late, params[0], params[2]),
        scratch=[pltpu.VMEM((cells, width), F32), pltpu.VMEM((width, LANES), F32)],
        smem=1,
    )
    if hyper:
        factor_got = swap(factor, 1)
        late_got = swap(factor_late, 1)
        got = swap(peer, 1)
        sums_got = swap(sums_peer, 1)
        quarter = width // 8

        def shapes(cols):
            return [((rows, cols), BF16) for rows in (2 * quarter, quarter, quarter)]

        factors = (factor, factor_got, factor_late, late_got)
        early = call(
            early_body, shapes(len(EARLY) * inner),
            (mine, got, *factors[: 2 * (EARLY[-1] // 2 + 1)]),
        )
        late = call(
            late_body, shapes(len(LATE) * inner + LANES),
            (mine, got, *factors, sums, sums_got),
        )
        parts = (*sum_early(*early, lon_count), *sum_late(*late, lon_count))
        d_qkv, d_out, gain, bias = call(
            functools.partial(end_body, norm_factor),
            [((share, n * inner), F32) for n in (3, 1)] + [((1, share), F32)] * 2,
            parts, near_out=0,
        )
    else:
        half = width // 2
        normed_t = jnp.concatenate([mine[:half], peer[:half]], axis=0)
        cot_t = jnp.concatenate([mine[half:], peer[half:]], axis=0)
        whole = jnp.concatenate(
            [
                dot(cot_t, factor[:, :inner], ((1,), (0,))),
                dot(normed_t, factor[:, inner:], ((1,), (0,))),
                dot(normed_t, factor_late, ((1,), (0,))),
                jnp.concatenate([sums, sums_peer], axis=0),
            ],
            axis=1,
        )
        whole = lax.psum_scatter(whole, "lat", scatter_dimension=0, tiled=True)
        whole = lax.psum_scatter(whole, "lon", scatter_dimension=0, tiled=True)
        whole = whole * norm_factor
        d_out = whole[:, :inner]
        d_qkv = jnp.concatenate([whole[:, 2 * inner : 4 * inner], whole[:, inner : 2 * inner]], axis=1)
        gain, bias = whole[:, 4 * inner], whole[:, 4 * inner + 1]
    east = lax.ppermute(east, ("lat", "lon"), moved(0, 1))
    (both,) = call(join_body, [((2, *part), BF16)], (north, east))
    both = lax.ppermute(both, ("lat", "lon"), moved(1, 0))
    y_out, token_gradient = call(
        unpack_body, [(grid, BF16)] * 2, (stay, east, both, tok, params[1]), near_out=0,
        scratch=[pltpu.VMEM((*grid[:-1], inner), BF16)],
    )
    return (
        y_out.transpose(2, 0, 1, 3),
        token_gradient.transpose(2, 0, 1, 3),
        d_qkv,
        d_out.T,
        gain.reshape(share),
        bias.reshape(share),
    )


def solution(mesh):
    in_specs = (P(None, "lat", "lon", None), P(), P(), P(), P(), P(None, "lat", "lon", None))
    out_specs = (
        P(None, "lat", "lon", None),
        P(None, "lat", "lon", None),
        P(("lat", "lon"), None),
        P(None, ("lat", "lon")),
        P(("lat", "lon")),
        P(("lat", "lon")),
    )
    return jax.shard_map(
        device_step, mesh=mesh, in_specs=in_specs, out_specs=out_specs, check_vma=False
    )
```
